128 devices in a mesh: data: 1, store: 2 (over core), model: 64 (over z, y, x).
Axes of the slice: x: 4, y: 4, z: 4, core: 2. Of those that a mesh axis runs over, the one named last changes fastest.
Arguments:
- queries: bfloat16 [16, 2560], P('data')
- w_head: bfloat16 [2560, 51200], P(None, 'model')
- store_keys: bfloat16 [262144, 2560], P(('store', 'model'))
- store_tok: int32 [262144], P(('store', 'model'))
- temperature: float32 [], replicated
- mix_weight: float32 [], replicated
Outputs:
- output: float32 [16, 51200], P(('data', 'store'), 'model')
All inputs are finite; a program needn't handle non-finite values.
Results may differ from the reference program's by a relative error of at most 0.001.
Values are sent between devices in bfloat16 or wider.
A program may use at most 1 GiB of HBM per device.

```python
import jax
import jax.numpy as jnp
from jax import lax

HIDDEN = 2560
VOCAB = 51200
ROWS_DEV = 8
KEYS_DEV = 2048
STORE_DEVS = 2
MODEL_DEVS = 64
BATCH = ROWS_DEV * STORE_DEVS
SHARDS = STORE_DEVS * MODEL_DEVS
N_KEYS = KEYS_DEV * SHARDS


def setup_inputs(seed: int = 0, part: int = 0) -> dict:
    base_key = jax.random.key(seed)
    part_key = jax.random.fold_in(base_key, part)
    key_head, key_store, key_tok_a, key_tok_b, key_temp, key_mix = jax.random.split(base_key, 6)
    queries = jax.random.normal(part_key, (BATCH, HIDDEN), jnp.float32)
    w_head = jax.random.normal(key_head, (HIDDEN, VOCAB), jnp.float32) * HIDDEN ** -0.5
    store_keys = jax.random.normal(key_store, (N_KEYS, HIDDEN), jnp.float32)
    tok_a = jax.random.randint(key_tok_a, (N_KEYS,), 0, VOCAB, jnp.int32)
    tok_b = jax.random.randint(key_tok_b, (N_KEYS,), 0, VOCAB, jnp.int32)
    store_tok = jnp.minimum(tok_a, tok_b).at[0].set(0).at[N_KEYS - 1].set(VOCAB - 1)
    temperature = (6.0 * HIDDEN) ** 0.5 / 1.5 * jax.random.uniform(key_temp, (), jnp.float32, minval=0.6, maxval=1.5)
    mix_weight = jax.random.uniform(key_mix, (), jnp.float32, minval=0.25, maxval=0.5)
    return {"queries": queries.astype(jnp.bfloat16), "w_head": w_head.astype(jnp.bfloat16), "store_keys": store_keys.astype(jnp.bfloat16), "store_tok": store_tok, "temperature": temperature, "mix_weight": mix_weight}


def reference(queries, w_head, store_keys, store_tok, temperature, mix_weight):
    key_blocks = store_keys.reshape(SHARDS, KEYS_DEV, HIDDEN)
    tok_blocks = store_tok.reshape(SHARDS, KEYS_DEV)

    def block_scores(block):
        key_dots = jnp.dot(block, queries.T, preferred_element_type=jnp.float32)
        key_norms = jnp.sum(jnp.square(block.astype(jnp.float32)), axis=1)
        return (2.0 * key_dots - key_norms[:, None]) / temperature

    block_top = lax.map(lambda block: jnp.max(block_scores(block), axis=0), key_blocks)
    row_top = jnp.max(block_top, axis=0)

    def accumulate(carry, pair):
        histogram, row_total = carry
        block, tok_ids = pair
        weights = jnp.exp(block_scores(block) - row_top)
        histogram = histogram + jax.ops.segment_sum(weights, tok_ids, num_segments=VOCAB)
        row_total = row_total + jnp.sum(weights, axis=0)
        return (histogram, row_total), None

    init_state = (jnp.zeros((VOCAB, BATCH), jnp.float32), jnp.zeros((BATCH,), jnp.float32))
    (histogram, row_total), _ = lax.scan(accumulate, init_state, (key_blocks, tok_blocks))
    knn_prob = (histogram / row_total).T
    logits = jnp.dot(queries, w_head, preferred_element_type=jnp.float32)
    lm_exp = jnp.exp(logits - jnp.max(logits, axis=1, keepdims=True))
    lm_prob = lm_exp / jnp.sum(lm_exp, axis=1, keepdims=True)
    return jnp.log(mix_weight * knn_prob + (1.0 - mix_weight) * lm_prob)
```

```python
import functools

import jax
import jax.numpy as jnp
from jax import lax
from jax.experimental import pallas as pl
from jax.experimental.pallas import tpu as pltpu
from jax.sharding import PartitionSpec as P

F32 = jnp.float32
LANES = 128
RING = 4
CHIPS = RING**3
ROWS = 8
GROUPS = LANES // ROWS
SLOTS = 18
PARTS = 3
BLOCK = SLOTS * CHIPS // RING
MSG = BLOCK + 8
BLOCK2 = BLOCK // RING
MSG2 = BLOCK2 + 8
MSG3 = 24
NBUF = 4
HROWS = 2 * SLOTS * CHIPS * PARTS
MESH = pl.DeviceIdType.MESH


def fit(cond, a, b):
    return jnp.where(cond, a, b)


def local_kernel(tau_ref, idx_ref, grp_ref, q_ref, k_ref, out_ref, qrep, sc, wx, top, *hist):
    step = pl.program_id(0)
    steps = pl.num_programs(0)
    kb = k_ref.shape[0]
    n_keys = sc.shape[0]

    @pl.when(step == 0)
    def _():
        for h in range(2):
            half = q_ref[h * ROWS : (h + 1) * ROWS, :].astype(F32)
            pair = jnp.concatenate([half, half], axis=0).astype(jnp.bfloat16)
            for g in range(GROUPS // 2):
                qrep[pl.ds(h * LANES + g * 2 * ROWS, 2 * ROWS), :] = pair
        top[...] = jnp.full(top.shape, -jnp.inf, F32)

    zero_rows = HROWS * NBUF // steps // NBUF
    span = 288

    @pl.loop(0, zero_rows // span)
    def _(i):
        for buf in hist:
            buf[pl.ds(pl.multiple_of(step * zero_rows + i * span, 8), span), :] = jnp.zeros((span, LANES), F32)

    keys = k_ref[...]
    dots = lax.dot_general(keys, qrep[...], (((1,), (1,)), ((), ())), preferred_element_type=F32)
    kf = keys.astype(F32)
    norms = jnp.sum(kf * kf, axis=1, keepdims=True)
    scores = (2.0 * dots - norms) / tau_ref[0, 0]
    sc[pl.ds(pl.multiple_of(step * kb, kb), kb), :] = scores
    top[...] = jnp.maximum(top[...], jnp.max(scores.reshape(kb // 8, 8, 2 * LANES), axis=0))

    @pl.when(step == steps - 1)
    def _():
        m = jnp.max(top[...], axis=0, keepdims=True)
        lane_group = (lax.broadcasted_iota(jnp.int32, (LANES, LANES), 1) // ROWS).astype(F32)

        def expand(c, z):
            s = sc[pl.ds(pl.multiple_of(c * LANES, LANES), LANES), :]
            w = jnp.exp(s - m)
            mine = jnp.broadcast_to(grp_ref[pl.ds(c, 1), :], (LANES, LANES)).T == lane_group
            for h in range(2):
                wx[pl.ds(c * 2 * LANES + h, LANES, stride=2), :] = jnp.where(mine, w[:, h * LANES : (h + 1) * LANES], 0.0)
            return z + jnp.sum(w.reshape(LANES // 8, 8, 2 * LANES), axis=0)

        z = lax.fori_loop(0, n_keys // LANES, expand, jnp.zeros((8, 2 * LANES), F32))
        z = jnp.sum(z, axis=0, keepdims=True)

        unroll = 8

        @pl.loop(0, n_keys // unroll)
        def _(i):
            for u in range(0, unroll, NBUF):
                at = [pl.ds(pl.multiple_of(idx_ref[i * unroll + u + b], 2), 2) for b in range(NBUF)]
                new = [
                    hist[b][at[b], :] + wx[pl.ds(pl.multiple_of((i * unroll + u + b) * 2, 2), 2), :]
                    for b in range(NBUF)
                ]
                for b in range(NBUF):
                    hist[b][at[b], :] = new[b]

        pad = jnp.zeros((6, LANES), F32)

        @pl.loop(0, PARTS * RING)
        def _(blk):
            for h in range(2):
                for t in range(BLOCK // 8):
                    at = pl.ds(blk * 2 * BLOCK + t * 16 + h, 8, stride=2)
                    total = hist[0][at, :]
                    for b in range(1, NBUF):
                        total = total + hist[b][at, :]
                    out_ref[h, blk, t * 8 : t * 8 + 8, :] = total
                lanes = slice(h * LANES, (h + 1) * LANES)
                out_ref[h, blk, BLOCK:MSG, :] = jnp.concatenate([m[:, lanes], z[:, lanes], pad], axis=0)


def comm_kernel(
    mix_ref, hist, q_ref, w_hbm, out_ref,
    wv, logits, din, d, r1, e, r2, g3, r3, tsc, knn,
    wsem, s0, v0, s1, v1, s2, v2, s3, v3,
):
    core = lax.axis_index("store")
    chip = lax.axis_index("model")
    x, y, z = chip % RING, (chip // RING) % RING, chip // (RING * RING)
    dims = ((x, 1), (y, RING), (z, RING * RING))
    order = ((0, 1, 2), (1, 2, 0), (2, 0, 1))

    def peer(axis, delta):
        at, stride = dims[axis]
        return {"model": chip + ((at + delta) % RING - at) * stride}

    barrier = pltpu.get_barrier_semaphore()
    pl.semaphore_signal(barrier, inc=1, device_id={"store": 1 - core}, device_id_type=MESH)
    for axis in range(3):
        for delta in range(1, RING):
            pl.semaphore_signal(barrier, inc=1, device_id=peer(axis, delta), device_id_type=MESH)
    head = pltpu.make_async_copy(w_hbm, wv, wsem)
    head.start()
    pl.semaphore_wait(barrier, 10)

    sends = []

    def send(src, dst, ssem, rsem, to):
        copy = pltpu.make_async_remote_copy(src_ref=src, dst_ref=dst, send_sem=ssem, recv_sem=rsem, device_id=to, device_id_type=MESH)
        copy.start()
        sends.append(copy)
        return copy

    deltas = (2, 1, 3, 0)
    first = {}
    for delta in deltas:
        for p in range(PARTS):
            at = dims[order[p][0]][0]
            blk = p * RING + (at + delta) % RING
            n = p * RING + delta
            first[p, delta] = (blk, send(hist.at[1 - core, blk], din.at[blk], s0.at[n], v0.at[n], {"store": 1 - core}))

    head.wait()
    both = lax.dot_general(q_ref[...], wv[...], (((1,), (0,)), ((), ())), preferred_element_type=F32)
    mine = jnp.where(core == 0, both[:ROWS], both[ROWS:])
    logits[...] = mine
    lm_top = jnp.max(mine, axis=1, keepdims=True)
    lm_sum = jnp.sum(jnp.exp(mine - lm_top), axis=1, keepdims=True)
    lane = lax.broadcasted_iota(jnp.int32, (ROWS, LANES), 1)
    pair = jnp.where(lane == 0, lm_top, lm_sum)
    tsc[...] = jnp.concatenate([pair] * GROUPS, axis=0)
    pair = tsc[...].T
    lm_stats = pair[0:2, :]

    pad = jnp.zeros((4, LANES), F32)

    m_own = hist[core, 0, BLOCK : BLOCK + 1, :]
    z_own = hist[core, 0, BLOCK + 1 : BLOCK + 2, :]
    stage1 = {}
    scale = None
    for delta in deltas:
        for p in range(PARTS):
            blk, copy = first[p, delta]
            copy.wait_recv()
            if scale is None:
                m_par = din[blk, BLOCK : BLOCK + 1, :]
                m = jnp.maximum(m_own, m_par)
                a, b = jnp.exp(m_own - m), jnp.exp(m_par - m)
                zz = a * z_own + b * din[blk, BLOCK + 1 : BLOCK + 2, :]
                stats = jnp.concatenate([m, zz, lm_stats, pad], axis=0)
                scale = a, b
            a, b = scale
            d[blk, 0:BLOCK, :] = a * hist[core, blk, 0:BLOCK, :] + b * din[blk, 0:BLOCK, :]
            d[blk, BLOCK:MSG, :] = stats
            if delta:
                n = p * 3 + delta - 1
                stage1[p, delta] = send(d.at[blk], r1.at[p, delta - 1], s1.at[n], v1.at[n], peer(order[p][0], delta))

    def combine(stats):
        m = functools.reduce(jnp.maximum, [s[0:1] for s in stats])
        scales = [jnp.exp(s[0:1] - m) for s in stats]
        zz = sum(c * s[1:2] for c, s in zip(scales, stats))
        lm_m = functools.reduce(jnp.maximum, [s[2:3] for s in stats])
        lm_z = sum(jnp.exp(s[2:3] - lm_m) * s[3:4] for s in stats)
        return scales, jnp.concatenate([m, zz, lm_m, lm_z, pad], axis=0)

    stage2 = {}
    for p in range(PARTS):
        for delta in range(1, RING):
            stage1[p, delta].wait_recv()
        own = p * RING + dims[order[p][0]][0]
        scales, stats = combine([d[own, BLOCK:MSG, :]] + [r1[p, i, BLOCK:MSG, :] for i in range(3)])
        for c in range(RING):
            rows = slice(c * BLOCK2, (c + 1) * BLOCK2)
            total = scales[0] * d[own, rows, :]
            for i in range(3):
                total = total + scales[i + 1] * r1[p, i, rows, :]
            e[p, c, 0:BLOCK2, :] = total
            e[p, c, BLOCK2:MSG2, :] = stats
        for delta in deltas[:3]:
            to = (dims[order[p][1]][0] + delta) % RING
            n = p * 3 + delta - 1
            stage2[p, delta] = send(e.at[p, to], r2.at[p, delta - 1], s2.at[n], v2.at[n], peer(order[p][1], delta))

    stage3 = {}
    for p in range(PARTS):
        for delta in range(1, RING):
            stage2[p, delta].wait_recv()
        own = dims[order[p][1]][0]
        scales, stats = combine([e[p, own, BLOCK2:MSG2, :]] + [r2[p, i, BLOCK2:MSG2, :] for i in range(3)])
        for c in range(RING):
            rows = slice(c * SLOTS, (c + 1) * SLOTS)
            total = scales[0] * e[p, own, rows, :]
            for i in range(3):
                total = total + scales[i + 1] * r2[p, i, rows, :]
            g3[p, c, 0:SLOTS, :] = total
            g3[p, c, SLOTS:MSG3, :] = stats[0 : MSG3 - SLOTS]
        for delta in deltas[:3]:
            to = (dims[order[p][2]][0] + delta) % RING
            n = p * 3 + delta - 1
            stage3[p, delta] = send(g3.at[p, to], r3.at[p, delta - 1], s3.at[n], v3.at[n], peer(order[p][2], delta))

    tsc[...] = jnp.zeros(tsc.shape, F32)
    slots = logits.shape[1] // GROUPS
    for p in range(PARTS):
        for delta in range(1, RING):
            stage3[p, delta].wait_recv()
        own = dims[order[p][2]][0]
        blocks = [g3[p, own]] + [r3[p, i] for i in range(3)]
        scales, stats = combine([v[SLOTS : SLOTS + 4] for v in blocks])
        count = min(SLOTS, slots - p * SLOTS)
        total = sum(c * v[0:count] for c, v in zip(scales, blocks))
        tsc[p * SLOTS : p * SLOTS + count, :] = total / stats[1:2]
        if p == 0:
            tsc[slots : slots + 2, :] = stats[2:4]

    turned = tsc[...].T
    for g in range(GROUPS):
        knn[:, g * slots : (g + 1) * slots] = turned[g * ROWS : (g + 1) * ROWS, 0:slots]
    lm = jnp.exp(logits[...] - turned[0:ROWS, slots : slots + 1]) / turned[0:ROWS, slots + 1 : slots + 2]
    mix = mix_ref[0, 0]
    out_ref[...] = jnp.log(mix * knn[...] + (1.0 - mix) * lm)

    for copy in sends:
        copy.wait_send()


def solution(mesh):
    def local_step(queries, w_head, store_keys, store_tok, temperature, mix_weight):
        n_keys, width = store_keys.shape
        vocab_loc = w_head.shape[1]
        slots = vocab_loc // GROUPS
        kb = n_keys // 4

        chip, within = store_tok // vocab_loc, store_tok % vocab_loc
        group, slot = within // slots, within % slots
        part, row = slot // SLOTS, slot % SLOTS
        x, y, z = chip % RING, (chip // RING) % RING, chip // (RING * RING)
        first = jnp.where(part == 0, x, jnp.where(part == 1, y, z))
        second = jnp.where(part == 0, y, jnp.where(part == 1, z, x))
        third = jnp.where(part == 0, z, jnp.where(part == 1, x, y))
        place = ((part * RING + first) * RING + second) * RING + third
        index = (place * SLOTS + row) * 2
        group = group.astype(F32).reshape(n_keys // LANES, LANES)

        hist = pl.pallas_call(
            local_kernel,
            grid=(n_keys // kb,),
            out_shape=jax.ShapeDtypeStruct((2, PARTS * RING, MSG, LANES), F32),
            in_specs=[
                pl.BlockSpec(memory_space=pltpu.SMEM),
                pl.BlockSpec(memory_space=pltpu.SMEM),
                pl.BlockSpec((n_keys // LANES, LANES), lambda i: (0, 0)),
                pl.BlockSpec(queries.shape, lambda i: (0, 0)),
                pl.BlockSpec((kb, width), lambda i: (i, 0)),
            ],
            out_specs=pl.BlockSpec((2, PARTS * RING, MSG, LANES), lambda i: (0, 0, 0, 0)),
            scratch_shapes=[
                pltpu.VMEM((2 * LANES, width), jnp.bfloat16),
                pltpu.VMEM((n_keys, 2 * LANES), F32),
                pltpu.VMEM((2 * n_keys, LANES), F32),
                pltpu.VMEM((8, 2 * LANES), F32),
            ]
            + [pltpu.VMEM((HROWS, LANES), F32)] * NBUF,
            compiler_params=pltpu.CompilerParams(vmem_limit_bytes=56 * 2**20),
            name="histogram",
        )(temperature.reshape(1, 1), index, group, queries, store_keys)

        return pl.pallas_call(
            comm_kernel,
            out_shape=jax.ShapeDtypeStruct((ROWS, vocab_loc), F32),
            in_specs=[
                pl.BlockSpec(memory_space=pltpu.SMEM),
                pl.BlockSpec(memory_space=pltpu.VMEM),
                pl.BlockSpec(memory_space=pltpu.VMEM),
                pl.BlockSpec(memory_space=pl.ANY),
            ],
            out_specs=pl.BlockSpec(memory_space=pltpu.VMEM),
            scratch_shapes=[
                pltpu.VMEM(w_head.shape, jnp.bfloat16),
                pltpu.VMEM((ROWS, vocab_loc), F32),
                pltpu.VMEM((PARTS * RING, MSG, LANES), F32),
                pltpu.VMEM((PARTS * RING, MSG, LANES), F32),
                pltpu.VMEM((PARTS, RING - 1, MSG, LANES), F32),
                pltpu.VMEM((PARTS, RING, MSG2, LANES), F32),
                pltpu.VMEM((PARTS, RING - 1, MSG2, LANES), F32),
                pltpu.VMEM((PARTS, RING, MSG3, LANES), F32),
                pltpu.VMEM((PARTS, RING - 1, MSG3, LANES), F32),
                pltpu.VMEM((LANES, LANES), F32),
                pltpu.VMEM((ROWS, vocab_loc), F32),
                pltpu.SemaphoreType.DMA,
                pltpu.SemaphoreType.DMA((12,)),
                pltpu.SemaphoreType.DMA((12,)),
            ]
            + [pltpu.SemaphoreType.DMA((9,))] * 6,
            compiler_params=pltpu.CompilerParams(collective_id=0, has_side_effects=True, vmem_limit_bytes=48 * 2**20),
            name="exchange",
        )(mix_weight.reshape(1, 1), hist, queries, w_head)

    return jax.shard_map(
        local_step,
        mesh=mesh,
        in_specs=(P("data", None), P(None, "model"), P(("store", "model"), None), P(("store", "model")), P(), P()),
        out_specs=P(("data", "store"), "model"),
        check_vma=False,
    )
```

```python
import functools

import jax
import jax.numpy as jnp
from jax import lax
from jax.experimental import pallas as pl
from jax.experimental.pallas import tpu as pltpu
from jax.sharding import PartitionSpec as P

F32 = jnp.float32
LANES = 128
RING = 4
CHIPS = RING**3
ROWS = 8
GROUPS = LANES // ROWS
SLOTS = 18
PARTS = 3
BLOCK = SLOTS * CHIPS // RING
MSG = BLOCK + 8
BLOCK2 = BLOCK // RING
MSG2 = BLOCK2 + 8
MSG3 = 24
NBUF = 4
HROWS = 2 * SLOTS * CHIPS * PARTS
MESH = pl.DeviceIdType.MESH


def fit(cond, a, b):
    return jnp.where(cond, a, b)


def local_kernel(tau_ref, idx_ref, grp_ref, q_ref, k_ref, out_ref, qrep, sc, wx, top, *hist):
    step = pl.program_id(0)
    steps = pl.num_programs(0)
    kb = k_ref.shape[0]
    n_keys = sc.shape[0]

    @pl.when(step == 0)
    def _():
        for h in range(2):
            half = q_ref[h * ROWS : (h + 1) * ROWS, :].astype(F32)
            pair = jnp.concatenate([half, half], axis=0).astype(jnp.bfloat16)
            for g in range(GROUPS // 2):
                qrep[pl.ds(h * LANES + g * 2 * ROWS, 2 * ROWS), :] = pair
        top[...] = jnp.full(top.shape, -jnp.inf, F32)

    zero_rows = HROWS * NBUF // steps // NBUF
    span = 288

    @pl.loop(0, zero_rows // span)
    def _(i):
        for buf in hist:
            buf[pl.ds(pl.multiple_of(step * zero_rows + i * span, 8), span), :] = jnp.zeros((span, LANES), F32)

    keys = k_ref[...]
    dots = lax.dot_general(keys, qrep[...], (((1,), (1,)), ((), ())), preferred_element_type=F32)
    kf = keys.astype(F32)
    norms = jnp.sum(kf * kf, axis=1, keepdims=True)
    scores = (2.0 * dots - norms) / tau_ref[0, 0]
    sc[pl.ds(pl.multiple_of(step * kb, kb), kb), :] = scores
    top[...] = jnp.maximum(top[...], jnp.max(scores.reshape(kb // 8, 8, 2 * LANES), axis=0))

    @pl.when(step == steps - 1)
    def _():
        m = jnp.max(top[...], axis=0, keepdims=True)
        lane_group = (lax.broadcasted_iota(jnp.int32, (LANES, LANES), 1) // ROWS).astype(F32)

        def expand(c, z):
            s = sc[pl.ds(pl.multiple_of(c * LANES, LANES), LANES), :]
            w = jnp.exp(s - m)
            mine = jnp.broadcast_to(grp_ref[pl.ds(c, 1), :], (LANES, LANES)).T == lane_group
            for h in range(2):
                wx[pl.ds(c * 2 * LANES + h, LANES, stride=2), :] = jnp.where(mine, w[:, h * LANES : (h + 1) * LANES], 0.0)
            return z + jnp.sum(w.reshape(LANES // 8, 8, 2 * LANES), axis=0)

        z = lax.fori_loop(0, n_keys // LANES, expand, jnp.zeros((8, 2 * LANES), F32))
        z = jnp.sum(z, axis=0, keepdims=True)

        unroll = 8

        @pl.loop(0, n_keys // unroll)
        def _(i):
            for u in range(0, unroll, NBUF):
                at = [pl.ds(pl.multiple_of(idx_ref[i * unroll + u + b], 2), 2) for b in range(NBUF)]
                new = [
                    hist[b][at[b], :] + wx[pl.ds(pl.multiple_of((i * unroll + u + b) * 2, 2), 2), :]
                    for b in range(NBUF)
                ]
                for b in range(NBUF):
                    hist[b][at[b], :] = new[b]

        pad = jnp.zeros((6, LANES), F32)

        @pl.loop(0, PARTS * RING)
        def _(blk):
            for h in range(2):
                for t in range(BLOCK // 8):
                    at = pl.ds(blk * 2 * BLOCK + t * 16 + h, 8, stride=2)
                    total = hist[0][at, :]
                    for b in range(1, NBUF):
                        total = total + hist[b][at, :]
                    out_ref[h, blk, t * 8 : t * 8 + 8, :] = total
                lanes = slice(h * LANES, (h + 1) * LANES)
                out_ref[h, blk, BLOCK:MSG, :] = jnp.concatenate([m[:, lanes], z[:, lanes], pad], axis=0)


def comm_kernel(
    mix_ref, hist, q_ref, w_ref, out_ref,
    logits, din, d, r1, e, r2, g3, r3, tsc, knn,
    s0, v0, s1, v1, s2, v2, s3, v3,
):
    core = lax.axis_index("store")
    chip = lax.axis_index("model")
    x, y, z = chip % RING, (chip // RING) % RING, chip // (RING * RING)
    dims = ((x, 1), (y, RING), (z, RING * RING))
    order = ((0, 1, 2), (1, 2, 0), (2, 0, 1))

    def peer(axis, delta):
        at, stride = dims[axis]
        return {"model": chip + ((at + delta) % RING - at) * stride}

    barrier = pltpu.get_barrier_semaphore()
    pl.semaphore_signal(barrier, inc=1, device_id={"store": 1 - core}, device_id_type=MESH)
    for axis in range(3):
        for delta in range(1, RING):
            pl.semaphore_signal(barrier, inc=1, device_id=peer(axis, delta), device_id_type=MESH)
    pl.semaphore_wait(barrier, 10)

    sends = []

    def send(src, dst, ssem, rsem, to):
        copy = pltpu.make_async_remote_copy(src_ref=src, dst_ref=dst, send_sem=ssem, recv_sem=rsem, device_id=to, device_id_type=MESH)
        copy.start()
        sends.append(copy)
        return copy

    deltas = (2, 1, 3, 0)
    first = {}
    for delta in deltas:
        for p in range(PARTS):
            at = dims[order[p][0]][0]
            blk = p * RING + (at + delta) % RING
            n = p * RING + delta
            first[p, delta] = (blk, send(hist.at[1 - core, blk], din.at[blk], s0.at[n], v0.at[n], {"store": 1 - core}))

    both = lax.dot_general(q_ref[...], w_ref[...], (((1,), (1,)), ((), ())), preferred_element_type=F32)
    mine = jnp.where(core == 0, both[:ROWS], both[ROWS:])
    logits[...] = mine
    lm_top = jnp.max(mine, axis=1, keepdims=True)
    lm_sum = jnp.sum(jnp.exp(mine - lm_top), axis=1, keepdims=True)
    lane = lax.broadcasted_iota(jnp.int32, (ROWS, LANES), 1)
    pair = jnp.where(lane == 0, lm_top, lm_sum)
    tsc[...] = jnp.concatenate([pair] * GROUPS, axis=0)
    pair = tsc[...].T
    lm_stats = pair[0:2, :]

    pad = jnp.zeros((4, LANES), F32)

    m_own = hist[core, 0, BLOCK : BLOCK + 1, :]
    z_own = hist[core, 0, BLOCK + 1 : BLOCK + 2, :]
    stage1 = {}
    scale = None
    for delta in deltas:
        for p in range(PARTS):
            blk, copy = first[p, delta]
            copy.wait_recv()
            if scale is None:
                m_par = din[blk, BLOCK : BLOCK + 1, :]
                m = jnp.maximum(m_own, m_par)
                a, b = jnp.exp(m_own - m), jnp.exp(m_par - m)
                zz = a * z_own + b * din[blk, BLOCK + 1 : BLOCK + 2, :]
                stats = jnp.concatenate([m, zz, lm_stats, pad], axis=0)
                scale = a, b
            a, b = scale
            d[blk, 0:BLOCK, :] = a * hist[core, blk, 0:BLOCK, :] + b * din[blk, 0:BLOCK, :]
            d[blk, BLOCK:MSG, :] = stats
            if delta:
                n = p * 3 + delta - 1
                stage1[p, delta] = send(d.at[blk], r1.at[p, delta - 1], s1.at[n], v1.at[n], peer(order[p][0], delta))

    def combine(stats):
        m = functools.reduce(jnp.maximum, [s[0:1] for s in stats])
        scales = [jnp.exp(s[0:1] - m) for s in stats]
        zz = sum(c * s[1:2] for c, s in zip(scales, stats))
        lm_m = functools.reduce(jnp.maximum, [s[2:3] for s in stats])
        lm_z = sum(jnp.exp(s[2:3] - lm_m) * s[3:4] for s in stats)
        return scales, jnp.concatenate([m, zz, lm_m, lm_z, pad], axis=0)

    stage2 = {}
    for p in range(PARTS):
        for delta in range(1, RING):
            stage1[p, delta].wait_recv()
        own = p * RING + dims[order[p][0]][0]
        scales, stats = combine([d[own, BLOCK:MSG, :]] + [r1[p, i, BLOCK:MSG, :] for i in range(3)])
        for c in range(RING):
            rows = slice(c * BLOCK2, (c + 1) * BLOCK2)
            total = scales[0] * d[own, rows, :]
            for i in range(3):
                total = total + scales[i + 1] * r1[p, i, rows, :]
            e[p, c, 0:BLOCK2, :] = total
            e[p, c, BLOCK2:MSG2, :] = stats
        for delta in deltas[:3]:
            to = (dims[order[p][1]][0] + delta) % RING
            n = p * 3 + delta - 1
            stage2[p, delta] = send(e.at[p, to], r2.at[p, delta - 1], s2.at[n], v2.at[n], peer(order[p][1], delta))

    stage3 = {}
    for p in range(PARTS):
        for delta in range(1, RING):
            stage2[p, delta].wait_recv()
        own = dims[order[p][1]][0]
        scales, stats = combine([e[p, own, BLOCK2:MSG2, :]] + [r2[p, i, BLOCK2:MSG2, :] for i in range(3)])
        for c in range(RING):
            rows = slice(c * SLOTS, (c + 1) * SLOTS)
            total = scales[0] * e[p, own, rows, :]
            for i in range(3):
                total = total + scales[i + 1] * r2[p, i, rows, :]
            g3[p, c, 0:SLOTS, :] = total
            g3[p, c, SLOTS:MSG3, :] = stats[0 : MSG3 - SLOTS]
        for delta in deltas[:3]:
            to = (dims[order[p][2]][0] + delta) % RING
            n = p * 3 + delta - 1
            stage3[p, delta] = send(g3.at[p, to], r3.at[p, delta - 1], s3.at[n], v3.at[n], peer(order[p][2], delta))

    tsc[...] = jnp.zeros(tsc.shape, F32)
    slots = logits.shape[1] // GROUPS
    for p in range(PARTS):
        for delta in range(1, RING):
            stage3[p, delta].wait_recv()
        own = dims[order[p][2]][0]
        blocks = [g3[p, own]] + [r3[p, i] for i in range(3)]
        scales, stats = combine([v[SLOTS : SLOTS + 4] for v in blocks])
        count = min(SLOTS, slots - p * SLOTS)
        total = sum(c * v[0:count] for c, v in zip(scales, blocks))
        tsc[p * SLOTS : p * SLOTS + count, :] = total / stats[1:2]
        if p == 0:
            tsc[slots : slots + 2, :] = stats[2:4]

    turned = tsc[...].T
    for g in range(GROUPS):
        knn[:, g * slots : (g + 1) * slots] = turned[g * ROWS : (g + 1) * ROWS, 0:slots]
    lm = jnp.exp(logits[...] - turned[0:ROWS, slots : slots + 1]) / turned[0:ROWS, slots + 1 : slots + 2]
    mix = mix_ref[0, 0]
    out_ref[...] = jnp.log(mix * knn[...] + (1.0 - mix) * lm)

    for copy in sends:
        copy.wait_send()


def solution(mesh):
    def local_step(queries, w_head, store_keys, store_tok, temperature, mix_weight):
        n_keys, width = store_keys.shape
        vocab_loc = w_head.shape[1]
        slots = vocab_loc // GROUPS
        kb = n_keys // 4

        chip, within = store_tok // vocab_loc, store_tok % vocab_loc
        group, slot = within // slots, within % slots
        part, row = slot // SLOTS, slot % SLOTS
        x, y, z = chip % RING, (chip // RING) % RING, chip // (RING * RING)
        first = jnp.where(part == 0, x, jnp.where(part == 1, y, z))
        second = jnp.where(part == 0, y, jnp.where(part == 1, z, x))
        third = jnp.where(part == 0, z, jnp.where(part == 1, x, y))
        place = ((part * RING + first) * RING + second) * RING + third
        index = (place * SLOTS + row) * 2
        group = group.astype(F32).reshape(n_keys // LANES, LANES)

        hist = pl.pallas_call(
            local_kernel,
            grid=(n_keys // kb,),
            out_shape=jax.ShapeDtypeStruct((2, PARTS * RING, MSG, LANES), F32),
            in_specs=[
                pl.BlockSpec(memory_space=pltpu.SMEM),
                pl.BlockSpec(memory_space=pltpu.SMEM),
                pl.BlockSpec((n_keys // LANES, LANES), lambda i: (0, 0)),
                pl.BlockSpec(queries.shape, lambda i: (0, 0)),
                pl.BlockSpec((kb, width), lambda i: (i, 0)),
            ],
            out_specs=pl.BlockSpec((2, PARTS * RING, MSG, LANES), lambda i: (0, 0, 0, 0)),
            scratch_shapes=[
                pltpu.VMEM((2 * LANES, width), jnp.bfloat16),
                pltpu.VMEM((n_keys, 2 * LANES), F32),
                pltpu.VMEM((2 * n_keys, LANES), F32),
                pltpu.VMEM((8, 2 * LANES), F32),
            ]
            + [pltpu.VMEM((HROWS, LANES), F32)] * NBUF,
            compiler_params=pltpu.CompilerParams(vmem_limit_bytes=50 * 2**20),
            name="histogram",
        )(temperature.reshape(1, 1), index, group, queries, store_keys)

        return pl.pallas_call(
            comm_kernel,
            out_shape=jax.ShapeDtypeStruct((ROWS, vocab_loc), F32),
            in_specs=[
                pl.BlockSpec(memory_space=pltpu.SMEM),
                pl.BlockSpec(memory_space=pltpu.VMEM),
                pl.BlockSpec(memory_space=pltpu.VMEM),
                pl.BlockSpec(memory_space=pltpu.VMEM),
            ],
            out_specs=pl.BlockSpec(memory_space=pltpu.VMEM),
            scratch_shapes=[
                pltpu.VMEM((ROWS, vocab_loc), F32),
                pltpu.VMEM((PARTS * RING, MSG, LANES), F32),
                pltpu.VMEM((PARTS * RING, MSG, LANES), F32),
                pltpu.VMEM((PARTS, RING - 1, MSG, LANES), F32),
                pltpu.VMEM((PARTS, RING, MSG2, LANES), F32),
                pltpu.VMEM((PARTS, RING - 1, MSG2, LANES), F32),
                pltpu.VMEM((PARTS, RING, MSG3, LANES), F32),
                pltpu.VMEM((PARTS, RING - 1, MSG3, LANES), F32),
                pltpu.VMEM((LANES, LANES), F32),
                pltpu.VMEM((ROWS, vocab_loc), F32),
                pltpu.SemaphoreType.DMA((12,)),
                pltpu.SemaphoreType.DMA((12,)),
            ]
            + [pltpu.SemaphoreType.DMA((9,))] * 6,
            compiler_params=pltpu.CompilerParams(collective_id=0, has_side_effects=True, vmem_limit_bytes=20 * 2**20),
            name="exchange",
        )(mix_weight.reshape(1, 1), hist, queries, w_head.T)

    return jax.shard_map(
        local_step,
        mesh=mesh,
        in_specs=(P("data", None), P(None, "model"), P(("store", "model"), None), P(("store", "model")), P(), P()),
        out_specs=P(("data", "store"), "model"),
        check_vma=False,
    )
```

```python
import functools

import jax
import jax.numpy as jnp
from jax import lax
from jax.experimental import pallas as pl
from jax.experimental.pallas import tpu as pltpu
from jax.sharding import PartitionSpec as P

F32 = jnp.float32
LANES = 128
RING = 4
CHIPS = RING**3
ROWS = 8
GROUPS = LANES // ROWS
SLOTS = 18
PARTS = 3
BLOCK = SLOTS * CHIPS // RING
BLOCK2 = BLOCK // RING
STAT = 8
MSG = STAT + BLOCK
MSG2 = STAT + BLOCK2
MSG3 = 24
NBUF = 4
KA_LIMIT = 36
KB_LIMIT = 36
HROWS = 2 * SLOTS * CHIPS * PARTS
MESH = pl.DeviceIdType.MESH


def local_kernel(vocab_loc, tau_ref, tok_hbm, q_hbm, k_hbm, *refs):
    hist, stats_ref = refs[:NBUF], refs[NBUF]
    q_ref, k_ref, qrep, sc, wx, grp, idx, idx_smem, tok_ref, qsem, isem, tsem, ksem = refs[NBUF + 1 :]
    n_keys = k_ref.shape[0]
    quarter = n_keys // NBUF
    chunk = quarter // 2

    def fetch(j):
        rows = pl.ds(pl.multiple_of(j * chunk, chunk), chunk)
        return pltpu.make_async_copy(k_hbm.at[rows], k_ref.at[rows], ksem.at[j])

    get_tok = pltpu.make_async_copy(tok_hbm, tok_ref, tsem)
    get_tok.start()
    get_q = pltpu.make_async_copy(q_hbm, q_ref, qsem)
    get_q.start()
    for j in range(n_keys // chunk):
        fetch(j).start()

    span = 288

    @pl.loop(0, HROWS // span)
    def _(i):
        for buf in hist:
            buf[pl.ds(pl.multiple_of(i * span, 8), span), :] = jnp.zeros((span, LANES), F32)

    get_tok.wait()
    tok = tok_ref[...]
    chip, within = tok // vocab_loc, tok % vocab_loc
    slots = vocab_loc // GROUPS
    group, slot = within // slots, within % slots
    part, row = slot // SLOTS, slot % SLOTS
    x, y, z = chip % RING, (chip // RING) % RING, chip // (RING * RING)
    first = jnp.where(part == 0, x, jnp.where(part == 1, y, z))
    second = jnp.where(part == 0, y, jnp.where(part == 1, z, x))
    third = jnp.where(part == 0, z, jnp.where(part == 1, x, y))
    place = ((part * RING + first) * RING + second) * RING + third
    idx[...] = (place * SLOTS + row) * 2
    put_idx = pltpu.make_async_copy(idx, idx_smem, isem)
    put_idx.start()
    group = group.astype(F32)
    for c in range(n_keys // LANES):
        grp[c * LANES : (c + 1) * LANES, :] = jnp.broadcast_to(group[c : c + 1, :], (LANES, LANES)).T

    get_q.wait()
    for h in range(2):
        half = q_ref[h * ROWS : (h + 1) * ROWS, :].astype(F32)
        pair = jnp.concatenate([half, half], axis=0).astype(jnp.bfloat16)
        for g in range(GROUPS // 2):
            qrep[pl.ds(h * LANES + g * 2 * ROWS, 2 * ROWS), :] = pair

    tau = tau_ref[0, 0]
    lane_group = (lax.broadcasted_iota(jnp.int32, (LANES, LANES), 1) // ROWS).astype(F32)

    @pl.loop(0, NBUF)
    def _(b):
        top = jnp.full((8, 2 * LANES), -jnp.inf, F32)
        for sub in range(2):
            fetch(b * 2 + sub).wait()
            keys = k_ref[pl.ds(pl.multiple_of((b * 2 + sub) * chunk, chunk), chunk), :]
            dots = lax.dot_general(keys, qrep[...], (((1,), (1,)), ((), ())), preferred_element_type=F32)
            kf = keys.astype(F32)
            norms = jnp.sum(kf * kf, axis=1, keepdims=True)
            scores = (2.0 * dots - norms) / tau
            sc[sub * chunk : (sub + 1) * chunk, :] = scores
            top = jnp.maximum(top, jnp.max(scores.reshape(chunk // 8, 8, 2 * LANES), axis=0))
        m = jnp.max(top, axis=0, keepdims=True)
        total = jnp.zeros((8, 2 * LANES), F32)
        for c in range(quarter // LANES):
            w = jnp.exp(sc[c * LANES : (c + 1) * LANES, :] - m)
            total = total + jnp.sum(w.reshape(LANES // 8, 8, 2 * LANES), axis=0)
            at = b * quarter + c * LANES
            mine = grp[pl.ds(pl.multiple_of(at, LANES), LANES), :] == lane_group
            for h in range(2):
                wx[pl.ds(at * 2 + h, LANES, stride=2), :] = jnp.where(mine, w[:, h * LANES : (h + 1) * LANES], 0.0)
        total = jnp.sum(total, axis=0, keepdims=True)
        stats_ref[pl.ds(b, 1), :] = m
        stats_ref[pl.ds(NBUF + b, 1), :] = total

    put_idx.wait()
    unroll = 2

    @pl.loop(0, quarter // LANES)
    def _(c):
        @pl.loop(0, LANES // unroll)
        def _(i):
            for u in range(unroll):
                lane = i * unroll + u
                at = [pl.ds(pl.multiple_of(idx_smem[b * (quarter // LANES) + c, lane], 2), 2) for b in range(NBUF)]
                key = c * LANES + lane
                new = [
                    hist[b][at[b], :] + wx[pl.ds(pl.multiple_of((b * quarter + key) * 2, 2), 2), :]
                    for b in range(NBUF)
                ]
                for b in range(NBUF):
                    hist[b][at[b], :] = new[b]


def comm_kernel(
    mix_ref, h0, h1, h2, h3, kstats, q_ref, w_hbm, out_ref,
    w_ref, logits, loc, din, d, r1, e, r2, g3, r3, lt, lr, tsc, knn,
    wsem, s0, v0, s1, v1, s2, v2, s3, v3, sl, vl,
):
    core = lax.axis_index("store")
    chip = lax.axis_index("model")
    x, y, z = chip % RING, (chip // RING) % RING, chip // (RING * RING)
    dims = ((x, 1), (y, RING), (z, RING * RING))
    order = ((0, 1, 2), (1, 2, 0), (2, 0, 1))
    scope = jax.named_scope

    def peer(axis, delta):
        at, stride = dims[axis]
        return {"model": chip + ((at + delta) % RING - at) * stride}

    barrier = pltpu.get_barrier_semaphore()
    pl.semaphore_signal(barrier, inc=1, device_id={"store": 1 - core}, device_id_type=MESH)
    for axis in range(3):
        for delta in range(1, RING):
            pl.semaphore_signal(barrier, inc=1, device_id=peer(axis, delta), device_id_type=MESH)
    head = pltpu.make_async_copy(w_hbm, w_ref, wsem)
    head.start()

    hist = (h0, h1, h2, h3)
    top = functools.reduce(jnp.maximum, [kstats[b : b + 1, :] for b in range(NBUF)])
    scales = [jnp.exp(kstats[b : b + 1, :] - top) for b in range(NBUF)]
    mass = sum(c * kstats[NBUF + b : NBUF + b + 1, :] for b, c in enumerate(scales))
    half = [slice(h * LANES, (h + 1) * LANES) for h in range(2)]

    with scope("sum"):

        @pl.loop(0, PARTS * RING)
        def _(blk):
            for h in range(2):
                loc[h, blk, 0:STAT, :] = jnp.concatenate(
                    [top[:, half[h]], mass[:, half[h]], jnp.zeros((STAT - 2, LANES), F32)], axis=0
                )
                for t in range(BLOCK // 8):
                    at = pl.ds(blk * 2 * BLOCK + t * 16 + h, 8, stride=2)
                    total = scales[0][:, half[h]] * hist[0][at, :]
                    for b in range(1, NBUF):
                        total = total + scales[b][:, half[h]] * hist[b][at, :]
                    loc[h, blk, STAT + t * 8 : STAT + t * 8 + 8, :] = total

    with scope("barrier"):
        pl.semaphore_wait(barrier, 10)

    def copy(src, dst, ssem, rsem, to):
        return pltpu.make_async_remote_copy(src_ref=src, dst_ref=dst, send_sem=ssem, recv_sem=rsem, device_id=to, device_id_type=MESH)

    def span(b):
        return slice(0, MSG2) if b == 0 else slice(STAT + b * BLOCK2, STAT + (b + 1) * BLOCK2)

    def body(b):
        return slice(STAT + b * BLOCK2, STAT + (b + 1) * BLOCK2)

    near = {}
    for b in range(RING):
        for p in range(PARTS):
            blks = slice(p * RING, (p + 1) * RING)
            n = b * PARTS + p
            near[b, p] = copy(loc.at[1 - core, blks, span(b)], din.at[blks, span(b)], s0.at[n], v0.at[n], {"store": 1 - core})
            near[b, p].start()

    stage1 = {}
    for b in range(RING):
        for p in range(PARTS):
            with scope("w0"):
                near[b, p].wait_recv()
            if b == 0 and p == 0:
                m_own, m_par = loc[core, 0, 0:1, :], din[0, 0:1, :]
                m = jnp.maximum(m_own, m_par)
                c_own, c_par = jnp.exp(m_own - m), jnp.exp(m_par - m)
                zz = c_own * loc[core, 0, 1:2, :] + c_par * din[0, 1:2, :]
                stats = jnp.concatenate([m, zz, jnp.zeros((STAT - 2, LANES), F32)], axis=0)
            at = dims[order[p][0]][0]
            for delta in (2, 1, 3, 0):
                blk = p * RING + (at + delta) % RING
                if b == 0:
                    d[blk, 0:STAT, :] = stats
                d[blk, body(b), :] = c_own * loc[core, blk, body(b), :] + c_par * din[blk, body(b), :]
                if delta:
                    n = (b * PARTS + p) * 3 + delta - 1
                    stage1[b, p, delta] = copy(
                        d.at[blk, span(b)], r1.at[p, delta - 1, span(b)], s1.at[n], v1.at[n], peer(order[p][0], delta)
                    )
                    stage1[b, p, delta].start()

    links = {}

    def link(axis, tile):
        lt[axis] = tile
        for delta in range(1, RING):
            n = axis * 3 + delta - 1
            links[axis, delta] = copy(lt.at[axis], lr.at[axis, delta - 1], sl.at[n], vl.at[n], peer(axis, delta))
            links[axis, delta].start()

    def unlink(axis):
        for delta in range(1, RING):
            links[axis, delta].wait_recv()
        tiles = [lt[axis]] + [lr[axis, i] for i in range(3)]
        top = functools.reduce(jnp.maximum, [t[0:1] for t in tiles])
        total = sum(jnp.exp(t[0:1] - top) * t[1:2] for t in tiles)
        return jnp.concatenate([top, total, jnp.zeros((6, LANES), F32)], axis=0)

    with scope("lm"):
        head.wait()
        both = lax.dot_general(q_ref[...], w_ref[...], (((1,), (1,)), ((), ())), preferred_element_type=F32)
        mine = jnp.where(core == 0, both[:ROWS], both[ROWS:])
        logits[...] = mine
        lm_top = jnp.max(mine, axis=1, keepdims=True)
        lm_sum = jnp.sum(jnp.exp(mine - lm_top), axis=1, keepdims=True)
        lane = lax.broadcasted_iota(jnp.int32, (ROWS, LANES), 1)
        pair = jnp.where(lane == 0, lm_top, lm_sum)
        pair = jnp.concatenate([pair] * GROUPS, axis=0).T
        link(0, pair[0:8, :])

    def combine(stats):
        m = functools.reduce(jnp.maximum, [s[0:1] for s in stats])
        scales = [jnp.exp(s[0:1] - m) for s in stats]
        zz = sum(c * s[1:2] for c, s in zip(scales, stats))
        return scales, jnp.concatenate([m, zz, jnp.zeros((STAT - 2, LANES), F32)], axis=0)

    def second(p, delta, to):
        n = p * 3 + delta - 1
        return copy(e.at[p, to], r2.at[p, delta - 1], s2.at[n], v2.at[n], peer(order[p][1], delta))

    factors = {}
    for b in range(RING):
        for p in range(PARTS):
            with scope("w1"):
                for delta in range(1, RING):
                    stage1[b, p, delta].wait_recv()
            own = p * RING + dims[order[p][0]][0]
            if b == 0:
                factors[p] = combine([d[own, 0:STAT, :]] + [r1[p, i, 0:STAT, :] for i in range(3)])
            scales, stats = factors[p]
            total = scales[0] * d[own, body(b), :]
            for i in range(3):
                total = total + scales[i + 1] * r1[p, i, body(b), :]
            e[p, b, 0:STAT, :] = stats
            e[p, b, STAT:MSG2, :] = total
            here = dims[order[p][1]][0]

            @pl.when(here != b)
            def _():
                second(p, (b - here + RING) % RING, b).start()

    link(1, unlink(0))

    def third(p, delta, to):
        n = p * 3 + delta - 1
        return copy(g3.at[p, to], r3.at[p, delta - 1], s3.at[n], v3.at[n], peer(order[p][2], delta))

    for p in range(PARTS):
        own = dims[order[p][1]][0]
        with scope("w2"):
            for delta in range(1, RING):
                second(p, delta, (own + delta) % RING).wait_recv()
        scales, stats = combine([e[p, own, 0:STAT, :]] + [r2[p, i, 0:STAT, :] for i in range(3)])
        for c in range(RING):
            rows = slice(STAT + c * SLOTS, STAT + (c + 1) * SLOTS)
            total = scales[0] * e[p, own, rows, :]
            for i in range(3):
                total = total + scales[i + 1] * r2[p, i, rows, :]
            g3[p, c, 0:SLOTS, :] = total
            g3[p, c, SLOTS:MSG3, :] = stats[0 : MSG3 - SLOTS]
        here = dims[order[p][2]][0]
        for delta in (2, 1, 3):
            third(p, delta, (here + delta) % RING).start()
    link(2, unlink(1))

    tsc[...] = jnp.zeros(tsc.shape, F32)
    slots = logits.shape[1] // GROUPS
    for p in range(PARTS):
        own = dims[order[p][2]][0]
        with scope("w3"):
            for delta in range(1, RING):
                third(p, delta, (own + delta) % RING).wait_recv()
        blocks = [g3[p, own]] + [r3[p, i] for i in range(3)]
        scales, stats = combine([v[SLOTS : SLOTS + 2] for v in blocks])
        count = min(SLOTS, slots - p * SLOTS)
        total = sum(c * v[0:count] for c, v in zip(scales, blocks))
        tsc[p * SLOTS : p * SLOTS + count, :] = total / stats[1:2]
    tsc[slots : slots + 2, :] = unlink(2)[0:2]

    with scope("final"):
        turned = tsc[...].T
        for g in range(GROUPS):
            knn[:, g * slots : (g + 1) * slots] = turned[g * ROWS : (g + 1) * ROWS, 0:slots]
        lm = jnp.exp(logits[...] - turned[0:ROWS, slots : slots + 1]) / turned[0:ROWS, slots + 1 : slots + 2]
        mix = mix_ref[0, 0]
        out_ref[...] = jnp.log(mix * knn[...] + (1.0 - mix) * lm)

    for sent in list(near.values()) + list(stage1.values()) + list(links.values()):
        sent.wait_send()
    for p in range(PARTS):
        for delta in range(1, RING):
            second(p, delta, (dims[order[p][1]][0] + delta) % RING).wait_send()
            third(p, delta, (dims[order[p][2]][0] + delta) % RING).wait_send()


def solution(mesh):
    def local_step(queries, w_head, store_keys, store_tok, temperature, mix_weight):
        n_keys, width = store_keys.shape
        vocab_loc = w_head.shape[1]
        vmem, smem, hbm = (pl.BlockSpec(memory_space=s) for s in (pltpu.VMEM, pltpu.SMEM, pltpu.HBM))

        in_hbm = lambda a: pltpu.with_memory_space_constraint(a, pltpu.HBM)
        *hist, stats = pl.pallas_call(
            functools.partial(local_kernel, vocab_loc),
            out_shape=[jax.ShapeDtypeStruct((HROWS, LANES), F32)] * NBUF + [jax.ShapeDtypeStruct((2 * NBUF, 2 * LANES), F32)],
            in_specs=[smem, hbm, hbm, hbm],
            out_specs=[vmem] * (NBUF + 1),
            scratch_shapes=[
                pltpu.VMEM(queries.shape, jnp.bfloat16),
                pltpu.VMEM(store_keys.shape, jnp.bfloat16),
                pltpu.VMEM((2 * LANES, width), jnp.bfloat16),
                pltpu.VMEM((n_keys // NBUF, 2 * LANES), F32),
                pltpu.VMEM((2 * n_keys, LANES), F32),
                pltpu.VMEM((n_keys, LANES), F32),
                pltpu.VMEM((n_keys // LANES, LANES), jnp.int32),
                pltpu.SMEM((n_keys // LANES, LANES), jnp.int32),
                pltpu.VMEM((n_keys // LANES, LANES), jnp.int32),
                pltpu.SemaphoreType.DMA,
                pltpu.SemaphoreType.DMA,
                pltpu.SemaphoreType.DMA,
                pltpu.SemaphoreType.DMA((2 * NBUF,)),
            ],
            compiler_params=pltpu.CompilerParams(vmem_limit_bytes=KA_LIMIT * 2**20),
            name="histogram",
        )(temperature.reshape(1, 1), in_hbm(store_tok.reshape(n_keys // LANES, LANES)), in_hbm(queries), in_hbm(store_keys))

        return pl.pallas_call(
            comm_kernel,
            out_shape=jax.ShapeDtypeStruct((ROWS, vocab_loc), F32),
            in_specs=[smem] + [vmem] * (NBUF + 2) + [hbm],
            out_specs=vmem,
            scratch_shapes=[
                pltpu.VMEM(w_head.shape[::-1], jnp.bfloat16),
                pltpu.VMEM((ROWS, vocab_loc), F32),
                pltpu.VMEM((2, PARTS * RING, MSG, LANES), F32),
                pltpu.VMEM((PARTS * RING, MSG, LANES), F32),
                pltpu.VMEM((PARTS * RING, MSG, LANES), F32),
                pltpu.VMEM((PARTS, RING - 1, MSG, LANES), F32),
                pltpu.VMEM((PARTS, RING, MSG2, LANES), F32),
                pltpu.VMEM((PARTS, RING - 1, MSG2, LANES), F32),
                pltpu.VMEM((PARTS, RING, MSG3, LANES), F32),
                pltpu.VMEM((PARTS, RING - 1, MSG3, LANES), F32),
                pltpu.VMEM((3, STAT, LANES), F32),
                pltpu.VMEM((3, RING - 1, STAT, LANES), F32),
                pltpu.VMEM((LANES, LANES), F32),
                pltpu.VMEM((ROWS, vocab_loc), F32),
                pltpu.SemaphoreType.DMA,
                pltpu.SemaphoreType.DMA((12,)),
                pltpu.SemaphoreType.DMA((12,)),
                pltpu.SemaphoreType.DMA((36,)),
                pltpu.SemaphoreType.DMA((36,)),
            ]
            + [pltpu.SemaphoreType.DMA((9,))] * 6,
            compiler_params=pltpu.CompilerParams(collective_id=0, has_side_effects=True, vmem_limit_bytes=KB_LIMIT * 2**20),
            name="exchange",
        )(mix_weight.reshape(1, 1), *hist, stats, queries, in_hbm(w_head.T))

    return jax.shard_map(
        local_step,
        mesh=mesh,
        in_specs=(P("data", None), P(None, "model"), P(("store", "model"), None), P(("store", "model")), P(), P()),
        out_specs=P(("data", "store"), "model"),
        check_vma=False,
    )
```

```python
import functools

import jax
import jax.numpy as jnp
from jax import lax
from jax.experimental import pallas as pl
from jax.experimental.pallas import tpu as pltpu
from jax.sharding import PartitionSpec as P

F32 = jnp.float32
LANES = 128
RING = 4
CHIPS = RING**3
ROWS = 8
GROUPS = LANES // ROWS
SLOTS = 18
PARTS = 3
BLOCK = SLOTS * CHIPS // RING
BLOCK2 = BLOCK // RING
STAT = 8
MSG = STAT + BLOCK
MSG2 = STAT + BLOCK2
MSG3 = 24
NBUF = 4
KA_LIMIT = 36
KB_LIMIT = 36
HROWS = 2 * SLOTS * CHIPS * PARTS
MESH = pl.DeviceIdType.MESH
scope = jax.named_scope


def below(a, n):
    return ((a.astype(F32) + 0.5) * (1.0 / n)).astype(jnp.int32)


def local_kernel(vocab_loc, tau_ref, tok_hbm, q_hbm, k_hbm, *refs):
    hist, stats_ref = refs[:NBUF], refs[NBUF]
    q_ref, k_ref, qrep, sc, wx, grp, idx, idx_smem, tok_ref, qsem, isem, tsem, ksem = refs[NBUF + 1 :]
    n_keys = k_ref.shape[0]
    quarter = n_keys // NBUF
    chunk = quarter // 2

    def fetch(j):
        rows = pl.ds(pl.multiple_of(j * chunk, chunk), chunk)
        return pltpu.make_async_copy(k_hbm.at[rows], k_ref.at[rows], ksem.at[j])

    get_tok = pltpu.make_async_copy(tok_hbm, tok_ref, tsem)
    get_tok.start()
    get_q = pltpu.make_async_copy(q_hbm, q_ref, qsem)
    get_q.start()
    for j in range(2):
        fetch(j).start()
    span = 288
    pieces = HROWS // span // 3

    for third in range(3):

        @pl.loop(third * pieces, (third + 1) * pieces)
        def _(i):
            for buf in hist:
                buf[pl.ds(pl.multiple_of(i * span, 8), span), :] = jnp.zeros((span, LANES), F32)

        for j in range(2 + third * 2, 4 + third * 2):
            fetch(j).start()

    get_tok.wait()
    with scope("index"):
        tok = tok_ref[...]
        chip = below(tok, vocab_loc)
        within = tok - chip * vocab_loc
        slots = vocab_loc // GROUPS
        group = below(within, slots)
        slot = within - group * slots
        part = (slot >= SLOTS).astype(jnp.int32) + (slot >= 2 * SLOTS).astype(jnp.int32)
        row = slot - part * SLOTS
        x, y, z = chip & 3, (chip >> 2) & 3, chip >> 4
        first = jnp.where(part == 0, x, jnp.where(part == 1, y, z))
        second = jnp.where(part == 0, y, jnp.where(part == 1, z, x))
        third = jnp.where(part == 0, z, jnp.where(part == 1, x, y))
        place = ((part * RING + first) * RING + second) * RING + third
        idx[...] = (place * SLOTS + row) * 2
        put_idx = pltpu.make_async_copy(idx, idx_smem, isem)
        put_idx.start()
    with scope("mask"):
        group = group.astype(F32)
        square = (LANES, LANES)
        eye = lax.broadcasted_iota(jnp.int32, square, 0) == lax.broadcasted_iota(jnp.int32, square, 1)
        ones = jnp.ones(square, jnp.bfloat16)
        for c in range(n_keys // LANES):
            spread = jnp.where(eye, jnp.broadcast_to(group[c : c + 1, :], square), 0.0).astype(jnp.bfloat16)
            grp[c * LANES : (c + 1) * LANES, :] = jnp.dot(spread, ones, preferred_element_type=F32)

    with scope("turn"):
        get_q.wait()
        pick = (2 * ROWS, 2 * LANES)
        lane = lax.broadcasted_iota(jnp.int32, pick, 1)
        pick = lax.broadcasted_iota(jnp.int32, pick, 0) == (lane // LANES) * ROWS + lane % ROWS
        pick = pick.astype(F32).astype(jnp.bfloat16)
        wide = 512
        for c in range(0, q_ref.shape[1], wide):
            turned = lax.dot_general(q_ref[:, c : c + wide], pick, (((0,), (0,)), ((), ())), preferred_element_type=F32)
            qrep[c : c + wide, :] = turned.astype(jnp.bfloat16)

    inv = 1.0 / tau_ref[0, 0]
    lane_group = (lax.broadcasted_iota(jnp.int32, (LANES, LANES), 1) // ROWS).astype(F32)

    @pl.loop(0, NBUF)
    def _(b):
        with scope("kw"):
            for sub in range(2):
                fetch(b * 2 + sub).wait()
        with scope("dots"):
            keys = k_ref[pl.ds(pl.multiple_of(b * quarter, quarter), quarter), :]
            dots = jnp.dot(keys, qrep[...], preferred_element_type=F32)
            kf = keys.astype(F32)
            norms = jnp.sum(kf * kf, axis=1, keepdims=True)
            scores = (2.0 * dots - norms) * inv
            sc[...] = scores
            top = jnp.max(scores.reshape(quarter // 8, 8, 2 * LANES), axis=0)
            m = jnp.max(top, axis=0, keepdims=True)
        with scope("expand"):
            total = jnp.zeros((8, 2 * LANES), F32)
            for c in range(quarter // LANES):
                w = jnp.exp(sc[c * LANES : (c + 1) * LANES, :] - m)
                total = total + jnp.sum(w.reshape(LANES // 8, 8, 2 * LANES), axis=0)
                at = b * quarter + c * LANES
                mine = grp[pl.ds(pl.multiple_of(at, LANES), LANES), :] == lane_group
                for h in range(2):
                    wx[pl.ds(at * 2 + h, LANES, stride=2), :] = jnp.where(mine, w[:, h * LANES : (h + 1) * LANES], 0.0)
            total = jnp.sum(total, axis=0, keepdims=True)
            stats_ref[pl.ds(b, 1), :] = m
            stats_ref[pl.ds(NBUF + b, 1), :] = total

    put_idx.wait()
    unroll = 8
    rows = quarter // LANES
    with scope("scatter"):
        for c in range(rows):

            @pl.loop(0, LANES // unroll)
            def _(i):
                for u in range(unroll):
                    lane = i * unroll + u
                    at = [pl.ds(pl.multiple_of(idx_smem[b * rows + c, lane], 2), 2) for b in range(NBUF)]
                    new = [
                        hist[b][at[b], :] + wx[pl.ds(pl.multiple_of(((b * rows + c) * LANES + lane) * 2, 2), 2), :]
                        for b in range(NBUF)
                    ]
                    for b in range(NBUF):
                        hist[b][at[b], :] = new[b]


def comm_kernel(
    mix_ref, h0, h1, h2, h3, kstats, q_ref, w_hbm, out_ref,
    w_ref, logits, loc, din, d, r1, e, r2, g3, r3, lt, lr, tsc, knn,
    wsem, s0, v0, s1, v1, s2, v2, s3, v3, sl, vl,
):
    core = lax.axis_index("store")
    chip = lax.axis_index("model")
    x, y, z = chip % RING, (chip // RING) % RING, chip // (RING * RING)
    dims = ((x, 1), (y, RING), (z, RING * RING))
    order = ((0, 1, 2), (1, 2, 0), (2, 0, 1))

    def peer(axis, delta):
        at, stride = dims[axis]
        return {"model": chip + ((at + delta) % RING - at) * stride}

    barrier = pltpu.get_barrier_semaphore()
    pl.semaphore_signal(barrier, inc=1, device_id={"store": 1 - core}, device_id_type=MESH)
    for axis in range(3):
        for delta in range(1, RING):
            pl.semaphore_signal(barrier, inc=1, device_id=peer(axis, delta), device_id_type=MESH)
    head = pltpu.make_async_copy(w_hbm, w_ref, wsem)
    head.start()

    hist = (h0, h1, h2, h3)
    top = functools.reduce(jnp.maximum, [kstats[b : b + 1, :] for b in range(NBUF)])
    scales = [jnp.exp(kstats[b : b + 1, :] - top) for b in range(NBUF)]
    mass = sum(c * kstats[NBUF + b : NBUF + b + 1, :] for b, c in enumerate(scales))
    half = [slice(h * LANES, (h + 1) * LANES) for h in range(2)]

    with scope("sum"):

        @pl.loop(0, PARTS * RING)
        def _(blk):
            for h in range(2):
                loc[h, blk, 0:STAT, :] = jnp.concatenate(
                    [top[:, half[h]], mass[:, half[h]], jnp.zeros((STAT - 2, LANES), F32)], axis=0
                )
                for t in range(BLOCK // 8):
                    at = pl.ds(blk * 2 * BLOCK + t * 16 + h, 8, stride=2)
                    total = scales[0][:, half[h]] * hist[0][at, :]
                    for b in range(1, NBUF):
                        total = total + scales[b][:, half[h]] * hist[b][at, :]
                    loc[h, blk, STAT + t * 8 : STAT + t * 8 + 8, :] = total

    with scope("barrier"):
        pl.semaphore_wait(barrier, 10)

    def copy(src, dst, ssem, rsem, to):
        return pltpu.make_async_remote_copy(src_ref=src, dst_ref=dst, send_sem=ssem, recv_sem=rsem, device_id=to, device_id_type=MESH)

    def span(b):
        return slice(0, MSG2) if b == 0 else slice(STAT + b * BLOCK2, STAT + (b + 1) * BLOCK2)

    def body(b):
        return slice(STAT + b * BLOCK2, STAT + (b + 1) * BLOCK2)

    partner = {"store": 1 - core}
    first = [dims[order[p][0]][0] for p in range(PARTS)]
    mid = [dims[order[p][1]][0] for p in range(PARTS)]
    last = [dims[order[p][2]][0] for p in range(PARTS)]

    def near(b, p):
        blks = slice(p * RING, (p + 1) * RING)
        return copy(loc.at[1 - core, blks, span(b)], din.at[blks, span(b)], s0, v0.at[b * PARTS + p], partner)

    for b in range(RING):
        for p in range(PARTS):
            near(b, p).start()

    def link(axis, tile):
        lt[axis] = tile
        for delta in range(1, RING):
            copy(lt.at[axis], lr.at[axis, delta - 1], sl, vl.at[axis], peer(axis, delta)).start()

    def unlink(axis):
        copy(lr.at[axis], lr.at[axis], sl, vl.at[axis], partner).wait_recv()
        tiles = [lt[axis]] + [lr[axis, i] for i in range(3)]
        top = functools.reduce(jnp.maximum, [t[0:1] for t in tiles])
        total = sum(jnp.exp(t[0:1] - top) * t[1:2] for t in tiles)
        return jnp.concatenate([top, total, jnp.zeros((6, LANES), F32)], axis=0)

    for b in range(RING):
        for p in range(PARTS):
            with scope("w0"):
                near(b, p).wait_recv()
            if b == 0 and p == 0:
                m_own, m_par = loc[core, 0, 0:1, :], din[0, 0:1, :]
                m = jnp.maximum(m_own, m_par)
                c_own, c_par = jnp.exp(m_own - m), jnp.exp(m_par - m)
                zz = c_own * loc[core, 0, 1:2, :] + c_par * din[0, 1:2, :]
                stats = jnp.concatenate([m, zz, jnp.zeros((STAT - 2, LANES), F32)], axis=0)
            for delta in (2, 1, 3, 0):
                blk = p * RING + (first[p] + delta) % RING
                if b == 0:
                    d[blk, 0:STAT, :] = stats
                d[blk, body(b), :] = c_own * loc[core, blk, body(b), :] + c_par * din[blk, body(b), :]
                if delta:
                    to = peer(order[p][0], delta)
                    copy(d.at[blk, span(b)], r1.at[p, delta - 1, span(b)], s1, v1.at[b * PARTS + p], to).start()

        if b == 0:
            with scope("lm"):
                head.wait()
                both = lax.dot_general(q_ref[...], w_ref[...], (((1,), (1,)), ((), ())), preferred_element_type=F32)
                mine = jnp.where(core == 0, both[:ROWS], both[ROWS:])
                logits[...] = mine
                lm_top = jnp.max(mine, axis=1, keepdims=True)
                lm_sum = jnp.sum(jnp.exp(mine - lm_top), axis=1, keepdims=True)
                lane = lax.broadcasted_iota(jnp.int32, (ROWS, LANES), 1)
                pair = jnp.where(lane == 0, lm_top, lm_sum)
                pair = jnp.concatenate([pair] * GROUPS, axis=0).T
                link(0, pair[0:8, :])

    def combine(stats):
        m = functools.reduce(jnp.maximum, [s[0:1] for s in stats])
        scales = [jnp.exp(s[0:1] - m) for s in stats]
        zz = sum(c * s[1:2] for c, s in zip(scales, stats))
        return scales, jnp.concatenate([m, zz, jnp.zeros((STAT - 2, LANES), F32)], axis=0)

    factors = {}
    for b in range(RING):
        for p in range(PARTS):
            with scope("w1"):
                dst = r1.at[p, :, span(b)]
                copy(dst, dst, s1, v1.at[b * PARTS + p], partner).wait_recv()
            own = p * RING + first[p]
            if b == 0:
                factors[p] = combine([d[own, 0:STAT, :]] + [r1[p, i, 0:STAT, :] for i in range(3)])
            scales, stats = factors[p]
            total = scales[0] * d[own, body(b), :]
            for i in range(3):
                total = total + scales[i + 1] * r1[p, i, body(b), :]
            e[p, b, 0:STAT, :] = stats
            e[p, b, STAT:MSG2, :] = total

            @pl.when(mid[p] != b)
            def _():
                delta = (b - mid[p] + RING) % RING
                copy(e.at[p, b], r2.at[p, delta - 1], s2, v2.at[p], peer(order[p][1], delta)).start()

        if b == 1:
            link(1, unlink(0))
        if b == 3:
            link(2, unlink(1))

    for p in range(PARTS):
        with scope("w2"):
            copy(r2.at[p], r2.at[p], s2, v2.at[p], partner).wait_recv()
        own = mid[p]
        scales, stats = combine([e[p, own, 0:STAT, :]] + [r2[p, i, 0:STAT, :] for i in range(3)])
        for c in range(RING):
            rows = slice(STAT + c * SLOTS, STAT + (c + 1) * SLOTS)
            total = scales[0] * e[p, own, rows, :]
            for i in range(3):
                total = total + scales[i + 1] * r2[p, i, rows, :]
            g3[p, c, 0:SLOTS, :] = total
            g3[p, c, SLOTS:MSG3, :] = stats[0 : MSG3 - SLOTS]
        for delta in (2, 1, 3):
            to = (last[p] + delta) % RING
            copy(g3.at[p, to], r3.at[p, delta - 1], s3, v3.at[p], peer(order[p][2], delta)).start()

    slots = logits.shape[1] // GROUPS
    mix = mix_ref[0, 0]
    with scope("lm2"):
        tsc[...] = jnp.zeros(tsc.shape, F32)
        tsc[0:STAT, :] = unlink(2)
        turned = tsc[...].T
        lm = jnp.exp(logits[...] - turned[0:ROWS, 0:1]) / turned[0:ROWS, 1:2]
        logits[...] = (1.0 - mix) * lm
        copy(loc.at[1 - core], din, s0, v0.at[0], partner).wait_send()
        copy(r1, r1, s1, v1.at[0], partner).wait_send()
        copy(r2, r2, s2, v2.at[0], partner).wait_send()
        copy(lr, lr, sl, vl.at[0], partner).wait_send()

    for p in range(PARTS):
        with scope("w3"):
            copy(r3.at[p], r3.at[p], s3, v3.at[p], partner).wait_recv()
        blocks = [g3[p, last[p]]] + [r3[p, i] for i in range(3)]
        scales, stats = combine([v[SLOTS : SLOTS + 2] for v in blocks])
        count = min(SLOTS, slots - p * SLOTS)
        total = sum(c * v[0:count] for c, v in zip(scales, blocks))
        tsc[p * SLOTS : p * SLOTS + count, :] = total / stats[1:2]

    with scope("final"):
        turned = tsc[...].T
        for g in range(GROUPS):
            knn[:, g * slots : (g + 1) * slots] = turned[g * ROWS : (g + 1) * ROWS, 0:slots]
        out_ref[...] = jnp.log(mix * knn[...] + logits[...])

    copy(r3, r3, s3, v3.at[0], partner).wait_send()


def solution(mesh):
    def local_step(queries, w_head, store_keys, store_tok, temperature, mix_weight):
        n_keys, width = store_keys.shape
        vocab_loc = w_head.shape[1]
        vmem, smem, hbm = (pl.BlockSpec(memory_space=s) for s in (pltpu.VMEM, pltpu.SMEM, pltpu.HBM))

        in_hbm = lambda a: pltpu.with_memory_space_constraint(a, pltpu.HBM)
        *hist, stats = pl.pallas_call(
            functools.partial(local_kernel, vocab_loc),
            out_shape=[jax.ShapeDtypeStruct((HROWS, LANES), F32)] * NBUF + [jax.ShapeDtypeStruct((2 * NBUF, 2 * LANES), F32)],
            in_specs=[smem, hbm, hbm, hbm],
            out_specs=[vmem] * (NBUF + 1),
            scratch_shapes=[
                pltpu.VMEM(queries.shape, jnp.bfloat16),
                pltpu.VMEM(store_keys.shape, jnp.bfloat16),
                pltpu.VMEM((width, 2 * LANES), jnp.bfloat16),
                pltpu.VMEM((n_keys // NBUF, 2 * LANES), F32),
                pltpu.VMEM((2 * n_keys, LANES), F32),
                pltpu.VMEM((n_keys, LANES), F32),
                pltpu.VMEM((n_keys // LANES, LANES), jnp.int32),
                pltpu.SMEM((n_keys // LANES, LANES), jnp.int32),
                pltpu.VMEM((n_keys // LANES, LANES), jnp.int32),
                pltpu.SemaphoreType.DMA,
                pltpu.SemaphoreType.DMA,
                pltpu.SemaphoreType.DMA,
                pltpu.SemaphoreType.DMA((2 * NBUF,)),
            ],
            compiler_params=pltpu.CompilerParams(vmem_limit_bytes=KA_LIMIT * 2**20),
            name="histogram",
        )(temperature.reshape(1, 1), in_hbm(store_tok.reshape(n_keys // LANES, LANES)), in_hbm(queries), in_hbm(store_keys))

        return pl.pallas_call(
            comm_kernel,
            out_shape=jax.ShapeDtypeStruct((ROWS, vocab_loc), F32),
            in_specs=[smem] + [vmem] * (NBUF + 2) + [hbm],
            out_specs=vmem,
            scratch_shapes=[
                pltpu.VMEM(w_head.shape[::-1], jnp.bfloat16),
                pltpu.VMEM((ROWS, vocab_loc), F32),
                pltpu.VMEM((2, PARTS * RING, MSG, LANES), F32),
                pltpu.VMEM((PARTS * RING, MSG, LANES), F32),
                pltpu.VMEM((PARTS * RING, MSG, LANES), F32),
                pltpu.VMEM((PARTS, RING - 1, MSG, LANES), F32),
                pltpu.VMEM((PARTS, RING, MSG2, LANES), F32),
                pltpu.VMEM((PARTS, RING - 1, MSG2, LANES), F32),
                pltpu.VMEM((PARTS, RING, MSG3, LANES), F32),
                pltpu.VMEM((PARTS, RING - 1, MSG3, LANES), F32),
                pltpu.VMEM((3, STAT, LANES), F32),
                pltpu.VMEM((3, RING - 1, STAT, LANES), F32),
                pltpu.VMEM((LANES, LANES), F32),
                pltpu.VMEM((ROWS, vocab_loc), F32),
                pltpu.SemaphoreType.DMA,
                pltpu.SemaphoreType.DMA,
                pltpu.SemaphoreType.DMA((12,)),
                pltpu.SemaphoreType.DMA,
                pltpu.SemaphoreType.DMA((12,)),
            ]
            + [pltpu.SemaphoreType.DMA, pltpu.SemaphoreType.DMA((3,))] * 3,
            compiler_params=pltpu.CompilerParams(collective_id=0, has_side_effects=True, vmem_limit_bytes=KB_LIMIT * 2**20),
            name="exchange",
        )(mix_weight.reshape(1, 1), *hist, stats, queries, in_hbm(w_head.T))

    return jax.shard_map(
        local_step,
        mesh=mesh,
        in_specs=(P("data", None), P(None, "model"), P(("store", "model"), None), P(("store", "model")), P(), P()),
        out_specs=P(("data", "store"), "model"),
        check_vma=False,
    )
```

```python
import functools

import jax
import jax.numpy as jnp
from jax import lax
from jax.experimental import pallas as pl
from jax.experimental.pallas import tpu as pltpu
from jax.sharding import PartitionSpec as P

F32 = jnp.float32
LANES = 128
RING = 4
CHIPS = RING**3
ROWS = 8
GROUPS = LANES // ROWS
SLOTS = 18
PARTS = 3
BLOCK = SLOTS * CHIPS // RING
BLOCK2 = BLOCK // RING
STAT = 8
MSG = STAT + BLOCK
MSG2 = STAT + BLOCK2
MSG3 = 24
LEAD = 40
HEAVY = 40
NBUF = 4
KA_LIMIT = 36
KB_LIMIT = 36
HROWS = 2 * SLOTS * CHIPS * PARTS
MESH = pl.DeviceIdType.MESH
scope = jax.named_scope


def below(a, n):
    return ((a.astype(F32) + 0.5) * (1.0 / n)).astype(jnp.int32)


def local_kernel(vocab_loc, tau_ref, tok_hbm, q_hbm, k_hbm, *refs):
    hist, stats_ref = refs[:NBUF], refs[NBUF]
    q_ref, k_ref, qrep, sc, wx, grp, idx, idx_smem, tok_ref, qsem, isem, tsem, ksem = refs[NBUF + 1 :]
    n_keys = k_ref.shape[0]
    quarter = n_keys // NBUF
    chunk = quarter // 2

    def fetch(j):
        rows = pl.ds(pl.multiple_of(j * chunk, chunk), chunk)
        return pltpu.make_async_copy(k_hbm.at[rows], k_ref.at[rows], ksem.at[j])

    get_tok = pltpu.make_async_copy(tok_hbm, tok_ref, tsem)
    get_tok.start()
    get_q = pltpu.make_async_copy(q_hbm, q_ref, qsem)
    get_q.start()
    for j in range(2):
        fetch(j).start()
    span = 288
    pieces = HROWS // span // 3

    for third in range(3):

        @pl.loop(third * pieces, (third + 1) * pieces)
        def _(i):
            for buf in hist:
                buf[pl.ds(pl.multiple_of(i * span, 8), span), :] = jnp.zeros((span, LANES), F32)

        for j in range(2 + third * 2, 4 + third * 2):
            fetch(j).start()

    get_tok.wait()
    with scope("index"):
        tok = tok_ref[...]
        chip = below(tok, vocab_loc)
        within = tok - chip * vocab_loc
        slots = vocab_loc // GROUPS
        group = below(within, slots)
        slot = within - group * slots
        part = (slot >= SLOTS).astype(jnp.int32) + (slot >= 2 * SLOTS).astype(jnp.int32)
        row = slot - part * SLOTS
        x, y, z = chip & 3, (chip >> 2) & 3, chip >> 4
        first = jnp.where(part == 0, x, jnp.where(part == 1, y, z))
        second = jnp.where(part == 0, y, jnp.where(part == 1, z, x))
        third = jnp.where(part == 0, z, jnp.where(part == 1, x, y))
        place = ((part * RING + first) * RING + second) * RING + third
        idx[...] = (place * SLOTS + row) * 2
        put_idx = pltpu.make_async_copy(idx, idx_smem, isem)
        put_idx.start()
    with scope("mask"):
        group = group.astype(F32)
        square = (LANES, LANES)
        eye = lax.broadcasted_iota(jnp.int32, square, 0) == lax.broadcasted_iota(jnp.int32, square, 1)
        ones = jnp.ones(square, jnp.bfloat16)
        for c in range(n_keys // LANES):
            spread = jnp.where(eye, jnp.broadcast_to(group[c : c + 1, :], square), 0.0).astype(jnp.bfloat16)
            grp[c * LANES : (c + 1) * LANES, :] = jnp.dot(spread, ones, preferred_element_type=F32)

    with scope("turn"):
        get_q.wait()
        pick = (2 * ROWS, 2 * LANES)
        lane = lax.broadcasted_iota(jnp.int32, pick, 1)
        pick = lax.broadcasted_iota(jnp.int32, pick, 0) == (lane // LANES) * ROWS + lane % ROWS
        pick = pick.astype(F32).astype(jnp.bfloat16)
        wide = 512
        for c in range(0, q_ref.shape[1], wide):
            turned = lax.dot_general(q_ref[:, c : c + wide], pick, (((0,), (0,)), ((), ())), preferred_element_type=F32)
            qrep[c : c + wide, :] = turned.astype(jnp.bfloat16)

    inv = 1.0 / tau_ref[0, 0]
    lane_group = (lax.broadcasted_iota(jnp.int32, (LANES, LANES), 1) // ROWS).astype(F32)

    @pl.loop(0, NBUF)
    def _(b):
        with scope("kw"):
            for sub in range(2):
                fetch(b * 2 + sub).wait()
        with scope("dots"):
            keys = k_ref[pl.ds(pl.multiple_of(b * quarter, quarter), quarter), :]
            dots = jnp.dot(keys, qrep[...], preferred_element_type=F32)
            kf = keys.astype(F32)
            norms = jnp.sum(kf * kf, axis=1, keepdims=True)
            scores = (2.0 * dots - norms) * inv
            sc[...] = scores
            top = jnp.max(scores.reshape(quarter // 8, 8, 2 * LANES), axis=0)
            m = jnp.max(top, axis=0, keepdims=True)
        with scope("expand"):
            total = jnp.zeros((8, 2 * LANES), F32)
            for c in range(quarter // LANES):
                w = jnp.exp(sc[c * LANES : (c + 1) * LANES, :] - m)
                total = total + jnp.sum(w.reshape(LANES // 8, 8, 2 * LANES), axis=0)
                at = b * quarter + c * LANES
                mine = grp[pl.ds(pl.multiple_of(at, LANES), LANES), :] == lane_group
                for h in range(2):
                    wx[pl.ds(at * 2 + h, LANES, stride=2), :] = jnp.where(mine, w[:, h * LANES : (h + 1) * LANES], 0.0)
            total = jnp.sum(total, axis=0, keepdims=True)
            stats_ref[pl.ds(b, 1), :] = m
            stats_ref[pl.ds(NBUF + b, 1), :] = total

    put_idx.wait()
    unroll = 8
    rows = quarter // LANES
    with scope("scatter"):
        for c in range(rows):

            @pl.loop(0, LANES // unroll)
            def _(i):
                for u in range(unroll):
                    lane = i * unroll + u
                    at = [pl.ds(pl.multiple_of(idx_smem[b * rows + c, lane], 2), 2) for b in range(NBUF)]
                    new = [
                        hist[b][at[b], :] + wx[pl.ds(pl.multiple_of(((b * rows + c) * LANES + lane) * 2, 2), 2), :]
                        for b in range(NBUF)
                    ]
                    for b in range(NBUF):
                        hist[b][at[b], :] = new[b]


def comm_kernel(
    mix_ref, h0, h1, h2, h3, kstats, q_ref, w_hbm, out_ref,
    w_ref, logits, loc, din, d, ra, rb, rc, rd, e, r2, g3, r3, lt, lr, tsc, knn,
    wsem, s0, v0, s1, va, vb, vc, s2, v2, s3, v3, sl, vl,
):
    core = lax.axis_index("store")
    chip = lax.axis_index("model")
    x, y, z = chip % RING, (chip // RING) % RING, chip // (RING * RING)
    dims = ((x, 1), (y, RING), (z, RING * RING))
    order = ((0, 1, 2), (1, 2, 0), (2, 0, 1))

    def peer(axis, delta):
        at, stride = dims[axis]
        return {"model": chip + ((at + delta) % RING - at) * stride}

    barrier = pltpu.get_barrier_semaphore()
    pl.semaphore_signal(barrier, inc=1, device_id={"store": 1 - core}, device_id_type=MESH)
    for axis in range(3):
        for delta in range(1, RING):
            pl.semaphore_signal(barrier, inc=1, device_id=peer(axis, delta), device_id_type=MESH)
    head = pltpu.make_async_copy(w_hbm, w_ref, wsem)
    head.start()

    hist = (h0, h1, h2, h3)
    top = functools.reduce(jnp.maximum, [kstats[b : b + 1, :] for b in range(NBUF)])
    scales = [jnp.exp(kstats[b : b + 1, :] - top) for b in range(NBUF)]
    mass = sum(c * kstats[NBUF + b : NBUF + b + 1, :] for b, c in enumerate(scales))
    half = [slice(h * LANES, (h + 1) * LANES) for h in range(2)]

    with scope("sum"):

        @pl.loop(0, PARTS * RING)
        def _(blk):
            for h in range(2):
                loc[h, blk, LEAD : LEAD + STAT, :] = jnp.concatenate(
                    [top[:, half[h]], mass[:, half[h]], jnp.zeros((STAT - 2, LANES), F32)], axis=0
                )
                for t in range(BLOCK // 8):
                    at = pl.ds(blk * 2 * BLOCK + t * 16 + h, 8, stride=2)
                    total = scales[0][:, half[h]] * hist[0][at, :]
                    for b in range(1, NBUF):
                        total = total + scales[b][:, half[h]] * hist[b][at, :]
                    row = t * 8 if t * 8 < LEAD else t * 8 + STAT
                    loc[h, blk, row : row + 8, :] = total

    with scope("barrier"):
        pl.semaphore_wait(barrier, 10)

    def copy(src, dst, ssem, rsem, to):
        return pltpu.make_async_remote_copy(src_ref=src, dst_ref=dst, send_sem=ssem, recv_sem=rsem, device_id=to, device_id_type=MESH)

    def span(b):
        return slice(0, MSG2) if b == 0 else slice(STAT + b * BLOCK2, STAT + (b + 1) * BLOCK2)

    def piece(b, half):
        cut = HEAVY if b % 2 == 0 else BLOCK2 - HEAVY
        start = STAT + b * BLOCK2
        if b == 0:
            return slice(0, LEAD) if half == 0 else slice(LEAD + STAT, MSG2)
        return slice(start, start + cut) if half == 0 else slice(start + cut, start + BLOCK2)

    def parcel(b, half):
        if b == 0:
            return slice(0, LEAD + STAT) if half == 0 else slice(LEAD, MSG2)
        return piece(b, half)

    tile = slice(LEAD, LEAD + STAT)
    toward = (1, RING - 1)
    partner = {"store": 1 - core}
    first = [dims[order[p][0]][0] for p in range(PARTS)]
    mid = [dims[order[p][1]][0] for p in range(PARTS)]
    last = [dims[order[p][2]][0] for p in range(PARTS)]

    def place(p, delta):
        return p * RING + (first[p] + delta) % RING

    def near(p, delta):
        blk = place(p, delta)
        return copy(loc.at[1 - core, blk], din.at[blk], s0, v0.at[p * RING + delta], partner)

    for delta in (2, 1, 3, 0):
        for p in range(PARTS):
            near(p, delta).start()

    def slot_of(b, p, half):
        return (b * PARTS + p) * 2 + half

    def incoming(dst, sem, b, p, half):
        ref = dst.at[half, p, parcel(b, half)]
        copy(ref, ref, s1, sem.at[slot_of(b, p, half)], partner).wait_recv()

    def link(axis, tile):
        lt[axis] = tile
        for delta in range(1, RING):
            copy(lt.at[axis], lr.at[axis, delta - 1], sl, vl.at[axis], peer(axis, delta)).start()

    def unlink(axis):
        copy(lr.at[axis], lr.at[axis], sl, vl.at[axis], partner).wait_recv()
        tiles = [lt[axis]] + [lr[axis, i] for i in range(3)]
        top = functools.reduce(jnp.maximum, [t[0:1] for t in tiles])
        total = sum(jnp.exp(t[0:1] - top) * t[1:2] for t in tiles)
        return jnp.concatenate([top, total, jnp.zeros((6, LANES), F32)], axis=0)

    def combine(stats):
        m = functools.reduce(jnp.maximum, [s[0:1] for s in stats])
        scales = [jnp.exp(s[0:1] - m) for s in stats]
        zz = sum(c * s[1:2] for c, s in zip(scales, stats))
        return scales, jnp.concatenate([m, zz, jnp.zeros((STAT - 2, LANES), F32)], axis=0)

    chipwise = []

    def issue(delta):
        for p in range(PARTS):
            blk = place(p, delta)
            with scope("w0"):
                near(p, delta).wait_recv()
            if not chipwise:
                chipwise.append(combine([loc[core, 0, tile, :], din[blk, tile, :]]))
            (c_own, c_par), stats = chipwise[0]
            d[blk, tile, :] = stats
            for b in range(RING):
                for half in range(2):
                    rows = piece(b, half)
                    d[blk, rows, :] = c_own * loc[core, blk, rows, :] + c_par * din[blk, rows, :]
                    n, send = slot_of(b, p, half), parcel(b, half)
                    if delta == 2:
                        to = peer(order[p][0], toward[half])
                        copy(d.at[blk, send], ra.at[half, p, send], s1, va.at[n], to).start()
                    elif delta and delta != toward[half]:
                        copy(d.at[blk, send], rb.at[half, p, send], s1, vb.at[n], peer(order[p][0], delta)).start()

    joint = {}

    def relay(b):
        for p in range(PARTS):
            for half in range(2):
                with scope("wa"):
                    incoming(ra, va, b, p, half)
                blk = place(p, toward[half])
                if b == 0:
                    joint[p, half] = combine([d[blk, tile, :], ra[half, p, tile, :]])
                    rd[half, p, tile, :] = joint[p, half][1]
                c_own, c_far = joint[p, half][0]
                rows = piece(b, half)
                rd[half, p, rows, :] = c_own * d[blk, rows, :] + c_far * ra[half, p, rows, :]
                rows, sem = parcel(b, half), vc.at[slot_of(b, p, half)]
                copy(rd.at[half, p, rows], rc.at[half, p, rows], s1, sem, peer(order[p][0], toward[half])).start()

    factors = {}

    def gather(b):
        for p in range(PARTS):
            own = place(p, 0)
            row = STAT
            for half in range(2):
                with scope("w1"):
                    incoming(rb, vb, b, p, half)
                    incoming(rc, vc, b, p, half)
                if b == 0:
                    factors[p, half] = combine([d[own, tile, :], rb[half, p, tile, :], rc[half, p, tile, :]])
                c_own, c_one, c_two = factors[p, half][0]
                rows = piece(b, half)
                count = rows.stop - rows.start
                e[p, b, row : row + count, :] = (
                    c_own * d[own, rows, :] + c_one * rb[half, p, rows, :] + c_two * rc[half, p, rows, :]
                )
                row += count
            e[p, b, 0:STAT, :] = factors[p, 0][1]

            @pl.when(mid[p] != b)
            def _():
                delta = (b - mid[p] + RING) % RING
                copy(e.at[p, b], r2.at[p, delta - 1], s2, v2.at[p], peer(order[p][1], delta)).start()

    issue(2)
    with scope("lm"):
        head.wait()
        both = lax.dot_general(q_ref[...], w_ref[...], (((1,), (1,)), ((), ())), preferred_element_type=F32)
        mine = jnp.where(core == 0, both[:ROWS], both[ROWS:])
        logits[...] = mine
        lm_top = jnp.max(mine, axis=1, keepdims=True)
        lm_sum = jnp.sum(jnp.exp(mine - lm_top), axis=1, keepdims=True)
        lane = lax.broadcasted_iota(jnp.int32, (ROWS, LANES), 1)
        pair = jnp.where(lane == 0, lm_top, lm_sum)
        pair = jnp.concatenate([pair] * GROUPS, axis=0).T
        link(0, pair[0:8, :])
    for delta in (1, 3, 0):
        issue(delta)
    for b in range(RING):
        relay(b)
    link(1, unlink(0))
    for b in range(RING):
        gather(b)
    link(2, unlink(1))

    for p in range(PARTS):
        with scope("w2"):
            copy(r2.at[p], r2.at[p], s2, v2.at[p], partner).wait_recv()
        own = mid[p]
        scales, stats = combine([e[p, own, 0:STAT, :]] + [r2[p, i, 0:STAT, :] for i in range(3)])
        for c in range(RING):
            rows = slice(STAT + c * SLOTS, STAT + (c + 1) * SLOTS)
            total = scales[0] * e[p, own, rows, :]
            for i in range(3):
                total = total + scales[i + 1] * r2[p, i, rows, :]
            g3[p, c, 0:SLOTS, :] = total
            g3[p, c, SLOTS:MSG3, :] = stats[0 : MSG3 - SLOTS]
        for delta in (2, 1, 3):
            to = (last[p] + delta) % RING
            copy(g3.at[p, to], r3.at[p, delta - 1], s3, v3.at[p], peer(order[p][2], delta)).start()

    slots = logits.shape[1] // GROUPS
    mix = mix_ref[0, 0]
    with scope("lm2"):
        tsc[...] = jnp.zeros(tsc.shape, F32)
        tsc[0:STAT, :] = unlink(2)
        turned = tsc[...].T
        lm = jnp.exp(logits[...] - turned[0:ROWS, 0:1]) / turned[0:ROWS, 1:2]
        logits[...] = (1.0 - mix) * lm
        copy(loc.at[1 - core], din, s0, v0.at[0], partner).wait_send()
        for sent in (ra, rb, rc):
            ref = sent.at[:, :, 0 : STAT + BLOCK // 2]
            copy(ref, ref, s1, va.at[0], partner).wait_send()
        copy(r2, r2, s2, v2.at[0], partner).wait_send()
        copy(lr, lr, sl, vl.at[0], partner).wait_send()

    for p in range(PARTS):
        with scope("w3"):
            copy(r3.at[p], r3.at[p], s3, v3.at[p], partner).wait_recv()
        blocks = [g3[p, last[p]]] + [r3[p, i] for i in range(3)]
        scales, stats = combine([v[SLOTS : SLOTS + 2] for v in blocks])
        count = min(SLOTS, slots - p * SLOTS)
        total = sum(c * v[0:count] for c, v in zip(scales, blocks))
        tsc[p * SLOTS : p * SLOTS + count, :] = total / stats[1:2]

    with scope("final"):
        turned = tsc[...].T
        for g in range(GROUPS):
            knn[:, g * slots : (g + 1) * slots] = turned[g * ROWS : (g + 1) * ROWS, 0:slots]
        out_ref[...] = jnp.log(mix * knn[...] + logits[...])

    copy(r3, r3, s3, v3.at[0], partner).wait_send()


def solution(mesh):
    def local_step(queries, w_head, store_keys, store_tok, temperature, mix_weight):
        n_keys, width = store_keys.shape
        vocab_loc = w_head.shape[1]
        vmem, smem, hbm = (pl.BlockSpec(memory_space=s) for s in (pltpu.VMEM, pltpu.SMEM, pltpu.HBM))

        in_hbm = lambda a: pltpu.with_memory_space_constraint(a, pltpu.HBM)
        *hist, stats = pl.pallas_call(
            functools.partial(local_kernel, vocab_loc),
            out_shape=[jax.ShapeDtypeStruct((HROWS, LANES), F32)] * NBUF + [jax.ShapeDtypeStruct((2 * NBUF, 2 * LANES), F32)],
            in_specs=[smem, hbm, hbm, hbm],
            out_specs=[vmem] * (NBUF + 1),
            scratch_shapes=[
                pltpu.VMEM(queries.shape, jnp.bfloat16),
                pltpu.VMEM(store_keys.shape, jnp.bfloat16),
                pltpu.VMEM((width, 2 * LANES), jnp.bfloat16),
                pltpu.VMEM((n_keys // NBUF, 2 * LANES), F32),
                pltpu.VMEM((2 * n_keys, LANES), F32),
                pltpu.VMEM((n_keys, LANES), F32),
                pltpu.VMEM((n_keys // LANES, LANES), jnp.int32),
                pltpu.SMEM((n_keys // LANES, LANES), jnp.int32),
                pltpu.VMEM((n_keys // LANES, LANES), jnp.int32),
                pltpu.SemaphoreType.DMA,
                pltpu.SemaphoreType.DMA,
                pltpu.SemaphoreType.DMA,
                pltpu.SemaphoreType.DMA((2 * NBUF,)),
            ],
            compiler_params=pltpu.CompilerParams(vmem_limit_bytes=KA_LIMIT * 2**20),
            name="histogram",
        )(temperature.reshape(1, 1), in_hbm(store_tok.reshape(n_keys // LANES, LANES)), in_hbm(queries), in_hbm(store_keys))

        return pl.pallas_call(
            comm_kernel,
            out_shape=jax.ShapeDtypeStruct((ROWS, vocab_loc), F32),
            in_specs=[smem] + [vmem] * (NBUF + 2) + [hbm],
            out_specs=vmem,
            scratch_shapes=[
                pltpu.VMEM(w_head.shape[::-1], jnp.bfloat16),
                pltpu.VMEM((ROWS, vocab_loc), F32),
                pltpu.VMEM((2, PARTS * RING, MSG, LANES), F32),
                pltpu.VMEM((PARTS * RING, MSG, LANES), F32),
                pltpu.VMEM((PARTS * RING, MSG, LANES), F32),
                pltpu.VMEM((2, PARTS, MSG, LANES), F32),
                pltpu.VMEM((2, PARTS, MSG, LANES), F32),
                pltpu.VMEM((2, PARTS, MSG, LANES), F32),
                pltpu.VMEM((2, PARTS, MSG, LANES), F32),
                pltpu.VMEM((PARTS, RING, MSG2, LANES), F32),
                pltpu.VMEM((PARTS, RING - 1, MSG2, LANES), F32),
                pltpu.VMEM((PARTS, RING, MSG3, LANES), F32),
                pltpu.VMEM((PARTS, RING - 1, MSG3, LANES), F32),
                pltpu.VMEM((3, STAT, LANES), F32),
                pltpu.VMEM((3, RING - 1, STAT, LANES), F32),
                pltpu.VMEM((LANES, LANES), F32),
                pltpu.VMEM((ROWS, vocab_loc), F32),
                pltpu.SemaphoreType.DMA,
                pltpu.SemaphoreType.DMA,
                pltpu.SemaphoreType.DMA((12,)),
                pltpu.SemaphoreType.DMA,
                pltpu.SemaphoreType.DMA((24,)),
                pltpu.SemaphoreType.DMA((24,)),
                pltpu.SemaphoreType.DMA((24,)),
            ]
            + [pltpu.SemaphoreType.DMA, pltpu.SemaphoreType.DMA((3,))] * 3,
            compiler_params=pltpu.CompilerParams(collective_id=0, has_side_effects=True, vmem_limit_bytes=KB_LIMIT * 2**20),
            name="exchange",
        )(mix_weight.reshape(1, 1), *hist, stats, queries, in_hbm(w_head.T))

    return jax.shard_map(
        local_step,
        mesh=mesh,
        in_specs=(P("data", None), P(None, "model"), P(("store", "model"), None), P(("store", "model")), P(), P()),
        out_specs=P(("data", "store"), "model"),
        check_vma=False,
    )
```

```python
import functools

import jax
import jax.numpy as jnp
from jax import lax
from jax.experimental import pallas as pl
from jax.experimental.pallas import tpu as pltpu
from jax.sharding import PartitionSpec as P

F32 = jnp.float32
LANES = 128
RING = 4
CHIPS = RING**3
ROWS = 8
GROUPS = LANES // ROWS
SLOTS = 18
PARTS = 3
BLOCK = SLOTS * CHIPS // RING
BLOCK2 = BLOCK // RING
STAT = 8
MSG2 = STAT + BLOCK2
MSG3 = 24
NEAR = {1: 3, 3: 4, 0: 5}
LEAD = 40
NBUF = 4
KA_LIMIT = 36
KB_LIMIT = 36
HALF = SLOTS * CHIPS * PARTS + 8
HROWS = 2 * HALF
MESH = pl.DeviceIdType.MESH
scope = jax.named_scope


def below(a, n):
    return ((a.astype(F32) + 0.5) * (1.0 / n)).astype(jnp.int32)


def local_kernel(vocab_loc, tau_ref, tok_hbm, q_hbm, k_hbm, *refs):
    hist, stats_ref = refs[:NBUF], refs[NBUF]
    q_ref, k_ref, qrep, sc, wx, grp, idx, idx_smem, tok_ref, qsem, isem, tsem, ksem = refs[NBUF + 1 :]
    n_keys = k_ref.shape[0]
    quarter = n_keys // NBUF
    chunk = quarter // 2
    part_rows = 64

    def fetch(j):
        rows = pl.ds(pl.multiple_of(j * chunk, chunk), chunk)
        return pltpu.make_async_copy(k_hbm.at[rows], k_ref.at[rows], ksem.at[j])

    get_tok = pltpu.make_async_copy(tok_hbm, tok_ref, tsem)
    get_tok.start()
    get_q = pltpu.make_async_copy(q_hbm, q_ref, qsem)
    get_q.start()
    for j in range(2):
        fetch(j).start()
    span = 288
    pieces = 8

    for third in range(3):

        @pl.loop(third * pieces, (third + 1) * pieces)
        def _(i):
            for buf in hist:
                buf[pl.ds(pl.multiple_of(i * span + (i // 12) * 8, 8), span), :] = jnp.zeros((span, LANES), F32)

        for j in range(2 + third * 2, 4 + third * 2):
            fetch(j).start()

    get_tok.wait()
    with scope("index"):
        tok = tok_ref[...]
        chip = below(tok, vocab_loc)
        within = tok - chip * vocab_loc
        slots = vocab_loc // GROUPS
        group = below(within, slots)
        slot = within - group * slots
        part = (slot >= SLOTS).astype(jnp.int32) + (slot >= 2 * SLOTS).astype(jnp.int32)
        row = slot - part * SLOTS
        x, y, z = chip & 3, (chip >> 2) & 3, chip >> 4
        first = jnp.where(part == 0, x, jnp.where(part == 1, y, z))
        second = jnp.where(part == 0, y, jnp.where(part == 1, z, x))
        third = jnp.where(part == 0, z, jnp.where(part == 1, x, y))
        place = ((part * RING + first) * RING + second) * RING + third
        idx[...] = place * SLOTS + row
        put_idx = pltpu.make_async_copy(idx, idx_smem, isem)
        put_idx.start()
    with scope("mask"):
        group = group.astype(F32)
        square = (LANES, LANES)
        eye = lax.broadcasted_iota(jnp.int32, square, 0) == lax.broadcasted_iota(jnp.int32, square, 1)
        ones = jnp.ones(square, jnp.bfloat16)
        for c in range(n_keys // LANES):
            spread = jnp.where(eye, jnp.broadcast_to(group[c : c + 1, :], square), 0.0).astype(jnp.bfloat16)
            grp[c * LANES : (c + 1) * LANES, :] = jnp.dot(spread, ones, preferred_element_type=F32)

    with scope("turn"):
        get_q.wait()
        pick = (2 * ROWS, 2 * LANES)
        lane = lax.broadcasted_iota(jnp.int32, pick, 1)
        pick = lax.broadcasted_iota(jnp.int32, pick, 0) == (lane // LANES) * ROWS + lane % ROWS
        pick = pick.astype(F32).astype(jnp.bfloat16)
        wide = 512
        for c in range(0, q_ref.shape[1], wide):
            turned = lax.dot_general(q_ref[:, c : c + wide], pick, (((0,), (0,)), ((), ())), preferred_element_type=F32)
            qrep[c : c + wide, :] = turned.astype(jnp.bfloat16)

    inv = 1.0 / tau_ref[0, 0]
    lane_group = (lax.broadcasted_iota(jnp.int32, (LANES, LANES), 1) // ROWS).astype(F32)

    @pl.loop(0, NBUF)
    def _(b):
        with scope("kw"):
            for sub in range(2):
                fetch(b * 2 + sub).wait()
        with scope("dots"):
            keys = k_ref[pl.ds(pl.multiple_of(b * quarter, quarter), quarter), :]
            dots = jnp.dot(keys, qrep[...], preferred_element_type=F32)
            tops = []
            for r in range(0, quarter, part_rows):
                squares = jnp.zeros((part_rows, LANES), F32)
                for c in range(0, keys.shape[1], LANES):
                    kf = keys[r : r + part_rows, c : c + LANES].astype(F32)
                    squares = squares + kf * kf
                norms = jnp.sum(squares, axis=1, keepdims=True)
                scores = (2.0 * dots[r : r + part_rows] - norms) * inv
                sc[r : r + part_rows, :] = scores
                tops.append(jnp.max(scores.reshape(part_rows // 8, 8, 2 * LANES), axis=0))
            m = jnp.max(functools.reduce(jnp.maximum, tops), axis=0, keepdims=True)
        with scope("expand"):
            total = jnp.zeros((8, 2 * LANES), F32)
            for c in range(quarter // LANES):
                w = jnp.exp(sc[c * LANES : (c + 1) * LANES, :] - m)
                total = total + jnp.sum(w.reshape(LANES // 8, 8, 2 * LANES), axis=0)
                at = b * quarter + c * LANES
                mine = grp[pl.ds(pl.multiple_of(at, LANES), LANES), :] == lane_group
                for h in range(2):
                    wx[pl.ds(at * 2 + h, LANES, stride=2), :] = jnp.where(mine, w[:, h * LANES : (h + 1) * LANES], 0.0)
            total = jnp.sum(total, axis=0, keepdims=True)
            stats_ref[pl.ds(b, 1), :] = m
            stats_ref[pl.ds(NBUF + b, 1), :] = total

    put_idx.wait()
    unroll = 8
    rows = quarter // LANES
    with scope("scatter"):
        for c in range(rows):

            @pl.loop(0, LANES // unroll)
            def _(i):
                views = []
                for b in range(NBUF):
                    start = ((b * rows + c) * LANES + i * unroll) * 2
                    views.append(wx.at[pl.ds(pl.multiple_of(start, 2 * unroll), 2 * unroll), :])
                for u in range(unroll):
                    lane = i * unroll + u
                    at = [pl.ds(idx_smem[b * rows + c, lane], 2, stride=HALF) for b in range(NBUF)]
                    new = [hist[b][at[b], :] + views[b][2 * u : 2 * u + 2, :] for b in range(NBUF)]
                    for b in range(NBUF):
                        hist[b][at[b], :] = new[b]


def comm_kernel(
    mix_ref, h0, h1, h2, h3, kstats, q_ref, w_hbm, out_ref,
    w_ref, logits, loc, din, d, ra, rb, rc, rd, e, r2, g3, r3, lt, lr, tsc, knn,
    wsem, s0, v0, s1, va, vb, s2, v2, s3, v3, sl, vl,
):
    core = lax.axis_index("store")
    chip = lax.axis_index("model")
    x, y, z = chip % RING, (chip // RING) % RING, chip // (RING * RING)
    dims = ((x, 1), (y, RING), (z, RING * RING))
    order = ((0, 1, 2), (1, 2, 0), (2, 0, 1))

    def peer(axis, delta):
        at, stride = dims[axis]
        return {"model": chip + ((at + delta) % RING - at) * stride}

    barrier = pltpu.get_barrier_semaphore()
    pl.semaphore_signal(barrier, inc=1, device_id={"store": 1 - core}, device_id_type=MESH)
    for axis in range(3):
        for delta in range(1, RING):
            pl.semaphore_signal(barrier, inc=1, device_id=peer(axis, delta), device_id_type=MESH)
    head = pltpu.make_async_copy(w_hbm, w_ref, wsem)
    head.start()

    hist = (h0, h1, h2, h3)
    top = functools.reduce(jnp.maximum, [kstats[b : b + 1, :] for b in range(NBUF)])
    scales = [jnp.exp(kstats[b : b + 1, :] - top) for b in range(NBUF)]
    mass = sum(c * kstats[NBUF + b : NBUF + b + 1, :] for b, c in enumerate(scales))
    half = [slice(h * LANES, (h + 1) * LANES) for h in range(2)]

    with scope("sum"):

        @pl.loop(0, PARTS * RING)
        def _(blk):
            for h in range(2):
                stats = jnp.concatenate([top[:, half[h]], mass[:, half[h]], jnp.zeros((STAT - 2, LANES), F32)], axis=0)
                for b in range(RING):
                    loc[h, blk, b, LEAD : LEAD + STAT, :] = stats
                    for t in range(BLOCK2 // 8):
                        at = pl.ds(pl.multiple_of(h * HALF + blk * BLOCK + b * BLOCK2 + t * 8, 8), 8)
                        total = scales[0][:, half[h]] * hist[0][at, :]
                        for n in range(1, NBUF):
                            total = total + scales[n][:, half[h]] * hist[n][at, :]
                        row = t * 8 if t * 8 < LEAD else t * 8 + STAT
                        loc[h, blk, b, row : row + 8, :] = total

    with scope("barrier"):
        pl.semaphore_wait(barrier, 10)

    def copy(src, dst, ssem, rsem, to):
        return pltpu.make_async_remote_copy(src_ref=src, dst_ref=dst, send_sem=ssem, recv_sem=rsem, device_id=to, device_id_type=MESH)

    tile = slice(LEAD, LEAD + STAT)
    pieces = (slice(0, LEAD), slice(LEAD + STAT, MSG2))
    turn = (2, 1, 3, 0)
    toward = (1, RING - 1)

    def parcel(k, way):
        half = (way + k) % 2
        if k == 0:
            return slice(0, LEAD + STAT) if half == 0 else slice(LEAD, MSG2)
        return pieces[half]

    partner = {"store": 1 - core}
    first = [dims[order[p][0]][0] for p in range(PARTS)]
    mid = [dims[order[p][1]][0] for p in range(PARTS)]
    last = [dims[order[p][2]][0] for p in range(PARTS)]

    def place(p, delta):
        return p * RING + (first[p] + delta) % RING

    def near(p, delta):
        blk = place(p, delta)
        return copy(loc.at[1 - core, blk], din.at[blk], s0, v0.at[p if delta == 2 else NEAR[delta]], partner)

    for delta in (2, 1, 3, 0):
        for p in range(PARTS):
            near(p, delta).start()

    def arrived(ref, sem, ssem=s1):
        copy(ref, ref, ssem, sem, partner).wait_recv()

    def link(axis, tile):
        lt[axis] = tile
        for delta in range(1, RING):
            copy(lt.at[axis], lr.at[axis, delta - 1], sl, vl.at[axis], peer(axis, delta)).start()

    def unlink(axis):
        copy(lr.at[axis], lr.at[axis], sl, vl.at[axis], partner).wait_recv()
        tiles = [lt[axis]] + [lr[axis, i] for i in range(3)]
        top = functools.reduce(jnp.maximum, [t[0:1] for t in tiles])
        total = sum(jnp.exp(t[0:1] - top) * t[1:2] for t in tiles)
        return jnp.concatenate([top, total, jnp.zeros((6, LANES), F32)], axis=0)

    def combine(stats):
        m = functools.reduce(jnp.maximum, [s[0:1] for s in stats])
        scales = [jnp.exp(s[0:1] - m) for s in stats]
        zz = sum(c * s[1:2] for c, s in zip(scales, stats))
        return scales, jnp.concatenate([m, zz, jnp.zeros((STAT - 2, LANES), F32)], axis=0)

    chipwise = []

    def issue(delta):
        for p in range(PARTS):
            blk = place(p, delta)
            with scope("w0"):
                if delta == 2:
                    near(p, delta).wait_recv()
                elif p == 0:
                    arrived(din.at[0:PARTS], v0.at[NEAR[delta]], s0)
            if not chipwise:
                chipwise.append(combine([loc[core, 0, 0, tile, :], din[blk, 0, tile, :]]))
            (c_own, c_par), stats = chipwise[0]
            for k in range(RING):
                b = (mid[p] + turn[k]) % RING
                if k == 0:
                    d[p, delta, k, tile, :] = stats
                for rows in pieces:
                    d[p, delta, k, rows, :] = c_own * loc[core, blk, b, rows, :] + c_par * din[blk, b, rows, :]
                for way in range(2):
                    rows = parcel(k, way)
                    if delta == 2:
                        to = peer(order[p][0], toward[way])
                        copy(d.at[p, delta, k, rows], ra.at[way, p, k, rows], s1, va.at[k], to).start()
                    elif delta == toward[1 - way]:
                        to = peer(order[p][0], delta)
                        copy(d.at[p, delta, k, rows], rb.at[way, p, k, rows], s1, vb.at[k * PARTS + p], to).start()

    joint = {}

    def relay(k):
        with scope("wa"):
            arrived(din.at[0:11, 0, 0:24] if k == 0 else ra.at[0, :, k, 0:BLOCK2], va.at[k])
        for p in range(PARTS):
            for way in range(2):
                if k == 0:
                    joint[p, way] = combine([d[p, toward[way], k, tile, :], ra[way, p, k, tile, :]])
                    rd[way, p, k, tile, :] = joint[p, way][1]
                c_own, c_far = joint[p, way][0]
                rows = pieces[(way + k) % 2]
                rd[way, p, k, rows, :] = c_own * d[p, toward[way], k, rows, :] + c_far * ra[way, p, k, rows, :]
                rows = parcel(k, way)
                to = peer(order[p][0], toward[way])
                copy(rd.at[way, p, k, rows], rc.at[way, p, k, rows], s1, vb.at[k * PARTS + p], to).start()

    factors = {}

    def gather(k):
        for p in range(PARTS):
            with scope("w1"):
                arrived(din.at[0:11, 0, 0:16] if k == 0 else din.at[0:2, 0, 0:BLOCK2], vb.at[k * PARTS + p])
            for way in range(2):
                if k == 0:
                    factors[p, way] = combine([d[p, 0, k, tile, :], rb[way, p, k, tile, :], rc[way, p, k, tile, :]])
                c_own, c_one, c_two = factors[p, way][0]
                rows = pieces[(way + k) % 2]
                at = STAT + (rows.start if rows.start == 0 else LEAD)
                e[p, k, at : at + rows.stop - rows.start, :] = (
                    c_own * d[p, 0, k, rows, :] + c_one * rb[way, p, k, rows, :] + c_two * rc[way, p, k, rows, :]
                )
            e[p, k, 0:STAT, :] = factors[p, 0][1]
            if turn[k]:
                copy(e.at[p, k], r2.at[p, turn[k] - 1], s2, v2.at[p], peer(order[p][1], turn[k])).start()

    issue(2)
    with scope("lm"):
        head.wait()
        both = lax.dot_general(q_ref[...], w_ref[...], (((1,), (1,)), ((), ())), preferred_element_type=F32)
        mine = jnp.where(core == 0, both[:ROWS], both[ROWS:])
        logits[...] = mine
        lm_top = jnp.max(mine, axis=1, keepdims=True)
        lm_sum = jnp.sum(jnp.exp(mine - lm_top), axis=1, keepdims=True)
        lane = lax.broadcasted_iota(jnp.int32, (ROWS, LANES), 1)
        pair = jnp.where(lane == 0, lm_top, lm_sum)
        pair = jnp.concatenate([pair] * GROUPS, axis=0).T
        link(0, pair[0:8, :])
    for delta in (1, 3, 0):
        issue(delta)
    for b in range(RING):
        relay(b)
    link(1, unlink(0))
    for b in range(RING):
        gather(b)
    link(2, unlink(1))

    for p in range(PARTS):
        with scope("w2"):
            copy(r2.at[p], r2.at[p], s2, v2.at[p], partner).wait_recv()
        scales, stats = combine([e[p, 3, 0:STAT, :]] + [r2[p, i, 0:STAT, :] for i in range(3)])
        for c in range(RING):
            rows = slice(STAT + c * SLOTS, STAT + (c + 1) * SLOTS)
            total = scales[0] * e[p, 3, rows, :]
            for i in range(3):
                total = total + scales[i + 1] * r2[p, i, rows, :]
            g3[p, c, 0:SLOTS, :] = total
            g3[p, c, SLOTS:MSG3, :] = stats[0 : MSG3 - SLOTS]
        for delta in (2, 1, 3):
            to = (last[p] + delta) % RING
            copy(g3.at[p, to], r3.at[p, delta - 1], s3, v3.at[p], peer(order[p][2], delta)).start()

    slots = logits.shape[1] // GROUPS
    mix = mix_ref[0, 0]
    with scope("lm2"):
        tsc[...] = jnp.zeros(tsc.shape, F32)
        tsc[0:STAT, :] = unlink(2)
        turned = tsc[...].T
        lm = jnp.exp(logits[...] - turned[0:ROWS, 0:1]) / turned[0:ROWS, 1:2]
        logits[...] = (1.0 - mix) * lm
        copy(loc.at[1 - core], din, s0, v0.at[0], partner).wait_send()
        for sent in (ra, rb, rc):
            for ref in (din.at[0:11, 0, 0:24], sent.at[0, :, 1:RING, 0:BLOCK2]):
                copy(ref, ref, s1, va.at[0], partner).wait_send()
        copy(r2, r2, s2, v2.at[0], partner).wait_send()
        copy(lr, lr, sl, vl.at[0], partner).wait_send()

    for p in range(PARTS):
        with scope("w3"):
            copy(r3.at[p], r3.at[p], s3, v3.at[p], partner).wait_recv()
        blocks = [g3[p, last[p]]] + [r3[p, i] for i in range(3)]
        scales, stats = combine([v[SLOTS : SLOTS + 2] for v in blocks])
        count = min(SLOTS, slots - p * SLOTS)
        total = sum(c * v[0:count] for c, v in zip(scales, blocks))
        tsc[p * SLOTS : p * SLOTS + count, :] = total / stats[1:2]

    with scope("final"):
        turned = tsc[...].T
        for g in range(GROUPS):
            knn[:, g * slots : (g + 1) * slots] = turned[g * ROWS : (g + 1) * ROWS, 0:slots]
        out_ref[...] = jnp.log(mix * knn[...] + logits[...])

    copy(r3, r3, s3, v3.at[0], partner).wait_send()


def solution(mesh):
    def local_step(queries, w_head, store_keys, store_tok, temperature, mix_weight):
        n_keys, width = store_keys.shape
        vocab_loc = w_head.shape[1]
        vmem, smem, hbm = (pl.BlockSpec(memory_space=s) for s in (pltpu.VMEM, pltpu.SMEM, pltpu.HBM))

        in_hbm = lambda a: pltpu.with_memory_space_constraint(a, pltpu.HBM)
        *hist, stats = pl.pallas_call(
            functools.partial(local_kernel, vocab_loc),
            out_shape=[jax.ShapeDtypeStruct((HROWS, LANES), F32)] * NBUF + [jax.ShapeDtypeStruct((2 * NBUF, 2 * LANES), F32)],
            in_specs=[smem, hbm, hbm, hbm],
            out_specs=[vmem] * (NBUF + 1),
            scratch_shapes=[
                pltpu.VMEM(queries.shape, jnp.bfloat16),
                pltpu.VMEM(store_keys.shape, jnp.bfloat16),
                pltpu.VMEM((width, 2 * LANES), jnp.bfloat16),
                pltpu.VMEM((n_keys // NBUF, 2 * LANES), F32),
                pltpu.VMEM((2 * n_keys, LANES), F32),
                pltpu.VMEM((n_keys, LANES), F32),
                pltpu.VMEM((n_keys // LANES, LANES), jnp.int32),
                pltpu.SMEM((n_keys // LANES, LANES), jnp.int32),
                pltpu.VMEM((n_keys // LANES, LANES), jnp.int32),
                pltpu.SemaphoreType.DMA,
                pltpu.SemaphoreType.DMA,
                pltpu.SemaphoreType.DMA,
                pltpu.SemaphoreType.DMA((2 * NBUF,)),
            ],
            compiler_params=pltpu.CompilerParams(vmem_limit_bytes=KA_LIMIT * 2**20),
            name="histogram",
        )(temperature.reshape(1, 1), in_hbm(store_tok.reshape(n_keys // LANES, LANES)), in_hbm(queries), in_hbm(store_keys))

        return pl.pallas_call(
            comm_kernel,
            out_shape=jax.ShapeDtypeStruct((ROWS, vocab_loc), F32),
            in_specs=[smem] + [vmem] * (NBUF + 2) + [hbm],
            out_specs=vmem,
            scratch_shapes=[
                pltpu.VMEM(w_head.shape[::-1], jnp.bfloat16),
                pltpu.VMEM((ROWS, vocab_loc), F32),
                pltpu.VMEM((2, PARTS * RING, RING, MSG2, LANES), F32),
                pltpu.VMEM((PARTS * RING, RING, MSG2, LANES), F32),
                pltpu.VMEM((PARTS, RING, RING, MSG2, LANES), F32),
                pltpu.VMEM((2, PARTS, RING, MSG2, LANES), F32),
                pltpu.VMEM((2, PARTS, RING, MSG2, LANES), F32),
                pltpu.VMEM((2, PARTS, RING, MSG2, LANES), F32),
                pltpu.VMEM((2, PARTS, RING, MSG2, LANES), F32),
                pltpu.VMEM((PARTS, RING, MSG2, LANES), F32),
                pltpu.VMEM((PARTS, RING - 1, MSG2, LANES), F32),
                pltpu.VMEM((PARTS, RING, MSG3, LANES), F32),
                pltpu.VMEM((PARTS, RING - 1, MSG3, LANES), F32),
                pltpu.VMEM((3, STAT, LANES), F32),
                pltpu.VMEM((3, RING - 1, STAT, LANES), F32),
                pltpu.VMEM((LANES, LANES), F32),
                pltpu.VMEM((ROWS, vocab_loc), F32),
                pltpu.SemaphoreType.DMA,
                pltpu.SemaphoreType.DMA,
                pltpu.SemaphoreType.DMA((6,)),
                pltpu.SemaphoreType.DMA,
                pltpu.SemaphoreType.DMA((4,)),
                pltpu.SemaphoreType.DMA((12,)),
            ]
            + [pltpu.SemaphoreType.DMA, pltpu.SemaphoreType.DMA((3,))] * 3,
            compiler_params=pltpu.CompilerParams(collective_id=0, has_side_effects=True, vmem_limit_bytes=KB_LIMIT * 2**20),
            name="exchange",
        )(mix_weight.reshape(1, 1), *hist, stats, queries, in_hbm(w_head.T))

    return jax.shard_map(
        local_step,
        mesh=mesh,
        in_specs=(P("data", None), P(None, "model"), P(("store", "model"), None), P(("store", "model")), P(), P()),
        out_specs=P(("data", "store"), "model"),
        check_vma=False,
    )
```

```python
import functools

import jax
import jax.numpy as jnp
from jax import lax
from jax.experimental import pallas as pl
from jax.experimental.pallas import tpu as pltpu
from jax.sharding import PartitionSpec as P

F32 = jnp.float32
LANES = 128
RING = 4
CHIPS = RING**3
ROWS = 8
GROUPS = LANES // ROWS
SLOTS = 18
PARTS = 3
BLOCK = SLOTS * CHIPS // RING
BLOCK2 = BLOCK // RING
STAT = 8
MSG2 = STAT + BLOCK2
MSG3 = 24
NEAR = {1: 3, 3: 4, 0: 5}
LEAD = 40
NBUF = 4
KA_LIMIT = 36
KB_LIMIT = 36
HALF = SLOTS * CHIPS * PARTS + 8
HROWS = 2 * HALF
MESH = pl.DeviceIdType.MESH
scope = jax.named_scope


def below(a, n):
    return ((a.astype(F32) + 0.5) * (1.0 / n)).astype(jnp.int32)


def local_kernel(vocab_loc, tau_ref, tok_hbm, q_hbm, k_hbm, *refs):
    hist, stats_ref = refs[:NBUF], refs[NBUF]
    q_ref, k_ref, qrep, sc, wx, grp, idx, idx_smem, tok_ref, qsem, isem, tsem, ksem = refs[NBUF + 1 :]
    n_keys = k_ref.shape[0]
    quarter = n_keys // NBUF
    chunk = quarter // 2
    part_rows = 64

    def fetch(j):
        rows = pl.ds(pl.multiple_of(j * chunk, chunk), chunk)
        return pltpu.make_async_copy(k_hbm.at[rows], k_ref.at[rows], ksem.at[j])

    get_tok = pltpu.make_async_copy(tok_hbm, tok_ref, tsem)
    get_tok.start()
    get_q = pltpu.make_async_copy(q_hbm, q_ref, qsem)
    get_q.start()
    for j in range(2):
        fetch(j).start()
    span = 288
    pieces = 8

    for third in range(3):

        @pl.loop(third * pieces, (third + 1) * pieces)
        def _(i):
            for buf in hist:
                buf[pl.ds(pl.multiple_of(i * span + (i // 12) * 8, 8), span), :] = jnp.zeros((span, LANES), F32)

        for j in ((), (2, 3), (4, 5, 6, 7))[third]:
            fetch(j).start()

    get_tok.wait()
    with scope("index"):
        tok = tok_ref[...]
        chip = below(tok, vocab_loc)
        within = tok - chip * vocab_loc
        slots = vocab_loc // GROUPS
        group = below(within, slots)
        slot = within - group * slots
        part = (slot >= SLOTS).astype(jnp.int32) + (slot >= 2 * SLOTS).astype(jnp.int32)
        row = slot - part * SLOTS
        x, y, z = chip & 3, (chip >> 2) & 3, chip >> 4
        first = jnp.where(part == 0, x, jnp.where(part == 1, y, z))
        second = jnp.where(part == 0, y, jnp.where(part == 1, z, x))
        third = jnp.where(part == 0, z, jnp.where(part == 1, x, y))
        place = ((part * RING + first) * RING + second) * RING + third
        place = place * SLOTS + row
        idx[...] = place
        for r in range(n_keys // LANES):
            pltpu.make_async_copy(idx.at[r], idx_smem.at[pl.ds(r * LANES, LANES)], isem).start()
        lane = lax.broadcasted_iota(jnp.int32, place.shape, 1)
        again = jnp.logical_and(place == pltpu.roll(place, 1, 1), lane % 2 == 1)
    with scope("mask"):
        group = group.astype(F32) + jnp.where(again, float(GROUPS), 0.0)
        square = (LANES, LANES)
        eye = lax.broadcasted_iota(jnp.int32, square, 0) == lax.broadcasted_iota(jnp.int32, square, 1)
        ones = jnp.ones(square, jnp.bfloat16)
        for c in range(n_keys // LANES):
            spread = jnp.where(eye, jnp.broadcast_to(group[c : c + 1, :], square), 0.0).astype(jnp.bfloat16)
            grp[c * LANES : (c + 1) * LANES, :] = jnp.dot(spread, ones, preferred_element_type=F32)

    with scope("turn"):
        get_q.wait()
        for h in range(2):
            half = q_ref[h * ROWS : (h + 1) * ROWS, :].astype(F32)
            pair = jnp.concatenate([half, half], axis=0).astype(jnp.bfloat16)
            for g in range(GROUPS // 2):
                qrep[pl.ds(h * LANES + g * 2 * ROWS, 2 * ROWS), :] = pair

    inv = 1.0 / tau_ref[0, 0]
    lane_group = (lax.broadcasted_iota(jnp.int32, (LANES, LANES), 1) // ROWS).astype(F32)

    @pl.loop(0, NBUF)
    def _(b):
        with scope("kw"):
            for sub in range(2):
                fetch(b * 2 + sub).wait()
        with scope("dots"):
            keys = k_ref[pl.ds(pl.multiple_of(b * quarter, quarter), quarter), :]
            dots = lax.dot_general(keys, qrep[...], (((1,), (1,)), ((), ())), preferred_element_type=F32)
            tops = []
            for r in range(0, quarter, part_rows):
                squares = jnp.zeros((part_rows, LANES), F32)
                for c in range(0, keys.shape[1], LANES):
                    kf = keys[r : r + part_rows, c : c + LANES].astype(F32)
                    squares = squares + kf * kf
                norms = jnp.sum(squares, axis=1, keepdims=True)
                scores = (2.0 * dots[r : r + part_rows] - norms) * inv
                sc[r : r + part_rows, :] = scores
                tops.append(jnp.max(scores.reshape(part_rows // 8, 8, 2 * LANES), axis=0))
            m = jnp.max(functools.reduce(jnp.maximum, tops), axis=0, keepdims=True)
        with scope("expand"):
            total = jnp.zeros((8, 2 * LANES), F32)
            for c in range(quarter // LANES):
                w = jnp.exp(sc[c * LANES : (c + 1) * LANES, :] - m)
                total = total + jnp.sum(w.reshape(LANES // 8, 8, 2 * LANES), axis=0)
                at = b * quarter + c * LANES
                tag = grp[pl.ds(pl.multiple_of(at, LANES), LANES), :]
                repeat = tag >= GROUPS
                mine = jnp.where(repeat, tag - GROUPS, tag) == lane_group
                for h in range(2):
                    own = jnp.where(mine, w[:, h * LANES : (h + 1) * LANES], 0.0)
                    before = pltpu.roll(own.reshape(LANES // 8, 8, LANES), 1, 1).reshape(LANES, LANES)
                    wx[pl.ds(at * 2 + h, LANES, stride=2), :] = own + jnp.where(repeat, before, 0.0)
            total = jnp.sum(total, axis=0, keepdims=True)
            stats_ref[pl.ds(b, 1), :] = m
            stats_ref[pl.ds(NBUF + b, 1), :] = total

    pltpu.make_async_copy(idx, tok_ref, isem).wait()
    unroll = 8
    rows = quarter // LANES
    with scope("scatter"):
        for c in range(rows):

            @pl.loop(0, LANES // unroll)
            def _(i):
                views = []
                for b in range(NBUF):
                    start = ((b * rows + c) * LANES + i * unroll) * 2
                    views.append(wx.at[pl.ds(pl.multiple_of(start, 2 * unroll), 2 * unroll), :])
                for u in range(0, unroll, 2):
                    both = [(b, v) for b in range(NBUF) for v in (u, u + 1)]
                    at = [idx_smem[(b * rows + c) * LANES + i * unroll + v] for b, v in both]
                    at = [pl.ds(row, 2, stride=HALF) for row in at]
                    new = [hist[b][at[n], :] + views[b][2 * v : 2 * v + 2, :] for n, (b, v) in enumerate(both)]
                    for n, (b, v) in enumerate(both):
                        hist[b][at[n], :] = new[n]


def comm_kernel(
    mix_ref, h0, h1, h2, h3, kstats, q_ref, w_hbm, out_ref,
    w_ref, logits, loc, din, d, ra, rb, rc, rd, e, r2, g3, r3, lt, lr, tsc, knn,
    wsem, s0, v0, s1, va, vb, ready, s2, v2, s3, v3, sl, vl,
):
    core = lax.axis_index("store")
    chip = lax.axis_index("model")
    x, y, z = chip % RING, (chip // RING) % RING, chip // (RING * RING)
    dims = ((x, 1), (y, RING), (z, RING * RING))
    order = ((0, 1, 2), (1, 2, 0), (2, 0, 1))

    def peer(axis, delta):
        at, stride = dims[axis]
        return {"model": chip + ((at + delta) % RING - at) * stride}

    barrier = pltpu.get_barrier_semaphore()
    pl.semaphore_signal(barrier, inc=1, device_id={"store": 1 - core}, device_id_type=MESH)
    beside = [peer(axis, delta) for axis in range(3) for delta in (1, RING - 1)]
    for to in beside:
        pl.semaphore_signal(barrier, inc=1, device_id=to, device_id_type=MESH)
    head = pltpu.make_async_copy(w_hbm, w_ref, wsem)
    head.start()

    hist = (h0, h1, h2, h3)
    top = functools.reduce(jnp.maximum, [kstats[b : b + 1, :] for b in range(NBUF)])
    scales = [jnp.exp(kstats[b : b + 1, :] - top) for b in range(NBUF)]
    mass = sum(c * kstats[NBUF + b : NBUF + b + 1, :] for b, c in enumerate(scales))
    half = [slice(h * LANES, (h + 1) * LANES) for h in range(2)]

    def add_up(j):
        turn, p = j // PARTS, j % PARTS
        delta = jnp.where(turn == 0, 2, jnp.where(turn == 1, 1, jnp.where(turn == 2, 3, 0)))
        blk = p * RING + ((chip >> (2 * p)) + delta) % RING
        for h in range(2):
            stats = jnp.concatenate([top[:, half[h]], mass[:, half[h]], jnp.zeros((STAT - 2, LANES), F32)], axis=0)
            for b in range(RING):
                loc[h, blk, b, LEAD : LEAD + STAT, :] = stats
                for t in range(BLOCK2 // 8):
                    at = pl.ds(pl.multiple_of(h * HALF + blk * BLOCK + b * BLOCK2 + t * 8, 8), 8)
                    total = scales[0][:, half[h]] * hist[0][at, :]
                    for n in range(1, NBUF):
                        total = total + scales[n][:, half[h]] * hist[n][at, :]
                    row = t * 8 if t * 8 < LEAD else t * 8 + STAT
                    loc[h, blk, b, row : row + 8, :] = total

    with scope("sum"):
        pl.loop(0, PARTS)(add_up)

    with scope("barrier"):
        pl.semaphore_wait(barrier, 7)
    for to in beside:
        pl.semaphore_signal(ready, inc=1, device_id=to, device_id_type=MESH)

    def copy(src, dst, ssem, rsem, to):
        return pltpu.make_async_remote_copy(src_ref=src, dst_ref=dst, send_sem=ssem, recv_sem=rsem, device_id=to, device_id_type=MESH)

    tile = slice(LEAD, LEAD + STAT)
    pieces = (slice(0, LEAD), slice(LEAD + STAT, MSG2))
    turn = (2, 1, 3, 0)
    toward = (1, RING - 1)

    def parcel(k, way):
        half = (way + k) % 2
        if k == 0:
            return slice(0, LEAD + STAT) if half == 0 else slice(LEAD, MSG2)
        return pieces[half]

    partner = {"store": 1 - core}
    first = [dims[order[p][0]][0] for p in range(PARTS)]
    mid = [dims[order[p][1]][0] for p in range(PARTS)]
    last = [dims[order[p][2]][0] for p in range(PARTS)]

    def place(p, delta):
        return p * RING + (first[p] + delta) % RING

    def near(p, delta):
        blk = place(p, delta)
        return copy(loc.at[1 - core, blk], din.at[blk], s0, v0.at[p if delta == 2 else NEAR[delta]], partner)

    for p in range(PARTS):
        near(p, 2).start()
    with scope("sum2"):
        pl.loop(PARTS, PARTS * RING)(add_up)
    for delta in (1, 3, 0):
        for p in range(PARTS):
            near(p, delta).start()

    def arrived(ref, sem, ssem=s1):
        copy(ref, ref, ssem, sem, partner).wait_recv()

    def link(axis, tile):
        lt[axis] = tile
        for delta in range(1, RING):
            copy(lt.at[axis], lr.at[axis, delta - 1], sl, vl.at[axis], peer(axis, delta)).start()

    def unlink(axis):
        copy(lr.at[axis], lr.at[axis], sl, vl.at[axis], partner).wait_recv()
        tiles = [lt[axis]] + [lr[axis, i] for i in range(3)]
        top = functools.reduce(jnp.maximum, [t[0:1] for t in tiles])
        total = sum(jnp.exp(t[0:1] - top) * t[1:2] for t in tiles)
        return jnp.concatenate([top, total, jnp.zeros((6, LANES), F32)], axis=0)

    def combine(stats):
        m = functools.reduce(jnp.maximum, [s[0:1] for s in stats])
        scales = [jnp.exp(s[0:1] - m) for s in stats]
        zz = sum(c * s[1:2] for c, s in zip(scales, stats))
        return scales, jnp.concatenate([m, zz, jnp.zeros((STAT - 2, LANES), F32)], axis=0)

    chipwise = []

    def issue(delta):
        for p in range(PARTS):
            blk = place(p, delta)
            with scope("w0"):
                if delta == 2:
                    near(p, delta).wait_recv()
                elif p == 0:
                    arrived(din.at[0:PARTS], v0.at[NEAR[delta]], s0)
            if not chipwise:
                chipwise.append(combine([loc[core, 0, 0, tile, :], din[blk, 0, tile, :]]))
            (c_own, c_par), stats = chipwise[0]
            for k in range(RING):
                b = (mid[p] + turn[k]) % RING
                if k == 0:
                    d[p, delta, k, tile, :] = stats
                for rows in pieces:
                    d[p, delta, k, rows, :] = c_own * loc[core, blk, b, rows, :] + c_par * din[blk, b, rows, :]
                for way in range(2):
                    rows = parcel(k, way)
                    if delta == 2:
                        to = peer(order[p][0], toward[way])
                        copy(d.at[p, delta, k, rows], ra.at[way, p, k, rows], s1, va.at[k], to).start()
                    elif delta == toward[1 - way]:
                        to = peer(order[p][0], delta)
                        copy(d.at[p, delta, k, rows], rb.at[way, p, k, rows], s1, vb.at[k * PARTS + p], to).start()

    joint = {}

    def relay(k):
        with scope("wa"):
            arrived(din.at[0:11, 0, 0:24] if k == 0 else ra.at[0, :, k, 0:BLOCK2], va.at[k])
        for p in range(PARTS):
            for way in range(2):
                if k == 0:
                    joint[p, way] = combine([d[p, toward[way], k, tile, :], ra[way, p, k, tile, :]])
                    rd[way, p, k, tile, :] = joint[p, way][1]
                c_own, c_far = joint[p, way][0]
                rows = pieces[(way + k) % 2]
                rd[way, p, k, rows, :] = c_own * d[p, toward[way], k, rows, :] + c_far * ra[way, p, k, rows, :]
                rows = parcel(k, way)
                to = peer(order[p][0], toward[way])
                copy(rd.at[way, p, k, rows], rc.at[way, p, k, rows], s1, vb.at[k * PARTS + p], to).start()

    factors = {}

    def gather(k):
        for p in range(PARTS):
            with scope("w1"):
                arrived(din.at[0:11, 0, 0:16] if k == 0 else din.at[0:2, 0, 0:BLOCK2], vb.at[k * PARTS + p])
            for way in range(2):
                if k == 0:
                    factors[p, way] = combine([d[p, 0, k, tile, :], rb[way, p, k, tile, :], rc[way, p, k, tile, :]])
                c_own, c_one, c_two = factors[p, way][0]
                rows = pieces[(way + k) % 2]
                at = STAT + (rows.start if rows.start == 0 else LEAD)
                e[p, k, at : at + rows.stop - rows.start, :] = (
                    c_own * d[p, 0, k, rows, :] + c_one * rb[way, p, k, rows, :] + c_two * rc[way, p, k, rows, :]
                )
            e[p, k, 0:STAT, :] = factors[p, 0][1]
            if turn[k]:
                copy(e.at[p, k], r2.at[p, turn[k] - 1], s2, v2.at[p], peer(order[p][1], turn[k])).start()

    issue(2)
    with scope("lm"):
        head.wait()
        both = lax.dot_general(q_ref[...], w_ref[...], (((1,), (1,)), ((), ())), preferred_element_type=F32)
        mine = jnp.where(core == 0, both[:ROWS], both[ROWS:])
        logits[...] = mine
        lm_top = jnp.max(mine, axis=1, keepdims=True)
        lm_sum = jnp.sum(jnp.exp(mine - lm_top), axis=1, keepdims=True)
        lane = lax.broadcasted_iota(jnp.int32, (ROWS, LANES), 1)
        pair = jnp.where(lane == 0, lm_top, lm_sum)
        pair = jnp.concatenate([pair] * GROUPS, axis=0).T
        pl.semaphore_wait(ready, 6)
        link(0, pair[0:8, :])
    for delta in (1, 3, 0):
        issue(delta)
    for b in range(RING):
        relay(b)
    link(1, unlink(0))
    for b in range(RING):
        gather(b)
    link(2, unlink(1))

    for p in range(PARTS):
        with scope("w2"):
            copy(r2.at[p], r2.at[p], s2, v2.at[p], partner).wait_recv()
        scales, stats = combine([e[p, 3, 0:STAT, :]] + [r2[p, i, 0:STAT, :] for i in range(3)])
        for c in range(RING):
            rows = slice(STAT + c * SLOTS, STAT + (c + 1) * SLOTS)
            total = scales[0] * e[p, 3, rows, :]
            for i in range(3):
                total = total + scales[i + 1] * r2[p, i, rows, :]
            g3[p, c, 0:SLOTS, :] = total
            g3[p, c, SLOTS:MSG3, :] = stats[0 : MSG3 - SLOTS]
        for delta in (2, 1, 3):
            to = (last[p] + delta) % RING
            copy(g3.at[p, to], r3.at[p, delta - 1], s3, v3.at[p], peer(order[p][2], delta)).start()

    slots = logits.shape[1] // GROUPS
    mix = mix_ref[0, 0]
    with scope("lm2"):
        tsc[...] = jnp.zeros(tsc.shape, F32)
        tsc[0:STAT, :] = unlink(2)
        turned = tsc[...].T
        lm = jnp.exp(logits[...] - turned[0:ROWS, 0:1]) / turned[0:ROWS, 1:2]
        logits[...] = (1.0 - mix) * lm
        copy(loc.at[1 - core], din, s0, v0.at[0], partner).wait_send()
        for sent in (ra, rb, rc):
            for ref in (din.at[0:11, 0, 0:24], sent.at[0, :, 1:RING, 0:BLOCK2]):
                copy(ref, ref, s1, va.at[0], partner).wait_send()
        copy(r2, r2, s2, v2.at[0], partner).wait_send()
        copy(lr, lr, sl, vl.at[0], partner).wait_send()

    for p in range(PARTS):
        with scope("w3"):
            copy(r3.at[p], r3.at[p], s3, v3.at[p], partner).wait_recv()
        blocks = [g3[p, last[p]]] + [r3[p, i] for i in range(3)]
        scales, stats = combine([v[SLOTS : SLOTS + 2] for v in blocks])
        count = min(SLOTS, slots - p * SLOTS)
        total = sum(c * v[0:count] for c, v in zip(scales, blocks))
        tsc[p * SLOTS : p * SLOTS + count, :] = total / stats[1:2]

    with scope("final"):
        turned = tsc[...].T
        for g in range(GROUPS):
            knn[:, g * slots : (g + 1) * slots] = turned[g * ROWS : (g + 1) * ROWS, 0:slots]
        out_ref[...] = jnp.log(mix * knn[...] + logits[...])

    copy(r3, r3, s3, v3.at[0], partner).wait_send()


def solution(mesh):
    def local_step(queries, w_head, store_keys, store_tok, temperature, mix_weight):
        n_keys, width = store_keys.shape
        vocab_loc = w_head.shape[1]
        vmem, smem, hbm = (pl.BlockSpec(memory_space=s) for s in (pltpu.VMEM, pltpu.SMEM, pltpu.HBM))

        in_hbm = lambda a: pltpu.with_memory_space_constraint(a, pltpu.HBM)
        *hist, stats = pl.pallas_call(
            functools.partial(local_kernel, vocab_loc),
            out_shape=[jax.ShapeDtypeStruct((HROWS, LANES), F32)] * NBUF + [jax.ShapeDtypeStruct((2 * NBUF, 2 * LANES), F32)],
            in_specs=[smem, hbm, hbm, hbm],
            out_specs=[vmem] * (NBUF + 1),
            scratch_shapes=[
                pltpu.VMEM(queries.shape, jnp.bfloat16),
                pltpu.VMEM(store_keys.shape, jnp.bfloat16),
                pltpu.VMEM((2 * LANES, width), jnp.bfloat16),
                pltpu.VMEM((n_keys // NBUF, 2 * LANES), F32),
                pltpu.VMEM((2 * n_keys, LANES), F32),
                pltpu.VMEM((n_keys, LANES), F32),
                pltpu.VMEM((n_keys // LANES, LANES), jnp.int32),
                pltpu.SMEM((n_keys,), jnp.int32),
                pltpu.VMEM((n_keys // LANES, LANES), jnp.int32),
                pltpu.SemaphoreType.DMA,
                pltpu.SemaphoreType.DMA,
                pltpu.SemaphoreType.DMA,
                pltpu.SemaphoreType.DMA((2 * NBUF,)),
            ],
            compiler_params=pltpu.CompilerParams(vmem_limit_bytes=KA_LIMIT * 2**20),
            name="histogram",
        )(temperature.reshape(1, 1), in_hbm(store_tok.reshape(n_keys // LANES, LANES)), in_hbm(queries), in_hbm(store_keys))

        return pl.pallas_call(
            comm_kernel,
            out_shape=jax.ShapeDtypeStruct((ROWS, vocab_loc), F32),
            in_specs=[smem] + [vmem] * (NBUF + 2) + [hbm],
            out_specs=vmem,
            scratch_shapes=[
                pltpu.VMEM(w_head.shape[::-1], jnp.bfloat16),
                pltpu.VMEM((ROWS, vocab_loc), F32),
                pltpu.VMEM((2, PARTS * RING, RING, MSG2, LANES), F32),
                pltpu.VMEM((PARTS * RING, RING, MSG2, LANES), F32),
                pltpu.VMEM((PARTS, RING, RING, MSG2, LANES), F32),
                pltpu.VMEM((2, PARTS, RING, MSG2, LANES), F32),
                pltpu.VMEM((2, PARTS, RING, MSG2, LANES), F32),
                pltpu.VMEM((2, PARTS, RING, MSG2, LANES), F32),
                pltpu.VMEM((2, PARTS, RING, MSG2, LANES), F32),
                pltpu.VMEM((PARTS, RING, MSG2, LANES), F32),
                pltpu.VMEM((PARTS, RING - 1, MSG2, LANES), F32),
                pltpu.VMEM((PARTS, RING, MSG3, LANES), F32),
                pltpu.VMEM((PARTS, RING - 1, MSG3, LANES), F32),
                pltpu.VMEM((3, STAT, LANES), F32),
                pltpu.VMEM((3, RING - 1, STAT, LANES), F32),
                pltpu.VMEM((LANES, LANES), F32),
                pltpu.VMEM((ROWS, vocab_loc), F32),
                pltpu.SemaphoreType.DMA,
                pltpu.SemaphoreType.DMA,
                pltpu.SemaphoreType.DMA((6,)),
                pltpu.SemaphoreType.DMA,
                pltpu.SemaphoreType.DMA((4,)),
                pltpu.SemaphoreType.DMA((12,)),
                pltpu.SemaphoreType.REGULAR,
            ]
            + [pltpu.SemaphoreType.DMA, pltpu.SemaphoreType.DMA((3,))] * 3,
            compiler_params=pltpu.CompilerParams(collective_id=0, has_side_effects=True, vmem_limit_bytes=KB_LIMIT * 2**20),
            name="exchange",
        )(mix_weight.reshape(1, 1), *hist, stats, queries, in_hbm(w_head.T))

    return jax.shard_map(
        local_step,
        mesh=mesh,
        in_specs=(P("data", None), P(None, "model"), P(("store", "model"), None), P(("store", "model")), P(), P()),
        out_specs=P(("data", "store"), "model"),
        check_vma=False,
    )
```

```python
import functools

import jax
import jax.numpy as jnp
from jax import lax
from jax.experimental import pallas as pl
from jax.experimental.pallas import tpu as pltpu
from jax.sharding import PartitionSpec as P

F32 = jnp.float32
LANES = 128
RING = 4
CHIPS = RING**3
ROWS = 8
GROUPS = LANES // ROWS
SLOTS = 18
PARTS = 3
BLOCK = SLOTS * CHIPS // RING
BLOCK2 = BLOCK // RING
STAT = 8
MSG2 = STAT + BLOCK2
MSG3 = 24
NEAR = {1: 3, 3: 4, 0: 5}
LEAD = 40
NBUF = 4
KA_LIMIT = 36
KB_LIMIT = 36
HALF = SLOTS * CHIPS * PARTS + 8
HROWS = 2 * HALF
MESH = pl.DeviceIdType.MESH
scope = jax.named_scope


def below(a, n):
    return ((a.astype(F32) + 0.5) * (1.0 / n)).astype(jnp.int32)


def local_kernel(vocab_loc, tau_ref, tok_hbm, q_hbm, k_hbm, *refs):
    hist, stats_ref = refs[:NBUF], refs[NBUF]
    q_ref, k_ref, qrep, sc, wx, grp, idx, idx_smem, tok_ref, qsem, isem, tsem, ksem = refs[NBUF + 1 :]
    n_keys = k_ref.shape[0]
    quarter = n_keys // NBUF
    chunk = quarter // 2
    part_rows = 64

    def fetch(j):
        rows = pl.ds(pl.multiple_of(j * chunk, chunk), chunk)
        return pltpu.make_async_copy(k_hbm.at[rows], k_ref.at[rows], ksem.at[j])

    get_tok = pltpu.make_async_copy(tok_hbm, tok_ref, tsem)
    get_tok.start()
    get_q = pltpu.make_async_copy(q_hbm, q_ref, qsem)
    get_q.start()
    for j in range(2):
        fetch(j).start()
    span = 288
    pieces = 8

    for third in range(3):

        @pl.loop(third * pieces, (third + 1) * pieces)
        def _(i):
            for buf in hist:
                buf[pl.ds(pl.multiple_of(i * span + (i // 12) * 8, 8), span), :] = jnp.zeros((span, LANES), F32)

        for j in ((), (2, 3), (4, 5, 6, 7))[third]:
            fetch(j).start()

    get_tok.wait()
    with scope("index"):
        tok = tok_ref[...]
        chip = below(tok, vocab_loc)
        within = tok - chip * vocab_loc
        slots = vocab_loc // GROUPS
        group = below(within, slots)
        slot = within - group * slots
        part = (slot >= SLOTS).astype(jnp.int32) + (slot >= 2 * SLOTS).astype(jnp.int32)
        row = slot - part * SLOTS
        x, y, z = chip & 3, (chip >> 2) & 3, chip >> 4
        first = jnp.where(part == 0, x, jnp.where(part == 1, y, z))
        second = jnp.where(part == 0, y, jnp.where(part == 1, z, x))
        third = jnp.where(part == 0, z, jnp.where(part == 1, x, y))
        place = ((part * RING + first) * RING + second) * RING + third
        place = place * SLOTS + row
        idx[...] = place
        for r in range(n_keys // LANES):
            pltpu.make_async_copy(idx.at[r], idx_smem.at[pl.ds(r * LANES, LANES)], isem).start()
        lane = lax.broadcasted_iota(jnp.int32, place.shape, 1)
        again = jnp.logical_and(place == pltpu.roll(place, 1, 1), lane % 2 == 1)
    with scope("mask"):
        group = group.astype(F32) + jnp.where(again, float(GROUPS), 0.0)
        square = (LANES, LANES)
        eye = lax.broadcasted_iota(jnp.int32, square, 0) == lax.broadcasted_iota(jnp.int32, square, 1)
        ones = jnp.ones(square, jnp.bfloat16)
        for c in range(n_keys // LANES):
            spread = jnp.where(eye, jnp.broadcast_to(group[c : c + 1, :], square), 0.0).astype(jnp.bfloat16)
            grp[c * LANES : (c + 1) * LANES, :] = jnp.dot(spread, ones, preferred_element_type=F32)

    with scope("turn"):
        get_q.wait()
        for h in range(2):
            half = q_ref[h * ROWS : (h + 1) * ROWS, :].astype(F32)
            pair = jnp.concatenate([half, half], axis=0).astype(jnp.bfloat16)
            for g in range(GROUPS // 2):
                qrep[pl.ds(h * LANES + g * 2 * ROWS, 2 * ROWS), :] = pair

    inv = 1.0 / tau_ref[0, 0]
    lane_group = (lax.broadcasted_iota(jnp.int32, (LANES, LANES), 1) // ROWS).astype(F32)

    @pl.loop(0, NBUF)
    def _(b):
        with scope("kw"):
            for sub in range(2):
                fetch(b * 2 + sub).wait()
        with scope("dots"):
            keys = k_ref[pl.ds(pl.multiple_of(b * quarter, quarter), quarter), :]
            dots = lax.dot_general(keys, qrep[...], (((1,), (1,)), ((), ())), preferred_element_type=F32)
            tops = []
            for r in range(0, quarter, part_rows):
                squares = jnp.zeros((part_rows, LANES), F32)
                for c in range(0, keys.shape[1], LANES):
                    kf = keys[r : r + part_rows, c : c + LANES].astype(F32)
                    squares = squares + kf * kf
                norms = jnp.sum(squares, axis=1, keepdims=True)
                scores = (2.0 * dots[r : r + part_rows] - norms) * inv
                sc[r : r + part_rows, :] = scores
                tops.append(jnp.max(scores.reshape(part_rows // 8, 8, 2 * LANES), axis=0))
            m = jnp.max(functools.reduce(jnp.maximum, tops), axis=0, keepdims=True)
        with scope("expand"):
            total = jnp.zeros((8, 2 * LANES), F32)
            for c in range(quarter // LANES):
                w = jnp.exp(sc[c * LANES : (c + 1) * LANES, :] - m)
                total = total + jnp.sum(w.reshape(LANES // 8, 8, 2 * LANES), axis=0)
                at = b * quarter + c * LANES
                tag = grp[pl.ds(pl.multiple_of(at, LANES), LANES), :]
                repeat = tag >= GROUPS
                mine = jnp.where(repeat, tag - GROUPS, tag) == lane_group
                for h in range(2):
                    own = jnp.where(mine, w[:, h * LANES : (h + 1) * LANES], 0.0)
                    before = pltpu.roll(own.reshape(LANES // 8, 8, LANES), 1, 1).reshape(LANES, LANES)
                    wx[pl.ds(at * 2 + h, LANES, stride=2), :] = own + jnp.where(repeat, before, 0.0)
            total = jnp.sum(total, axis=0, keepdims=True)
            stats_ref[pl.ds(b, 1), :] = m
            stats_ref[pl.ds(NBUF + b, 1), :] = total

    pltpu.make_async_copy(idx, tok_ref, isem).wait()
    unroll = 8
    rows = quarter // LANES
    with scope("scatter"):
        for c in range(rows):

            @pl.loop(0, LANES // unroll)
            def _(i):
                views = []
                for b in range(NBUF):
                    start = ((b * rows + c) * LANES + i * unroll) * 2
                    views.append(wx.at[pl.ds(pl.multiple_of(start, 2 * unroll), 2 * unroll), :])
                for u in range(0, unroll, 2):
                    both = [(b, v) for b in range(NBUF) for v in (u, u + 1)]
                    at = [idx_smem[(b * rows + c) * LANES + i * unroll + v] for b, v in both]
                    at = [pl.ds(row, 2, stride=HALF) for row in at]
                    new = [hist[b][at[n], :] + views[b][2 * v : 2 * v + 2, :] for n, (b, v) in enumerate(both)]
                    for n, (b, v) in enumerate(both):
                        hist[b][at[n], :] = new[n]


def comm_kernel(
    mix_ref, h0, h1, h2, h3, kstats, q_ref, w_hbm, out_ref,
    w_ref, logits, loc, din, d, ra, rb, rc, rd, e, r2, g3, r3, lt, lr, tsc, knn,
    wsem, s0, v0, s1, va, vb, ready, pal, s2, v2, s3, v3, sl, vl,
):
    core = lax.axis_index("store")
    chip = lax.axis_index("model")
    x, y, z = chip % RING, (chip // RING) % RING, chip // (RING * RING)
    dims = ((x, 1), (y, RING), (z, RING * RING))
    order = ((0, 1, 2), (1, 2, 0), (2, 0, 1))

    def peer(axis, delta):
        at, stride = dims[axis]
        return {"model": chip + ((at + delta) % RING - at) * stride}

    barrier = pltpu.get_barrier_semaphore()
    beside = [peer(axis, delta) for axis in range(3) for delta in (1, RING - 1)]
    for to in beside:
        pl.semaphore_signal(barrier, inc=1, device_id={**to, "store": 1}, device_id_type=MESH)

    @pl.when(core == 1)
    def _():
        pl.semaphore_signal(barrier, inc=1, device_id={"store": 0}, device_id_type=MESH)

    head = pltpu.make_async_copy(w_hbm, w_ref, wsem)
    head.start()

    @pl.when(core == 0)
    def _():
        pl.semaphore_wait(barrier, 1)
        pl.semaphore_signal(pal, inc=1, device_id={"store": 1}, device_id_type=MESH)

    hist = (h0, h1, h2, h3)
    top = functools.reduce(jnp.maximum, [kstats[b : b + 1, :] for b in range(NBUF)])
    scales = [jnp.exp(kstats[b : b + 1, :] - top) for b in range(NBUF)]
    mass = sum(c * kstats[NBUF + b : NBUF + b + 1, :] for b, c in enumerate(scales))
    half = [slice(h * LANES, (h + 1) * LANES) for h in range(2)]

    def add_up(j):
        turn, p = j // PARTS, j % PARTS
        delta = jnp.where(turn == 0, 2, jnp.where(turn == 1, 1, jnp.where(turn == 2, 3, 0)))
        blk = p * RING + ((chip >> (2 * p)) + delta) % RING
        for h in range(2):
            stats = jnp.concatenate([top[:, half[h]], mass[:, half[h]], jnp.zeros((STAT - 2, LANES), F32)], axis=0)
            for b in range(RING):
                loc[h, blk, b, LEAD : LEAD + STAT, :] = stats
                for t in range(BLOCK2 // 8):
                    at = pl.ds(pl.multiple_of(h * HALF + blk * BLOCK + b * BLOCK2 + t * 8, 8), 8)
                    total = scales[0][:, half[h]] * hist[0][at, :]
                    for n in range(1, NBUF):
                        total = total + scales[n][:, half[h]] * hist[n][at, :]
                    row = t * 8 if t * 8 < LEAD else t * 8 + STAT
                    loc[h, blk, b, row : row + 8, :] = total

    with scope("sum"):
        pl.loop(0, PARTS)(add_up)

    @pl.when(core == 1)
    def _():
        pl.semaphore_wait(pal, 1)

    def copy(src, dst, ssem, rsem, to):
        return pltpu.make_async_remote_copy(src_ref=src, dst_ref=dst, send_sem=ssem, recv_sem=rsem, device_id=to, device_id_type=MESH)

    tile = slice(LEAD, LEAD + STAT)
    pieces = (slice(0, LEAD), slice(LEAD + STAT, MSG2))
    turn = (2, 1, 3, 0)
    toward = (1, RING - 1)

    def parcel(k, way):
        half = (way + k) % 2
        if k == 0:
            return slice(0, LEAD + STAT) if half == 0 else slice(LEAD, MSG2)
        return pieces[half]

    partner = {"store": 1 - core}

    def across(axis, delta):
        return {**peer(axis, delta), "store": 1 - core} if delta else partner

    first = [dims[order[p][0]][0] for p in range(PARTS)]
    mid = [dims[order[p][1]][0] for p in range(PARTS)]
    last = [dims[order[p][2]][0] for p in range(PARTS)]

    def place(p, delta):
        return p * RING + (first[p] + delta) % RING

    def near(p, delta):
        blk = place(p, delta)
        return copy(loc.at[1 - core, blk], din.at[blk], s0, v0.at[p if delta == 2 else NEAR[delta]], partner)

    for p in range(PARTS):
        near(p, 2).start()
    with scope("sum2"):
        pl.loop(PARTS, PARTS * RING)(add_up)
    for delta in (1, 3, 0):
        for p in range(PARTS):
            near(p, delta).start()

    with scope("barrier"):

        @pl.when(core == 1)
        def _():
            pl.semaphore_wait(barrier, 12)
            pl.semaphore_signal(pal, inc=1, device_id={"store": 0}, device_id_type=MESH)

        @pl.when(core == 0)
        def _():
            pl.semaphore_wait(pal, 1)

    for to in beside:
        pl.semaphore_signal(ready, inc=1, device_id=to, device_id_type=MESH)

    def arrived(ref, sem, ssem=s1):
        copy(ref, ref, ssem, sem, partner).wait_recv()

    def link(axis, tile):
        lt[axis] = tile
        for delta in range(1, RING):
            copy(lt.at[axis], lr.at[axis, delta - 1], sl, vl.at[axis], peer(axis, delta)).start()

    def unlink(axis):
        copy(lr.at[axis], lr.at[axis], sl, vl.at[axis], partner).wait_recv()
        tiles = [lt[axis]] + [lr[axis, i] for i in range(3)]
        top = functools.reduce(jnp.maximum, [t[0:1] for t in tiles])
        total = sum(jnp.exp(t[0:1] - top) * t[1:2] for t in tiles)
        return jnp.concatenate([top, total, jnp.zeros((6, LANES), F32)], axis=0)

    def combine(stats):
        m = functools.reduce(jnp.maximum, [s[0:1] for s in stats])
        scales = [jnp.exp(s[0:1] - m) for s in stats]
        zz = sum(c * s[1:2] for c, s in zip(scales, stats))
        return scales, jnp.concatenate([m, zz, jnp.zeros((STAT - 2, LANES), F32)], axis=0)

    chipwise = []

    def issue(delta):
        for p in range(PARTS):
            blk = place(p, delta)
            with scope("w0"):
                if delta == 2:
                    near(p, delta).wait_recv()
                elif p == 0:
                    arrived(din.at[0:PARTS], v0.at[NEAR[delta]], s0)
            if not chipwise:
                chipwise.append(combine([loc[core, 0, 0, tile, :], din[blk, 0, tile, :]]))
            (c_own, c_par), stats = chipwise[0]
            for k in range(RING):
                b = (mid[p] + turn[k]) % RING
                if k == 0:
                    d[p, delta, k, tile, :] = stats
                for rows in pieces:
                    d[p, delta, k, rows, :] = c_own * loc[core, blk, b, rows, :] + c_par * din[blk, b, rows, :]
                for way in range(2):
                    rows = parcel(k, way)
                    if delta == 2:
                        to = peer(order[p][0], toward[way])
                        copy(d.at[p, delta, k, rows], ra.at[way, p, k, rows], s1, va.at[k], to).start()
                    elif delta == toward[1 - way]:
                        to = peer(order[p][0], delta)
                        copy(d.at[p, delta, k, rows], rb.at[way, p, k, rows], s1, vb.at[k * PARTS + p], to).start()

    joint = {}

    def relay(k):
        with scope("wa"):
            arrived(din.at[0:11, 0, 0:24] if k == 0 else ra.at[0, :, k, 0:BLOCK2], va.at[k])
        for p in range(PARTS):
            for way in range(2):
                if k == 0:
                    joint[p, way] = combine([d[p, toward[way], k, tile, :], ra[way, p, k, tile, :]])
                    rd[way, p, k, tile, :] = joint[p, way][1]
                c_own, c_far = joint[p, way][0]
                rows = pieces[(way + k) % 2]
                rd[way, p, k, rows, :] = c_own * d[p, toward[way], k, rows, :] + c_far * ra[way, p, k, rows, :]
                rows = parcel(k, way)
                to = peer(order[p][0], toward[way])
                copy(rd.at[way, p, k, rows], rc.at[way, p, k, rows], s1, vb.at[k * PARTS + p], to).start()

    factors = {}

    def gather(k):
        for p in range(PARTS):
            with scope("w1"):
                arrived(din.at[0:11, 0, 0:16] if k == 0 else din.at[0:2, 0, 0:BLOCK2], vb.at[k * PARTS + p])
            for way in range(2):
                if k == 0:
                    factors[p, way] = combine([d[p, 0, k, tile, :], rb[way, p, k, tile, :], rc[way, p, k, tile, :]])
                c_own, c_one, c_two = factors[p, way][0]
                rows = pieces[(way + k) % 2]
                at = STAT + (rows.start if rows.start == 0 else LEAD)
                e[p, k, at : at + rows.stop - rows.start, :] = (
                    c_own * d[p, 0, k, rows, :] + c_one * rb[way, p, k, rows, :] + c_two * rc[way, p, k, rows, :]
                )
            e[p, k, 0:STAT, :] = factors[p, 0][1]
            to = across(order[p][1], turn[k])
            copy(e.at[p, k], r2.at[p, turn[k]], s2, v2.at[p], to).start()

    issue(2)
    with scope("lm"):
        head.wait()
        both = lax.dot_general(q_ref[...], w_ref[...], (((1,), (1,)), ((), ())), preferred_element_type=F32)
        mine = jnp.where(core == 0, both[:ROWS], both[ROWS:])
        logits[...] = mine
        lm_top = jnp.max(mine, axis=1, keepdims=True)
        lm_sum = jnp.sum(jnp.exp(mine - lm_top), axis=1, keepdims=True)
        lane = lax.broadcasted_iota(jnp.int32, (ROWS, LANES), 1)
        pair = jnp.where(lane == 0, lm_top, lm_sum)
        pair = jnp.concatenate([pair] * GROUPS, axis=0).T
        pl.semaphore_wait(ready, 6)
        link(0, pair[0:8, :])
    for delta in (1, 3, 0):
        issue(delta)
    for b in range(RING):
        relay(b)
    link(1, unlink(0))
    for b in range(RING):
        gather(b)
    link(2, unlink(1))

    for p in range(PARTS):
        with scope("w2"):
            copy(r2.at[p], r2.at[p], s2, v2.at[p], partner).wait_recv()
        scales, stats = combine([r2[p, i, 0:STAT, :] for i in range(RING)])
        for c in range(RING):
            rows = slice(STAT + c * SLOTS, STAT + (c + 1) * SLOTS)
            total = scales[0] * r2[p, 0, rows, :]
            for i in range(1, RING):
                total = total + scales[i] * r2[p, i, rows, :]
            g3[p, c, 0:SLOTS, :] = total
            g3[p, c, SLOTS:MSG3, :] = stats[0 : MSG3 - SLOTS]
        for delta in (2, 1, 3, 0):
            to = (last[p] + delta) % RING
            copy(g3.at[p, to], r3.at[p, delta], s3, v3.at[p], across(order[p][2], delta)).start()

    slots = logits.shape[1] // GROUPS
    mix = mix_ref[0, 0]
    with scope("lm2"):
        tsc[...] = jnp.zeros(tsc.shape, F32)
        tsc[0:STAT, :] = unlink(2)
        turned = tsc[...].T
        lm = jnp.exp(logits[...] - turned[0:ROWS, 0:1]) / turned[0:ROWS, 1:2]
        logits[...] = (1.0 - mix) * lm
        copy(loc.at[1 - core], din, s0, v0.at[0], partner).wait_send()
        for sent in (ra, rb, rc):
            for ref in (din.at[0:11, 0, 0:24], sent.at[0, :, 1:RING, 0:BLOCK2]):
                copy(ref, ref, s1, va.at[0], partner).wait_send()
        copy(r2, r2, s2, v2.at[0], partner).wait_send()
        copy(lr, lr, sl, vl.at[0], partner).wait_send()

    for p in range(PARTS):
        with scope("w3"):
            copy(r3.at[p], r3.at[p], s3, v3.at[p], partner).wait_recv()
        blocks = [r3[p, i] for i in range(RING)]
        scales, stats = combine([v[SLOTS : SLOTS + 2] for v in blocks])
        count = min(SLOTS, slots - p * SLOTS)
        total = sum(c * v[0:count] for c, v in zip(scales, blocks))
        tsc[p * SLOTS : p * SLOTS + count, :] = total / stats[1:2]

    with scope("final"):
        turned = tsc[...].T
        for g in range(GROUPS):
            knn[:, g * slots : (g + 1) * slots] = turned[g * ROWS : (g + 1) * ROWS, 0:slots]
        out_ref[...] = jnp.log(mix * knn[...] + logits[...])

    copy(r3, r3, s3, v3.at[0], partner).wait_send()


def solution(mesh):
    def local_step(queries, w_head, store_keys, store_tok, temperature, mix_weight):
        n_keys, width = store_keys.shape
        vocab_loc = w_head.shape[1]
        vmem, smem, hbm = (pl.BlockSpec(memory_space=s) for s in (pltpu.VMEM, pltpu.SMEM, pltpu.HBM))

        in_hbm = lambda a: pltpu.with_memory_space_constraint(a, pltpu.HBM)
        *hist, stats = pl.pallas_call(
            functools.partial(local_kernel, vocab_loc),
            out_shape=[jax.ShapeDtypeStruct((HROWS, LANES), F32)] * NBUF + [jax.ShapeDtypeStruct((2 * NBUF, 2 * LANES), F32)],
            in_specs=[smem, hbm, hbm, hbm],
            out_specs=[vmem] * (NBUF + 1),
            scratch_shapes=[
                pltpu.VMEM(queries.shape, jnp.bfloat16),
                pltpu.VMEM(store_keys.shape, jnp.bfloat16),
                pltpu.VMEM((2 * LANES, width), jnp.bfloat16),
                pltpu.VMEM((n_keys // NBUF, 2 * LANES), F32),
                pltpu.VMEM((2 * n_keys, LANES), F32),
                pltpu.VMEM((n_keys, LANES), F32),
                pltpu.VMEM((n_keys // LANES, LANES), jnp.int32),
                pltpu.SMEM((n_keys,), jnp.int32),
                pltpu.VMEM((n_keys // LANES, LANES), jnp.int32),
                pltpu.SemaphoreType.DMA,
                pltpu.SemaphoreType.DMA,
                pltpu.SemaphoreType.DMA,
                pltpu.SemaphoreType.DMA((2 * NBUF,)),
            ],
            compiler_params=pltpu.CompilerParams(vmem_limit_bytes=KA_LIMIT * 2**20),
            name="histogram",
        )(temperature.reshape(1, 1), in_hbm(store_tok.reshape(n_keys // LANES, LANES)), in_hbm(queries), in_hbm(store_keys))

        return pl.pallas_call(
            comm_kernel,
            out_shape=jax.ShapeDtypeStruct((ROWS, vocab_loc), F32),
            in_specs=[smem] + [vmem] * (NBUF + 2) + [hbm],
            out_specs=vmem,
            scratch_shapes=[
                pltpu.VMEM(w_head.shape[::-1], jnp.bfloat16),
                pltpu.VMEM((ROWS, vocab_loc), F32),
                pltpu.VMEM((2, PARTS * RING, RING, MSG2, LANES), F32),
                pltpu.VMEM((PARTS * RING, RING, MSG2, LANES), F32),
                pltpu.VMEM((PARTS, RING, RING, MSG2, LANES), F32),
                pltpu.VMEM((2, PARTS, RING, MSG2, LANES), F32),
                pltpu.VMEM((2, PARTS, RING, MSG2, LANES), F32),
                pltpu.VMEM((2, PARTS, RING, MSG2, LANES), F32),
                pltpu.VMEM((2, PARTS, RING, MSG2, LANES), F32),
                pltpu.VMEM((PARTS, RING, MSG2, LANES), F32),
                pltpu.VMEM((PARTS, RING, MSG2, LANES), F32),
                pltpu.VMEM((PARTS, RING, MSG3, LANES), F32),
                pltpu.VMEM((PARTS, RING, MSG3, LANES), F32),
                pltpu.VMEM((3, STAT, LANES), F32),
                pltpu.VMEM((3, RING - 1, STAT, LANES), F32),
                pltpu.VMEM((LANES, LANES), F32),
                pltpu.VMEM((ROWS, vocab_loc), F32),
                pltpu.SemaphoreType.DMA,
                pltpu.SemaphoreType.DMA,
                pltpu.SemaphoreType.DMA((6,)),
                pltpu.SemaphoreType.DMA,
                pltpu.SemaphoreType.DMA((4,)),
                pltpu.SemaphoreType.DMA((12,)),
                pltpu.SemaphoreType.REGULAR,
                pltpu.SemaphoreType.REGULAR,
            ]
            + [pltpu.SemaphoreType.DMA, pltpu.SemaphoreType.DMA((3,))] * 3,
            compiler_params=pltpu.CompilerParams(collective_id=0, has_side_effects=True, vmem_limit_bytes=KB_LIMIT * 2**20),
            name="exchange",
        )(mix_weight.reshape(1, 1), *hist, stats, queries, in_hbm(w_head.T))

    return jax.shard_map(
        local_step,
        mesh=mesh,
        in_specs=(P("data", None), P(None, "model"), P(("store", "model"), None), P(("store", "model")), P(), P()),
        out_specs=P(("data", "store"), "model"),
        check_vma=False,
    )
```

```python
import functools

import jax
import jax.numpy as jnp
from jax import lax
from jax.experimental import pallas as pl
from jax.experimental.pallas import tpu as pltpu
from jax.sharding import PartitionSpec as P

F32 = jnp.float32
LANES = 128
RING = 4
CHIPS = RING**3
ROWS = 8
GROUPS = LANES // ROWS
SLOTS = 18
PARTS = 3
BLOCK = SLOTS * CHIPS // RING
BLOCK2 = BLOCK // RING
STAT = 8
MSG2 = STAT + BLOCK2
MSG3 = 24
NEAR = {1: 3, 3: 4, 0: 5}
LEAD = 40
NBUF = 4
KA_LIMIT = 36
KB_LIMIT = 36
HALF = SLOTS * CHIPS * PARTS + 8
HROWS = 2 * HALF
MESH = pl.DeviceIdType.MESH
scope = jax.named_scope


def below(a, n):
    return ((a.astype(F32) + 0.5) * (1.0 / n)).astype(jnp.int32)


def local_kernel(vocab_loc, tau_ref, tok_hbm, q_hbm, k_hbm, *refs):
    hist, stats_ref = refs[:NBUF], refs[NBUF]
    q_ref, k_ref, qrep, sc, wx, grp, idx, idx_smem, tok_ref, qsem, isem, tsem, ksem = refs[NBUF + 1 :]
    n_keys = k_ref.shape[0]
    quarter = n_keys // NBUF
    chunk = quarter // 2
    part_rows = 128

    def fetch(j):
        rows = pl.ds(pl.multiple_of(j * chunk, chunk), chunk)
        return pltpu.make_async_copy(k_hbm.at[rows], k_ref.at[rows], ksem.at[j])

    get_tok = pltpu.make_async_copy(tok_hbm, tok_ref, tsem)
    get_tok.start()
    get_q = pltpu.make_async_copy(q_hbm, q_ref, qsem)
    get_q.start()
    for j in range(2):
        fetch(j).start()
    span = 288
    pieces = 8

    for third in range(3):

        @pl.loop(third * pieces, (third + 1) * pieces)
        def _(i):
            for buf in hist:
                buf[pl.ds(pl.multiple_of(i * span + (i // 12) * 8, 8), span), :] = jnp.zeros((span, LANES), F32)

        for j in ((), (2, 3), (4, 5, 6, 7))[third]:
            fetch(j).start()

    get_tok.wait()
    with scope("index"):
        tok = tok_ref[...]
        chip = below(tok, vocab_loc)
        within = tok - chip * vocab_loc
        slots = vocab_loc // GROUPS
        group = below(within, slots)
        slot = within - group * slots
        part = (slot >= SLOTS).astype(jnp.int32) + (slot >= 2 * SLOTS).astype(jnp.int32)
        row = slot - part * SLOTS
        x, y, z = chip & 3, (chip >> 2) & 3, chip >> 4
        first = jnp.where(part == 0, x, jnp.where(part == 1, y, z))
        second = jnp.where(part == 0, y, jnp.where(part == 1, z, x))
        third = jnp.where(part == 0, z, jnp.where(part == 1, x, y))
        place = ((part * RING + first) * RING + second) * RING + third
        place = place * SLOTS + row
        idx[...] = place
        for r in range(n_keys // LANES):
            pltpu.make_async_copy(idx.at[r], idx_smem.at[pl.ds(r * LANES, LANES)], isem).start()
        lane = lax.broadcasted_iota(jnp.int32, place.shape, 1)
        again = jnp.logical_and(place == pltpu.roll(place, 1, 1), lane % 2 == 1)
    with scope("mask"):
        group = group.astype(F32) + jnp.where(again, float(GROUPS), 0.0)
        square = (LANES, LANES)
        eye = lax.broadcasted_iota(jnp.int32, square, 0) == lax.broadcasted_iota(jnp.int32, square, 1)
        ones = jnp.ones(square, jnp.bfloat16)
        for c in range(n_keys // LANES):
            spread = jnp.where(eye, jnp.broadcast_to(group[c : c + 1, :], square), 0.0).astype(jnp.bfloat16)
            grp[c * LANES : (c + 1) * LANES, :] = jnp.dot(spread, ones, preferred_element_type=F32)

    with scope("turn"):
        get_q.wait()
        for h in range(2):
            half = q_ref[h * ROWS : (h + 1) * ROWS, :].astype(F32)
            pair = jnp.concatenate([half, half], axis=0).astype(jnp.bfloat16)
            for g in range(GROUPS // 2):
                qrep[pl.ds(h * LANES + g * 2 * ROWS, 2 * ROWS), :] = pair

    inv = 1.0 / tau_ref[0, 0]
    lane_group = (lax.broadcasted_iota(jnp.int32, (LANES, LANES), 1) // ROWS).astype(F32)

    @pl.loop(0, NBUF)
    def _(b):
        with scope("kw"):
            for sub in range(2):
                fetch(b * 2 + sub).wait()
        with scope("dots"):
            keys = k_ref[pl.ds(pl.multiple_of(b * quarter, quarter), quarter), :]
            dots = lax.dot_general(keys, qrep[...], (((1,), (1,)), ((), ())), preferred_element_type=F32)
            tops = []
            for r in range(0, quarter, part_rows):
                squares = jnp.zeros((part_rows, LANES), F32)
                for c in range(0, keys.shape[1], LANES):
                    kf = keys[r : r + part_rows, c : c + LANES].astype(F32)
                    squares = squares + kf * kf
                norms = jnp.sum(squares, axis=1, keepdims=True)
                scores = (2.0 * dots[r : r + part_rows] - norms) * inv
                sc[r : r + part_rows, :] = scores
                tops.append(jnp.max(scores.reshape(part_rows // 8, 8, 2 * LANES), axis=0))
            m = jnp.max(functools.reduce(jnp.maximum, tops), axis=0, keepdims=True)
        with scope("expand"):
            total = jnp.zeros((8, 2 * LANES), F32)
            for c in range(quarter // LANES):
                w = jnp.exp(sc[c * LANES : (c + 1) * LANES, :] - m)
                total = total + jnp.sum(w.reshape(LANES // 8, 8, 2 * LANES), axis=0)
                at = b * quarter + c * LANES
                tag = grp[pl.ds(pl.multiple_of(at, LANES), LANES), :]
                repeat = tag >= GROUPS
                mine = jnp.where(repeat, tag - GROUPS, tag) == lane_group
                for h in range(2):
                    own = jnp.where(mine, w[:, h * LANES : (h + 1) * LANES], 0.0)
                    before = pltpu.roll(own.reshape(LANES // 8, 8, LANES), 1, 1).reshape(LANES, LANES)
                    wx[pl.ds(at * 2 + h, LANES, stride=2), :] = own + jnp.where(repeat, before, 0.0)
            total = jnp.sum(total, axis=0, keepdims=True)
            stats_ref[pl.ds(b, 1), :] = m
            stats_ref[pl.ds(NBUF + b, 1), :] = total

    pltpu.make_async_copy(idx, tok_ref, isem).wait()
    unroll = 16
    rows = quarter // LANES
    with scope("scatter"):
        for c in range(rows):

            @pl.loop(0, LANES // unroll)
            def _(i):
                views = []
                for b in range(NBUF):
                    start = ((b * rows + c) * LANES + i * unroll) * 2
                    views.append(wx.at[pl.ds(pl.multiple_of(start, 2 * unroll), 2 * unroll), :])
                for u in range(0, unroll, 2):
                    both = [(b, v) for b in range(NBUF) for v in (u, u + 1)]
                    at = [idx_smem[(b * rows + c) * LANES + i * unroll + v] for b, v in both]
                    at = [pl.ds(row, 2, stride=HALF) for row in at]
                    new = [hist[b][at[n], :] + views[b][2 * v : 2 * v + 2, :] for n, (b, v) in enumerate(both)]
                    for n, (b, v) in enumerate(both):
                        hist[b][at[n], :] = new[n]


def comm_kernel(
    mix_ref, h0, h1, h2, h3, kstats, q_ref, w_hbm, out_ref,
    w_ref, logits, loc, din, d, ra, rb, rc, rd, e, r2, g3, r3, lt, lr, tsc, knn,
    wsem, s0, v0, s1, va, vb, ready, pal, s2, v2, s3, v3, sl, vl,
):
    core = lax.axis_index("store")
    chip = lax.axis_index("model")
    x, y, z = chip % RING, (chip // RING) % RING, chip // (RING * RING)
    dims = ((x, 1), (y, RING), (z, RING * RING))
    order = ((0, 1, 2), (1, 2, 0), (2, 0, 1))

    def peer(axis, delta):
        at, stride = dims[axis]
        return {"model": chip + ((at + delta) % RING - at) * stride}

    barrier = pltpu.get_barrier_semaphore()
    beside = [peer(axis, delta) for axis in range(3) for delta in (1, RING - 1)]
    for to in beside:
        pl.semaphore_signal(barrier, inc=1, device_id={**to, "store": 1}, device_id_type=MESH)

    @pl.when(core == 1)
    def _():
        pl.semaphore_signal(barrier, inc=1, device_id={"store": 0}, device_id_type=MESH)

    head = pltpu.make_async_copy(w_hbm, w_ref, wsem)
    head.start()

    @pl.when(core == 0)
    def _():
        pl.semaphore_wait(barrier, 1)
        pl.semaphore_signal(pal, inc=1, device_id={"store": 1}, device_id_type=MESH)

    hist = (h0, h1, h2, h3)
    top = functools.reduce(jnp.maximum, [kstats[b : b + 1, :] for b in range(NBUF)])
    scales = [jnp.exp(kstats[b : b + 1, :] - top) for b in range(NBUF)]
    mass = sum(c * kstats[NBUF + b : NBUF + b + 1, :] for b, c in enumerate(scales))
    half = [slice(h * LANES, (h + 1) * LANES) for h in range(2)]

    def add_up(j):
        turn, p = j // PARTS, j % PARTS
        delta = jnp.where(turn == 0, 2, jnp.where(turn == 1, 1, jnp.where(turn == 2, 3, 0)))
        blk = p * RING + ((chip >> (2 * p)) + delta) % RING
        for h in range(2):
            stats = jnp.concatenate([top[:, half[h]], mass[:, half[h]], jnp.zeros((STAT - 2, LANES), F32)], axis=0)
            for b in range(RING):
                loc[h, blk, b, LEAD : LEAD + STAT, :] = stats
                for t in range(BLOCK2 // 8):
                    at = pl.ds(pl.multiple_of(h * HALF + blk * BLOCK + b * BLOCK2 + t * 8, 8), 8)
                    total = scales[0][:, half[h]] * hist[0][at, :]
                    for n in range(1, NBUF):
                        total = total + scales[n][:, half[h]] * hist[n][at, :]
                    row = t * 8 if t * 8 < LEAD else t * 8 + STAT
                    loc[h, blk, b, row : row + 8, :] = total

    with scope("sum"):
        pl.loop(0, PARTS)(add_up)

    @pl.when(core == 1)
    def _():
        pl.semaphore_wait(pal, 1)

    def copy(src, dst, ssem, rsem, to):
        return pltpu.make_async_remote_copy(src_ref=src, dst_ref=dst, send_sem=ssem, recv_sem=rsem, device_id=to, device_id_type=MESH)

    tile = slice(LEAD, LEAD + STAT)
    pieces = (slice(0, LEAD), slice(LEAD + STAT, MSG2))
    turn = (2, 1, 3, 0)
    toward = (1, RING - 1)

    def parcel(k, way):
        half = (way + k) % 2
        if k == 0:
            return slice(0, LEAD + STAT) if half == 0 else slice(LEAD, MSG2)
        return pieces[half]

    partner = {"store": 1 - core}

    def across(axis, delta):
        return {**peer(axis, delta), "store": 1 - core} if delta else partner

    first = [dims[order[p][0]][0] for p in range(PARTS)]
    mid = [dims[order[p][1]][0] for p in range(PARTS)]
    last = [dims[order[p][2]][0] for p in range(PARTS)]

    def place(p, delta):
        return p * RING + (first[p] + delta) % RING

    def near(p, delta):
        blk = place(p, delta)
        return copy(loc.at[1 - core, blk], din.at[blk], s0, v0.at[p if delta == 2 else NEAR[delta]], partner)

    for p in range(PARTS):
        near(p, 2).start()
    with scope("sum2"):
        pl.loop(PARTS, PARTS * RING)(add_up)
    for delta in (1, 3, 0):
        for p in range(PARTS):
            near(p, delta).start()

    with scope("barrier"):

        @pl.when(core == 1)
        def _():
            pl.semaphore_wait(barrier, 12)
            pl.semaphore_signal(pal, inc=1, device_id={"store": 0}, device_id_type=MESH)

        @pl.when(core == 0)
        def _():
            pl.semaphore_wait(pal, 1)

    for to in beside:
        pl.semaphore_signal(ready, inc=1, device_id=to, device_id_type=MESH)

    def arrived(ref, sem, ssem=s1):
        copy(ref, ref, ssem, sem, partner).wait_recv()

    def link(axis, tile):
        lt[axis] = tile
        for delta in range(1, RING):
            copy(lt.at[axis], lr.at[axis, delta - 1], sl, vl.at[axis], peer(axis, delta)).start()

    def unlink(axis):
        copy(lr.at[axis], lr.at[axis], sl, vl.at[axis], partner).wait_recv()
        tiles = [lt[axis]] + [lr[axis, i] for i in range(3)]
        top = functools.reduce(jnp.maximum, [t[0:1] for t in tiles])
        total = sum(jnp.exp(t[0:1] - top) * t[1:2] for t in tiles)
        return jnp.concatenate([top, total, jnp.zeros((6, LANES), F32)], axis=0)

    def combine(stats):
        m = functools.reduce(jnp.maximum, [s[0:1] for s in stats])
        scales = [jnp.exp(s[0:1] - m) for s in stats]
        zz = sum(c * s[1:2] for c, s in zip(scales, stats))
        return scales, jnp.concatenate([m, zz, jnp.zeros((STAT - 2, LANES), F32)], axis=0)

    chipwise = []

    def issue(delta):
        for p in range(PARTS):
            blk = place(p, delta)
            with scope("w0"):
                if delta == 2:
                    near(p, delta).wait_recv()
                elif p == 0:
                    arrived(din.at[0:PARTS], v0.at[NEAR[delta]], s0)
            if not chipwise:
                chipwise.append(combine([loc[core, 0, 0, tile, :], din[blk, 0, tile, :]]))
            (c_own, c_par), stats = chipwise[0]
            for k in range(RING):
                b = (mid[p] + turn[k]) % RING
                if k == 0:
                    d[p, delta, k, tile, :] = stats
                for rows in pieces:
                    d[p, delta, k, rows, :] = c_own * loc[core, blk, b, rows, :] + c_par * din[blk, b, rows, :]
                for way in range(2):
                    rows = parcel(k, way)
                    if delta == 2:
                        to = peer(order[p][0], toward[way])
                        copy(d.at[p, delta, k, rows], ra.at[way, p, k, rows], s1, va.at[k], to).start()
                    elif delta == toward[1 - way]:
                        to = peer(order[p][0], delta)
                        copy(d.at[p, delta, k, rows], rb.at[way, p, k, rows], s1, vb.at[k * PARTS + p], to).start()

    joint = {}

    def relay(k):
        with scope("wa"):
            arrived(din.at[0:11, 0, 0:24] if k == 0 else ra.at[0, :, k, 0:BLOCK2], va.at[k])
        for p in range(PARTS):
            for way in range(2):
                if k == 0:
                    joint[p, way] = combine([d[p, toward[way], k, tile, :], ra[way, p, k, tile, :]])
                    rd[way, p, k, tile, :] = joint[p, way][1]
                c_own, c_far = joint[p, way][0]
                rows = pieces[(way + k) % 2]
                rd[way, p, k, rows, :] = c_own * d[p, toward[way], k, rows, :] + c_far * ra[way, p, k, rows, :]
                rows = parcel(k, way)
                to = peer(order[p][0], toward[way])
                copy(rd.at[way, p, k, rows], rc.at[way, p, k, rows], s1, vb.at[k * PARTS + p], to).start()

    factors = {}

    def gather(k):
        for p in range(PARTS):
            with scope("w1"):
                arrived(din.at[0:11, 0, 0:16] if k == 0 else din.at[0:2, 0, 0:BLOCK2], vb.at[k * PARTS + p])
            for way in range(2):
                if k == 0:
                    factors[p, way] = combine([d[p, 0, k, tile, :], rb[way, p, k, tile, :], rc[way, p, k, tile, :]])
                c_own, c_one, c_two = factors[p, way][0]
                rows = pieces[(way + k) % 2]
                at = STAT + (rows.start if rows.start == 0 else LEAD)
                e[p, k, at : at + rows.stop - rows.start, :] = (
                    c_own * d[p, 0, k, rows, :] + c_one * rb[way, p, k, rows, :] + c_two * rc[way, p, k, rows, :]
                )
            e[p, k, 0:STAT, :] = factors[p, 0][1]
            to = across(order[p][1], turn[k])
            copy(e.at[p, k], r2.at[p, turn[k]], s2, v2.at[p], to).start()

    issue(2)
    issue(1)
    with scope("lm"):
        head.wait()
        both = lax.dot_general(q_ref[...], w_ref[...], (((1,), (1,)), ((), ())), preferred_element_type=F32)
        mine = jnp.where(core == 0, both[:ROWS], both[ROWS:])
        logits[...] = mine
        lm_top = jnp.max(mine, axis=1, keepdims=True)
        lm_sum = jnp.sum(jnp.exp(mine - lm_top), axis=1, keepdims=True)
        lane = lax.broadcasted_iota(jnp.int32, (ROWS, LANES), 1)
        pair = jnp.where(lane == 0, lm_top, lm_sum)
        pair = jnp.concatenate([pair] * GROUPS, axis=0).T
        pl.semaphore_wait(ready, 6)
        link(0, pair[0:8, :])
    issue(3)
    issue(0)
    for b in range(RING):
        relay(b)
    link(1, unlink(0))
    for b in range(RING):
        gather(b)
    link(2, unlink(1))

    for p in range(PARTS):
        with scope("w2"):
            copy(r2.at[p], r2.at[p], s2, v2.at[p], partner).wait_recv()
        scales, stats = combine([r2[p, i, 0:STAT, :] for i in range(RING)])
        for c in range(RING):
            rows = slice(STAT + c * SLOTS, STAT + (c + 1) * SLOTS)
            total = scales[0] * r2[p, 0, rows, :]
            for i in range(1, RING):
                total = total + scales[i] * r2[p, i, rows, :]
            g3[p, c, 0:SLOTS, :] = total
            g3[p, c, SLOTS:MSG3, :] = stats[0 : MSG3 - SLOTS]
        for delta in (2, 1, 3, 0):
            to = (last[p] + delta) % RING
            copy(g3.at[p, to], r3.at[p, delta], s3, v3.at[p], across(order[p][2], delta)).start()

    slots = logits.shape[1] // GROUPS
    mix = mix_ref[0, 0]
    with scope("lm2"):
        tsc[...] = jnp.zeros(tsc.shape, F32)
        tsc[0:STAT, :] = unlink(2)
        turned = tsc[...].T
        lm = jnp.exp(logits[...] - turned[0:ROWS, 0:1]) / turned[0:ROWS, 1:2]
        logits[...] = (1.0 - mix) * lm
        copy(loc.at[1 - core], din, s0, v0.at[0], partner).wait_send()
        for sent in (ra, rb, rc):
            for ref in (din.at[0:11, 0, 0:24], sent.at[0, :, 1:RING, 0:BLOCK2]):
                copy(ref, ref, s1, va.at[0], partner).wait_send()
        copy(r2, r2, s2, v2.at[0], partner).wait_send()
        copy(lr, lr, sl, vl.at[0], partner).wait_send()

    for p in range(PARTS):
        with scope("w3"):
            copy(r3.at[p], r3.at[p], s3, v3.at[p], partner).wait_recv()
        blocks = [r3[p, i] for i in range(RING)]
        scales, stats = combine([v[SLOTS : SLOTS + 2] for v in blocks])
        count = min(SLOTS, slots - p * SLOTS)
        total = sum(c * v[0:count] for c, v in zip(scales, blocks))
        tsc[p * SLOTS : p * SLOTS + count, :] = total / stats[1:2]

    with scope("final"):
        turned = tsc[...].T
        for g in range(GROUPS):
            knn[:, g * slots : (g + 1) * slots] = turned[g * ROWS : (g + 1) * ROWS, 0:slots]
        out_ref[...] = jnp.log(mix * knn[...] + logits[...])

    copy(r3, r3, s3, v3.at[0], partner).wait_send()


def solution(mesh):
    def local_step(queries, w_head, store_keys, store_tok, temperature, mix_weight):
        n_keys, width = store_keys.shape
        vocab_loc = w_head.shape[1]
        vmem, smem, hbm = (pl.BlockSpec(memory_space=s) for s in (pltpu.VMEM, pltpu.SMEM, pltpu.HBM))

        in_hbm = lambda a: pltpu.with_memory_space_constraint(a, pltpu.HBM)
        *hist, stats = pl.pallas_call(
            functools.partial(local_kernel, vocab_loc),
            out_shape=[jax.ShapeDtypeStruct((HROWS, LANES), F32)] * NBUF + [jax.ShapeDtypeStruct((2 * NBUF, 2 * LANES), F32)],
            in_specs=[smem, hbm, hbm, hbm],
            out_specs=[vmem] * (NBUF + 1),
            scratch_shapes=[
                pltpu.VMEM(queries.shape, jnp.bfloat16),
                pltpu.VMEM(store_keys.shape, jnp.bfloat16),
                pltpu.VMEM((2 * LANES, width), jnp.bfloat16),
                pltpu.VMEM((n_keys // NBUF, 2 * LANES), F32),
                pltpu.VMEM((2 * n_keys, LANES), F32),
                pltpu.VMEM((n_keys, LANES), F32),
                pltpu.VMEM((n_keys // LANES, LANES), jnp.int32),
                pltpu.SMEM((n_keys,), jnp.int32),
                pltpu.VMEM((n_keys // LANES, LANES), jnp.int32),
                pltpu.SemaphoreType.DMA,
                pltpu.SemaphoreType.DMA,
                pltpu.SemaphoreType.DMA,
                pltpu.SemaphoreType.DMA((2 * NBUF,)),
            ],
            compiler_params=pltpu.CompilerParams(vmem_limit_bytes=KA_LIMIT * 2**20),
            name="histogram",
        )(temperature.reshape(1, 1), in_hbm(store_tok.reshape(n_keys // LANES, LANES)), in_hbm(queries), in_hbm(store_keys))

        return pl.pallas_call(
            comm_kernel,
            out_shape=jax.ShapeDtypeStruct((ROWS, vocab_loc), F32),
            in_specs=[smem] + [vmem] * (NBUF + 2) + [hbm],
            out_specs=vmem,
            scratch_shapes=[
                pltpu.VMEM(w_head.shape[::-1], jnp.bfloat16),
                pltpu.VMEM((ROWS, vocab_loc), F32),
                pltpu.VMEM((2, PARTS * RING, RING, MSG2, LANES), F32),
                pltpu.VMEM((PARTS * RING, RING, MSG2, LANES), F32),
                pltpu.VMEM((PARTS, RING, RING, MSG2, LANES), F32),
                pltpu.VMEM((2, PARTS, RING, MSG2, LANES), F32),
                pltpu.VMEM((2, PARTS, RING, MSG2, LANES), F32),
                pltpu.VMEM((2, PARTS, RING, MSG2, LANES), F32),
                pltpu.VMEM((2, PARTS, RING, MSG2, LANES), F32),
                pltpu.VMEM((PARTS, RING, MSG2, LANES), F32),
                pltpu.VMEM((PARTS, RING, MSG2, LANES), F32),
                pltpu.VMEM((PARTS, RING, MSG3, LANES), F32),
                pltpu.VMEM((PARTS, RING, MSG3, LANES), F32),
                pltpu.VMEM((3, STAT, LANES), F32),
                pltpu.VMEM((3, RING - 1, STAT, LANES), F32),
                pltpu.VMEM((LANES, LANES), F32),
                pltpu.VMEM((ROWS, vocab_loc), F32),
                pltpu.SemaphoreType.DMA,
                pltpu.SemaphoreType.DMA,
                pltpu.SemaphoreType.DMA((6,)),
                pltpu.SemaphoreType.DMA,
                pltpu.SemaphoreType.DMA((4,)),
                pltpu.SemaphoreType.DMA((12,)),
                pltpu.SemaphoreType.REGULAR,
                pltpu.SemaphoreType.REGULAR,
            ]
            + [pltpu.SemaphoreType.DMA, pltpu.SemaphoreType.DMA((3,))] * 3,
            compiler_params=pltpu.CompilerParams(collective_id=0, has_side_effects=True, vmem_limit_bytes=KB_LIMIT * 2**20),
            name="exchange",
        )(mix_weight.reshape(1, 1), *hist, stats, queries, in_hbm(w_head.T))

    return jax.shard_map(
        local_step,
        mesh=mesh,
        in_specs=(P("data", None), P(None, "model"), P(("store", "model"), None), P(("store", "model")), P(), P()),
        out_specs=P(("data", "store"), "model"),
        check_vma=False,
    )
```

```python
import functools

import jax
import jax.numpy as jnp
from jax import lax
from jax.experimental import pallas as pl
from jax.experimental.pallas import tpu as pltpu
from jax.sharding import PartitionSpec as P

F32 = jnp.float32
LANES = 128
RING = 4
CHIPS = RING**3
ROWS = 8
GROUPS = LANES // ROWS
SLOTS = 18
PARTS = 3
BLOCK = SLOTS * CHIPS // RING
BLOCK2 = BLOCK // RING
STAT = 8
MSG2 = STAT + BLOCK2
MSG3 = 24
NEAR = {1: 3, 3: 4, 0: 5}
LEAD = 40
NBUF = 4
KA_LIMIT = 36
KB_LIMIT = 36
HALF = SLOTS * CHIPS * PARTS + 8
HROWS = 2 * HALF
MESH = pl.DeviceIdType.MESH
scope = jax.named_scope


def below(a, n):
    return ((a.astype(F32) + 0.5) * (1.0 / n)).astype(jnp.int32)


def local_kernel(vocab_loc, tau_ref, tok_hbm, q_hbm, k_hbm, *refs):
    hist, stats_ref = refs[:NBUF], refs[NBUF]
    q_ref, k_ref, qrep, sc, wx, grp, idx, idx_smem, tok_ref, qsem, isem, tsem, ksem = refs[NBUF + 1 :]
    n_keys = k_ref.shape[0]
    quarter = n_keys // NBUF
    chunk = quarter // 2
    part_rows = 128

    def fetch(j):
        rows = pl.ds(pl.multiple_of(j * chunk, chunk), chunk)
        return pltpu.make_async_copy(k_hbm.at[rows], k_ref.at[rows], ksem.at[j])

    get_tok = pltpu.make_async_copy(tok_hbm, tok_ref, tsem)
    get_tok.start()
    get_q = pltpu.make_async_copy(q_hbm, q_ref, qsem)
    get_q.start()
    for j in range(2):
        fetch(j).start()
    span = 288
    pieces = 8

    for third in range(3):

        @pl.loop(third * pieces, (third + 1) * pieces)
        def _(i):
            for buf in hist:
                buf[pl.ds(pl.multiple_of(i * span + (i // 12) * 8, 8), span), :] = jnp.zeros((span, LANES), F32)

        for j in ((), (2, 3), (4, 5, 6, 7))[third]:
            fetch(j).start()

    get_tok.wait()
    with scope("index"):
        tok = tok_ref[...]
        chip = below(tok, vocab_loc)
        within = tok - chip * vocab_loc
        slots = vocab_loc // GROUPS
        group = below(within, slots)
        slot = within - group * slots
        part = (slot >= SLOTS).astype(jnp.int32) + (slot >= 2 * SLOTS).astype(jnp.int32)
        row = slot - part * SLOTS
        x, y, z = chip & 3, (chip >> 2) & 3, chip >> 4
        first = jnp.where(part == 0, x, jnp.where(part == 1, y, z))
        second = jnp.where(part == 0, y, jnp.where(part == 1, z, x))
        third = jnp.where(part == 0, z, jnp.where(part == 1, x, y))
        place = ((part * RING + first) * RING + second) * RING + third
        place = place * SLOTS + row
        idx[...] = place
        for r in range(n_keys // LANES):
            pltpu.make_async_copy(idx.at[r], idx_smem.at[pl.ds(r * LANES, LANES)], isem).start()
        lane = lax.broadcasted_iota(jnp.int32, place.shape, 1)
        again = jnp.logical_and(place == pltpu.roll(place, 1, 1), lane % 2 == 1)
    with scope("mask"):
        group = group.astype(F32) + jnp.where(again, float(GROUPS), 0.0)
        square = (LANES, LANES)
        eye = lax.broadcasted_iota(jnp.int32, square, 0) == lax.broadcasted_iota(jnp.int32, square, 1)
        ones = jnp.ones(square, jnp.bfloat16)
        for c in range(n_keys // LANES):
            spread = jnp.where(eye, jnp.broadcast_to(group[c : c + 1, :], square), 0.0).astype(jnp.bfloat16)
            grp[c * LANES : (c + 1) * LANES, :] = jnp.dot(spread, ones, preferred_element_type=F32)

    with scope("turn"):
        get_q.wait()
        for h in range(2):
            half = q_ref[h * ROWS : (h + 1) * ROWS, :].astype(F32)
            pair = jnp.concatenate([half, half], axis=0).astype(jnp.bfloat16)
            for g in range(GROUPS // 2):
                qrep[pl.ds(h * LANES + g * 2 * ROWS, 2 * ROWS), :] = pair

    tau = tau_ref[0, 0]
    unit = jnp.where(tau > 1.0, 2.0**-64, 1.0)
    inv = 1.0 / (tau * unit)
    lane_group = (lax.broadcasted_iota(jnp.int32, (LANES, LANES), 1) // ROWS).astype(F32)

    @pl.loop(0, NBUF)
    def _(b):
        with scope("kw"):
            for sub in range(2):
                fetch(b * 2 + sub).wait()
        with scope("dots"):
            keys = k_ref[pl.ds(pl.multiple_of(b * quarter, quarter), quarter), :]
            dots = lax.dot_general(keys, qrep[...], (((1,), (1,)), ((), ())), preferred_element_type=F32)
            tops = []
            for r in range(0, quarter, part_rows):
                squares = jnp.zeros((part_rows, LANES), F32)
                for c in range(0, keys.shape[1], LANES):
                    kf = keys[r : r + part_rows, c : c + LANES].astype(F32)
                    squares = squares + kf * kf
                norms = jnp.sum(squares, axis=1, keepdims=True)
                scores = ((2.0 * unit) * dots[r : r + part_rows] - unit * norms) * inv
                sc[r : r + part_rows, :] = scores
                tops.append(jnp.max(scores.reshape(part_rows // 8, 8, 2 * LANES), axis=0))
            m = jnp.max(functools.reduce(jnp.maximum, tops), axis=0, keepdims=True)
        with scope("expand"):
            total = jnp.zeros((8, 2 * LANES), F32)
            for c in range(quarter // LANES):
                w = jnp.exp(sc[c * LANES : (c + 1) * LANES, :] - m)
                total = total + jnp.sum(w.reshape(LANES // 8, 8, 2 * LANES), axis=0)
                at = b * quarter + c * LANES
                tag = grp[pl.ds(pl.multiple_of(at, LANES), LANES), :]
                repeat = tag >= GROUPS
                mine = jnp.where(repeat, tag - GROUPS, tag) == lane_group
                for h in range(2):
                    own = jnp.where(mine, w[:, h * LANES : (h + 1) * LANES], 0.0)
                    before = pltpu.roll(own.reshape(LANES // 8, 8, LANES), 1, 1).reshape(LANES, LANES)
                    wx[pl.ds(at * 2 + h, LANES, stride=2), :] = own + jnp.where(repeat, before, 0.0)
            total = jnp.sum(total, axis=0, keepdims=True)
            stats_ref[pl.ds(b, 1), :] = m
            stats_ref[pl.ds(NBUF + b, 1), :] = total

    pltpu.make_async_copy(idx, tok_ref, isem).wait()
    unroll = 16
    rows = quarter // LANES
    with scope("scatter"):
        for c in range(rows):

            @pl.loop(0, LANES // unroll)
            def _(i):
                views = []
                for b in range(NBUF):
                    start = ((b * rows + c) * LANES + i * unroll) * 2
                    views.append(wx.at[pl.ds(pl.multiple_of(start, 2 * unroll), 2 * unroll), :])
                for u in range(0, unroll, 2):
                    both = [(b, v) for b in range(NBUF) for v in (u, u + 1)]
                    at = [idx_smem[(b * rows + c) * LANES + i * unroll + v] for b, v in both]
                    at = [pl.ds(row, 2, stride=HALF) for row in at]
                    new = [hist[b][at[n], :] + views[b][2 * v : 2 * v + 2, :] for n, (b, v) in enumerate(both)]
                    for n, (b, v) in enumerate(both):
                        hist[b][at[n], :] = new[n]


def comm_kernel(
    mix_ref, h0, h1, h2, h3, kstats, q_ref, w_hbm, out_ref,
    w_ref, logits, loc, din, d, ra, rb, rc, rd, e, r2, g3, r3, lt, lr, tsc, knn,
    wsem, s0, v0, s1, va, vb, ready, pal, s2, v2, s3, v3, sl, vl,
):
    core = lax.axis_index("store")
    chip = lax.axis_index("model")
    x, y, z = chip % RING, (chip // RING) % RING, chip // (RING * RING)
    dims = ((x, 1), (y, RING), (z, RING * RING))
    order = ((0, 1, 2), (1, 2, 0), (2, 0, 1))

    def peer(axis, delta):
        at, stride = dims[axis]
        return {"model": chip + ((at + delta) % RING - at) * stride}

    barrier = pltpu.get_barrier_semaphore()
    beside = [peer(axis, delta) for axis in range(3) for delta in (1, RING - 1)]
    for to in beside:
        pl.semaphore_signal(barrier, inc=1, device_id={**to, "store": 1}, device_id_type=MESH)

    @pl.when(core == 1)
    def _():
        pl.semaphore_signal(barrier, inc=1, device_id={"store": 0}, device_id_type=MESH)

    head = pltpu.make_async_copy(w_hbm, w_ref, wsem)
    head.start()

    @pl.when(core == 0)
    def _():
        pl.semaphore_wait(barrier, 1)
        pl.semaphore_signal(pal, inc=1, device_id={"store": 1}, device_id_type=MESH)

    hist = (h0, h1, h2, h3)
    top = functools.reduce(jnp.maximum, [kstats[b : b + 1, :] for b in range(NBUF)])
    scales = [jnp.exp(kstats[b : b + 1, :] - top) for b in range(NBUF)]
    mass = sum(c * kstats[NBUF + b : NBUF + b + 1, :] for b, c in enumerate(scales))
    half = [slice(h * LANES, (h + 1) * LANES) for h in range(2)]

    def add_up(j):
        turn, p = j // PARTS, j % PARTS
        delta = jnp.where(turn == 0, 2, jnp.where(turn == 1, 1, jnp.where(turn == 2, 3, 0)))
        blk = p * RING + ((chip >> (2 * p)) + delta) % RING
        for h in range(2):
            stats = jnp.concatenate([top[:, half[h]], mass[:, half[h]], jnp.zeros((STAT - 2, LANES), F32)], axis=0)
            for b in range(RING):
                loc[h, blk, b, LEAD : LEAD + STAT, :] = stats
                for t in range(BLOCK2 // 8):
                    at = pl.ds(pl.multiple_of(h * HALF + blk * BLOCK + b * BLOCK2 + t * 8, 8), 8)
                    total = scales[0][:, half[h]] * hist[0][at, :]
                    for n in range(1, NBUF):
                        total = total + scales[n][:, half[h]] * hist[n][at, :]
                    row = t * 8 if t * 8 < LEAD else t * 8 + STAT
                    loc[h, blk, b, row : row + 8, :] = total

    def copy(src, dst, ssem, rsem, to):
        return pltpu.make_async_remote_copy(src_ref=src, dst_ref=dst, send_sem=ssem, recv_sem=rsem, device_id=to, device_id_type=MESH)

    tile = slice(LEAD, LEAD + STAT)
    pieces = (slice(0, LEAD), slice(LEAD + STAT, MSG2))
    turn = (2, 1, 3, 0)
    toward = (1, RING - 1)

    def parcel(k, way):
        half = (way + k) % 2
        if k == 0:
            return slice(0, LEAD + STAT) if half == 0 else slice(LEAD, MSG2)
        return pieces[half]

    partner = {"store": 1 - core}

    def across(axis, delta):
        return {**peer(axis, delta), "store": 1 - core} if delta else partner

    first = [dims[order[p][0]][0] for p in range(PARTS)]
    mid = [dims[order[p][1]][0] for p in range(PARTS)]
    last = [dims[order[p][2]][0] for p in range(PARTS)]

    def place(p, delta):
        return p * RING + (first[p] + delta) % RING

    def near(p, delta):
        blk = place(p, delta)
        return copy(loc.at[1 - core, blk], din.at[blk], s0, v0.at[p if delta == 2 else NEAR[delta]], partner)

    with scope("sum"):

        @pl.loop(0, PARTS)
        def _(p):
            add_up(p)

            @pl.when(jnp.logical_and(core == 1, p == 0))
            def _():
                pl.semaphore_wait(pal, 1)

            blk = p * RING + ((chip >> (2 * p)) + 2) % RING
            copy(loc.at[1 - core, blk], din.at[blk], s0, v0.at[p], partner).start()

    with scope("sum2"):
        pl.loop(PARTS, 3 * PARTS)(add_up)
    for delta in (1, 3):
        for p in range(PARTS):
            near(p, delta).start()

    with scope("barrier"):

        @pl.when(core == 1)
        def _():
            pl.semaphore_wait(barrier, 12)
            pl.semaphore_signal(pal, inc=1, device_id={"store": 0}, device_id_type=MESH)

        @pl.when(core == 0)
        def _():
            pl.semaphore_wait(pal, 1)

    for to in beside:
        pl.semaphore_signal(ready, inc=1, device_id=to, device_id_type=MESH)

    def arrived(ref, sem, ssem=s1):
        copy(ref, ref, ssem, sem, partner).wait_recv()

    def link(axis, tile):
        lt[axis] = tile
        for delta in range(1, RING):
            copy(lt.at[axis], lr.at[axis, delta - 1], sl, vl.at[axis], peer(axis, delta)).start()

    def unlink(axis):
        copy(lr.at[axis], lr.at[axis], sl, vl.at[axis], partner).wait_recv()
        tiles = [lt[axis]] + [lr[axis, i] for i in range(3)]
        top = functools.reduce(jnp.maximum, [t[0:1] for t in tiles])
        total = sum(jnp.exp(t[0:1] - top) * t[1:2] for t in tiles)
        return jnp.concatenate([top, total, jnp.zeros((6, LANES), F32)], axis=0)

    def combine(stats):
        m = functools.reduce(jnp.maximum, [s[0:1] for s in stats])
        scales = [jnp.exp(s[0:1] - m) for s in stats]
        zz = sum(c * s[1:2] for c, s in zip(scales, stats))
        return scales, jnp.concatenate([m, zz, jnp.zeros((STAT - 2, LANES), F32)], axis=0)

    chipwise = []

    def issue(delta):
        for p in range(PARTS):
            blk = place(p, delta)
            with scope("w0"):
                if delta == 2:
                    near(p, delta).wait_recv()
                elif p == 0:
                    arrived(din.at[0:PARTS], v0.at[NEAR[delta]], s0)
            if not chipwise:
                chipwise.append(combine([loc[core, blk, 0, tile, :], din[blk, 0, tile, :]]))
            (c_own, c_par), stats = chipwise[0]
            for k in range(RING):
                b = (mid[p] + turn[k]) % RING
                if k == 0:
                    d[p, delta, k, tile, :] = stats
                for rows in pieces:
                    d[p, delta, k, rows, :] = c_own * loc[core, blk, b, rows, :] + c_par * din[blk, b, rows, :]
                for way in range(2):
                    rows = parcel(k, way)
                    if delta == 2:
                        to = peer(order[p][0], toward[way])
                        copy(d.at[p, delta, k, rows], ra.at[way, p, k, rows], s1, va.at[k], to).start()
                    elif delta == toward[1 - way]:
                        to = peer(order[p][0], delta)
                        copy(d.at[p, delta, k, rows], rb.at[way, p, k, rows], s1, vb.at[k * PARTS + p], to).start()

    joint = {}

    def relay(k):
        with scope("wa"):
            arrived(din.at[0:11, 0, 0:24] if k == 0 else ra.at[0, :, k, 0:BLOCK2], va.at[k])
        for p in range(PARTS):
            for way in range(2):
                if k == 0:
                    joint[p, way] = combine([d[p, toward[way], k, tile, :], ra[way, p, k, tile, :]])
                    rd[way, p, k, tile, :] = joint[p, way][1]
                c_own, c_far = joint[p, way][0]
                rows = pieces[(way + k) % 2]
                rd[way, p, k, rows, :] = c_own * d[p, toward[way], k, rows, :] + c_far * ra[way, p, k, rows, :]
                rows = parcel(k, way)
                to = peer(order[p][0], toward[way])
                copy(rd.at[way, p, k, rows], rc.at[way, p, k, rows], s1, vb.at[k * PARTS + p], to).start()

    factors = {}

    def gather(k):
        for p in range(PARTS):
            with scope("w1"):
                arrived(din.at[0:11, 0, 0:16] if k == 0 else din.at[0:2, 0, 0:BLOCK2], vb.at[k * PARTS + p])
            for way in range(2):
                if k == 0:
                    factors[p, way] = combine([d[p, 0, k, tile, :], rb[way, p, k, tile, :], rc[way, p, k, tile, :]])
                c_own, c_one, c_two = factors[p, way][0]
                rows = pieces[(way + k) % 2]
                at = STAT + (rows.start if rows.start == 0 else LEAD)
                e[p, k, at : at + rows.stop - rows.start, :] = (
                    c_own * d[p, 0, k, rows, :] + c_one * rb[way, p, k, rows, :] + c_two * rc[way, p, k, rows, :]
                )
            e[p, k, 0:STAT, :] = factors[p, 0][1]
            to = across(order[p][1], turn[k])
            copy(e.at[p, k], r2.at[p, turn[k]], s2, v2.at[p], to).start()

    issue(2)
    with scope("sum3"):
        pl.loop(3 * PARTS, 4 * PARTS)(add_up)
    for p in range(PARTS):
        near(p, 0).start()
    issue(1)
    with scope("lm"):
        head.wait()
        both = lax.dot_general(q_ref[...], w_ref[...], (((1,), (1,)), ((), ())), preferred_element_type=F32)
        mine = jnp.where(core == 0, both[:ROWS], both[ROWS:])
        logits[...] = mine
        lm_top = jnp.max(mine, axis=1, keepdims=True)
        lm_sum = jnp.sum(jnp.exp(mine - lm_top), axis=1, keepdims=True)
        lane = lax.broadcasted_iota(jnp.int32, (ROWS, LANES), 1)
        pair = jnp.where(lane == 0, lm_top, lm_sum)
        pair = jnp.concatenate([pair] * GROUPS, axis=0).T
        pl.semaphore_wait(ready, 6)
        link(0, pair[0:8, :])
    issue(3)
    issue(0)
    for b in range(RING):
        relay(b)
    link(1, unlink(0))
    for b in range(RING):
        gather(b)
    link(2, unlink(1))

    for p in range(PARTS):
        with scope("w2"):
            copy(r2.at[p], r2.at[p], s2, v2.at[p], partner).wait_recv()
        scales, stats = combine([r2[p, i, 0:STAT, :] for i in range(RING)])
        for c in range(RING):
            rows = slice(STAT + c * SLOTS, STAT + (c + 1) * SLOTS)
            total = scales[0] * r2[p, 0, rows, :]
            for i in range(1, RING):
                total = total + scales[i] * r2[p, i, rows, :]
            g3[p, c, 0:SLOTS, :] = total
            g3[p, c, SLOTS:MSG3, :] = stats[0 : MSG3 - SLOTS]
        for delta in (2, 1, 3, 0):
            to = (last[p] + delta) % RING
            copy(g3.at[p, to], r3.at[p, delta], s3, v3.at[p], across(order[p][2], delta)).start()

    slots = logits.shape[1] // GROUPS
    mix = mix_ref[0, 0]
    with scope("lm2"):
        tsc[...] = jnp.zeros(tsc.shape, F32)
        tsc[0:STAT, :] = unlink(2)
        turned = tsc[...].T
        lm = jnp.exp(logits[...] - turned[0:ROWS, 0:1]) / turned[0:ROWS, 1:2]
        logits[...] = (1.0 - mix) * lm
        copy(loc.at[1 - core], din, s0, v0.at[0], partner).wait_send()
        for sent in (ra, rb, rc):
            for ref in (din.at[0:11, 0, 0:24], sent.at[0, :, 1:RING, 0:BLOCK2]):
                copy(ref, ref, s1, va.at[0], partner).wait_send()
        copy(r2, r2, s2, v2.at[0], partner).wait_send()
        copy(lr, lr, sl, vl.at[0], partner).wait_send()

    for p in range(PARTS):
        with scope("w3"):
            copy(r3.at[p], r3.at[p], s3, v3.at[p], partner).wait_recv()
        blocks = [r3[p, i] for i in range(RING)]
        scales, stats = combine([v[SLOTS : SLOTS + 2] for v in blocks])
        count = min(SLOTS, slots - p * SLOTS)
        total = sum(c * v[0:count] for c, v in zip(scales, blocks))
        tsc[p * SLOTS : p * SLOTS + count, :] = total / stats[1:2]

    with scope("final"):
        turned = tsc[...].T
        for g in range(GROUPS):
            knn[:, g * slots : (g + 1) * slots] = turned[g * ROWS : (g + 1) * ROWS, 0:slots]
        out_ref[...] = jnp.log(mix * knn[...] + logits[...])

    copy(r3, r3, s3, v3.at[0], partner).wait_send()


def solution(mesh):
    def local_step(queries, w_head, store_keys, store_tok, temperature, mix_weight):
        n_keys, width = store_keys.shape
        vocab_loc = w_head.shape[1]
        vmem, smem, hbm = (pl.BlockSpec(memory_space=s) for s in (pltpu.VMEM, pltpu.SMEM, pltpu.HBM))

        in_hbm = lambda a: pltpu.with_memory_space_constraint(a, pltpu.HBM)
        *hist, stats = pl.pallas_call(
            functools.partial(local_kernel, vocab_loc),
            out_shape=[jax.ShapeDtypeStruct((HROWS, LANES), F32)] * NBUF + [jax.ShapeDtypeStruct((2 * NBUF, 2 * LANES), F32)],
            in_specs=[smem, hbm, hbm, hbm],
            out_specs=[vmem] * (NBUF + 1),
            scratch_shapes=[
                pltpu.VMEM(queries.shape, jnp.bfloat16),
                pltpu.VMEM(store_keys.shape, jnp.bfloat16),
                pltpu.VMEM((2 * LANES, width), jnp.bfloat16),
                pltpu.VMEM((n_keys // NBUF, 2 * LANES), F32),
                pltpu.VMEM((2 * n_keys, LANES), F32),
                pltpu.VMEM((n_keys, LANES), F32),
                pltpu.VMEM((n_keys // LANES, LANES), jnp.int32),
                pltpu.SMEM((n_keys,), jnp.int32),
                pltpu.VMEM((n_keys // LANES, LANES), jnp.int32),
                pltpu.SemaphoreType.DMA,
                pltpu.SemaphoreType.DMA,
                pltpu.SemaphoreType.DMA,
                pltpu.SemaphoreType.DMA((2 * NBUF,)),
            ],
            compiler_params=pltpu.CompilerParams(vmem_limit_bytes=KA_LIMIT * 2**20),
            name="histogram",
        )(temperature.reshape(1, 1), in_hbm(store_tok.reshape(n_keys // LANES, LANES)), in_hbm(queries), in_hbm(store_keys))

        return pl.pallas_call(
            comm_kernel,
            out_shape=jax.ShapeDtypeStruct((ROWS, vocab_loc), F32),
            in_specs=[smem] + [vmem] * (NBUF + 2) + [hbm],
            out_specs=vmem,
            scratch_shapes=[
                pltpu.VMEM(w_head.shape[::-1], jnp.bfloat16),
                pltpu.VMEM((ROWS, vocab_loc), F32),
                pltpu.VMEM((2, PARTS * RING, RING, MSG2, LANES), F32),
                pltpu.VMEM((PARTS * RING, RING, MSG2, LANES), F32),
                pltpu.VMEM((PARTS, RING, RING, MSG2, LANES), F32),
                pltpu.VMEM((2, PARTS, RING, MSG2, LANES), F32),
                pltpu.VMEM((2, PARTS, RING, MSG2, LANES), F32),
                pltpu.VMEM((2, PARTS, RING, MSG2, LANES), F32),
                pltpu.VMEM((2, PARTS, RING, MSG2, LANES), F32),
                pltpu.VMEM((PARTS, RING, MSG2, LANES), F32),
                pltpu.VMEM((PARTS, RING, MSG2, LANES), F32),
                pltpu.VMEM((PARTS, RING, MSG3, LANES), F32),
                pltpu.VMEM((PARTS, RING, MSG3, LANES), F32),
                pltpu.VMEM((3, STAT, LANES), F32),
                pltpu.VMEM((3, RING - 1, STAT, LANES), F32),
                pltpu.VMEM((LANES, LANES), F32),
                pltpu.VMEM((ROWS, vocab_loc), F32),
                pltpu.SemaphoreType.DMA,
                pltpu.SemaphoreType.DMA,
                pltpu.SemaphoreType.DMA((6,)),
                pltpu.SemaphoreType.DMA,
                pltpu.SemaphoreType.DMA((4,)),
                pltpu.SemaphoreType.DMA((12,)),
                pltpu.SemaphoreType.REGULAR,
                pltpu.SemaphoreType.REGULAR,
            ]
            + [pltpu.SemaphoreType.DMA, pltpu.SemaphoreType.DMA((3,))] * 3,
            compiler_params=pltpu.CompilerParams(collective_id=0, has_side_effects=True, vmem_limit_bytes=KB_LIMIT * 2**20),
            name="exchange",
        )(mix_weight.reshape(1, 1), *hist, stats, queries, in_hbm(w_head.T))

    return jax.shard_map(
        local_step,
        mesh=mesh,
        in_specs=(P("data", None), P(None, "model"), P(("store", "model"), None), P(("store", "model")), P(), P()),
        out_specs=P(("data", "store"), "model"),
        check_vma=False,
    )
```

```python
import functools

import jax
import jax.numpy as jnp
from jax import lax
from jax.experimental import pallas as pl
from jax.experimental.pallas import tpu as pltpu
from jax.sharding import PartitionSpec as P

F32 = jnp.float32
LANES = 128
RING = 4
CHIPS = RING**3
ROWS = 8
GROUPS = LANES // ROWS
SLOTS = 18
PARTS = 3
BLOCK = SLOTS * CHIPS // RING
BLOCK2 = BLOCK // RING
STAT = 8
MSG2 = STAT + BLOCK2
MSG3 = 24
NEAR = {1: 3, 3: 4, 0: 5}
LEAD = 40
NBUF = 4
KA_LIMIT = 36
KB_LIMIT = 36
HALF = SLOTS * CHIPS * PARTS + 8
HROWS = 2 * HALF
MESH = pl.DeviceIdType.MESH
scope = jax.named_scope


def below(a, n):
    return ((a.astype(F32) + 0.5) * (1.0 / n)).astype(jnp.int32)


def local_kernel(vocab_loc, tau_ref, tok_hbm, q_hbm, k_hbm, *refs):
    hist, stats_ref = refs[:NBUF], refs[NBUF]
    q_ref, k_ref, qrep, sc, wx, grp, idx, idx_smem, tok_ref, qsem, isem, tsem, ksem = refs[NBUF + 1 :]
    n_keys = k_ref.shape[0]
    quarter = n_keys // NBUF
    chunk = quarter // 2
    part_rows = 128

    def fetch(j):
        rows = pl.ds(pl.multiple_of(j * chunk, chunk), chunk)
        return pltpu.make_async_copy(k_hbm.at[rows], k_ref.at[rows], ksem.at[j])

    get_tok = pltpu.make_async_copy(tok_hbm, tok_ref, tsem)
    get_tok.start()
    get_q = pltpu.make_async_copy(q_hbm, q_ref, qsem)
    get_q.start()
    for j in range(2):
        fetch(j).start()
    span = 288
    pieces = 8

    for third in range(3):

        @pl.loop(third * pieces, (third + 1) * pieces)
        def _(i):
            for buf in hist:
                buf[pl.ds(pl.multiple_of(i * span + (i // 12) * 8, 8), span), :] = jnp.zeros((span, LANES), F32)

        for j in ((), (2, 3), (4, 5, 6, 7))[third]:
            fetch(j).start()

    get_tok.wait()
    with scope("index"):
        tok = tok_ref[...]
        chip = below(tok, vocab_loc)
        within = tok - chip * vocab_loc
        slots = vocab_loc // GROUPS
        group = below(within, slots)
        slot = within - group * slots
        part = (slot >= SLOTS).astype(jnp.int32) + (slot >= 2 * SLOTS).astype(jnp.int32)
        row = slot - part * SLOTS
        x, y, z = chip & 3, (chip >> 2) & 3, chip >> 4
        first = jnp.where(part == 0, x, jnp.where(part == 1, y, z))
        second = jnp.where(part == 0, y, jnp.where(part == 1, z, x))
        third = jnp.where(part == 0, z, jnp.where(part == 1, x, y))
        place = ((part * RING + first) * RING + second) * RING + third
        place = place * SLOTS + row
        idx[...] = place
        for r in range(n_keys // LANES):
            pltpu.make_async_copy(idx.at[r], idx_smem.at[pl.ds(r * LANES, LANES)], isem).start()
        lane = lax.broadcasted_iota(jnp.int32, place.shape, 1)
        again = jnp.logical_and(place == pltpu.roll(place, 1, 1), lane % 2 == 1)
    with scope("mask"):
        group = group.astype(F32) + jnp.where(again, float(GROUPS), 0.0)
        square = (LANES, LANES)
        eye = lax.broadcasted_iota(jnp.int32, square, 0) == lax.broadcasted_iota(jnp.int32, square, 1)
        ones = jnp.ones(square, jnp.bfloat16)
        for c in range(n_keys // LANES):
            spread = jnp.where(eye, jnp.broadcast_to(group[c : c + 1, :], square), 0.0).astype(jnp.bfloat16)
            grp[c * LANES : (c + 1) * LANES, :] = jnp.dot(spread, ones, preferred_element_type=F32)

    with scope("turn"):
        get_q.wait()
        for h in range(2):
            half = q_ref[h * ROWS : (h + 1) * ROWS, :].astype(F32)
            pair = jnp.concatenate([half, half], axis=0).astype(jnp.bfloat16)
            for g in range(GROUPS // 2):
                qrep[pl.ds(h * LANES + g * 2 * ROWS, 2 * ROWS), :] = pair

    tau = tau_ref[0, 0]
    unit = jnp.where(tau > 1.0, 2.0**-64, 1.0)
    inv = 1.0 / (tau * unit)
    lane_group = (lax.broadcasted_iota(jnp.int32, (LANES, LANES), 1) // ROWS).astype(F32)

    @pl.loop(0, NBUF)
    def _(b):
        with scope("kw"):
            for sub in range(2):
                fetch(b * 2 + sub).wait()
        with scope("dots"):
            keys = k_ref[pl.ds(pl.multiple_of(b * quarter, quarter), quarter), :]
            dots = lax.dot_general(keys, qrep[...], (((1,), (1,)), ((), ())), preferred_element_type=F32)
            tops = []
            for r in range(0, quarter, part_rows):
                squares = jnp.zeros((part_rows, LANES), F32)
                for c in range(0, keys.shape[1], LANES):
                    kf = keys[r : r + part_rows, c : c + LANES].astype(F32)
                    squares = squares + kf * kf
                norms = jnp.sum(squares, axis=1, keepdims=True)
                scores = ((2.0 * unit) * dots[r : r + part_rows] - unit * norms) * inv
                sc[r : r + part_rows, :] = scores
                tops.append(jnp.max(scores.reshape(part_rows // 8, 8, 2 * LANES), axis=0))
            m = jnp.max(functools.reduce(jnp.maximum, tops), axis=0, keepdims=True)
        with scope("expand"):
            total = jnp.zeros((8, 2 * LANES), F32)
            for c in range(quarter // LANES):
                w = jnp.exp(sc[c * LANES : (c + 1) * LANES, :] - m)
                total = total + jnp.sum(w.reshape(LANES // 8, 8, 2 * LANES), axis=0)
                at = b * quarter + c * LANES
                tag = grp[pl.ds(pl.multiple_of(at, LANES), LANES), :]
                repeat = tag >= GROUPS
                mine = jnp.where(repeat, tag - GROUPS, tag) == lane_group
                for h in range(2):
                    own = jnp.where(mine, w[:, h * LANES : (h + 1) * LANES], 0.0)
                    before = pltpu.roll(own.reshape(LANES // 8, 8, LANES), 1, 1).reshape(LANES, LANES)
                    wx[pl.ds(at * 2 + h, LANES, stride=2), :] = own + jnp.where(repeat, before, 0.0)
            total = jnp.sum(total, axis=0, keepdims=True)
            stats_ref[pl.ds(b, 1), :] = m
            stats_ref[pl.ds(NBUF + b, 1), :] = total

    pltpu.make_async_copy(idx, tok_ref, isem).wait()
    unroll = 32
    rows = quarter // LANES
    with scope("scatter"):
        for c in range(rows):

            @pl.loop(0, LANES // unroll)
            def _(i):
                views = []
                for b in range(NBUF):
                    start = ((b * rows + c) * LANES + i * unroll) * 2
                    views.append(wx.at[pl.ds(pl.multiple_of(start, 2 * unroll), 2 * unroll), :])
                for u in range(0, unroll, 2):
                    both = [(b, v) for b in range(NBUF) for v in (u, u + 1)]
                    at = [idx_smem[(b * rows + c) * LANES + i * unroll + v] for b, v in both]
                    at = [pl.ds(row, 2, stride=HALF) for row in at]
                    new = [hist[b][at[n], :] + views[b][2 * v : 2 * v + 2, :] for n, (b, v) in enumerate(both)]
                    for n, (b, v) in enumerate(both):
                        hist[b][at[n], :] = new[n]


def comm_kernel(
    mix_ref, h0, h1, h2, h3, kstats, q_ref, w_hbm, out_ref,
    w_ref, logits, loc, din, d, ra, rb, rc, rd, e, r2, g3, r3, lt, lr, tsc, knn,
    wsem, s0, v0, s1, va, vb, ready, pal, s2, v2, s3, v3, sl, vl,
):
    core = lax.axis_index("store")
    chip = lax.axis_index("model")
    x, y, z = chip % RING, (chip // RING) % RING, chip // (RING * RING)
    dims = ((x, 1), (y, RING), (z, RING * RING))
    order = ((0, 1, 2), (1, 2, 0), (2, 0, 1))

    def peer(axis, delta):
        at, stride = dims[axis]
        return {"model": chip + ((at + delta) % RING - at) * stride}

    barrier = pltpu.get_barrier_semaphore()
    beside = [peer(axis, delta) for axis in range(3) for delta in (1, RING - 1)]
    for to in beside:
        pl.semaphore_signal(barrier, inc=1, device_id={**to, "store": 1}, device_id_type=MESH)

    @pl.when(core == 1)
    def _():
        pl.semaphore_signal(barrier, inc=1, device_id={"store": 0}, device_id_type=MESH)

    head = pltpu.make_async_copy(w_hbm, w_ref, wsem)
    head.start()

    @pl.when(core == 0)
    def _():
        pl.semaphore_wait(barrier, 1)
        pl.semaphore_signal(pal, inc=1, device_id={"store": 1}, device_id_type=MESH)

    hist = (h0, h1, h2, h3)
    top = functools.reduce(jnp.maximum, [kstats[b : b + 1, :] for b in range(NBUF)])
    scales = [jnp.exp(kstats[b : b + 1, :] - top) for b in range(NBUF)]
    mass = sum(c * kstats[NBUF + b : NBUF + b + 1, :] for b, c in enumerate(scales))
    half = [slice(h * LANES, (h + 1) * LANES) for h in range(2)]

    def add_up(j):
        turn, p = j // PARTS, j % PARTS
        delta = jnp.where(turn == 0, 2, jnp.where(turn == 1, 1, jnp.where(turn == 2, 3, 0)))
        blk = p * RING + ((chip >> (2 * p)) + delta) % RING
        for h in range(2):
            stats = jnp.concatenate([top[:, half[h]], mass[:, half[h]], jnp.zeros((STAT - 2, LANES), F32)], axis=0)
            for b in range(RING):
                loc[h, blk, b, LEAD : LEAD + STAT, :] = stats
                for t in range(BLOCK2 // 8):
                    at = pl.ds(pl.multiple_of(h * HALF + blk * BLOCK + b * BLOCK2 + t * 8, 8), 8)
                    total = scales[0][:, half[h]] * hist[0][at, :]
                    for n in range(1, NBUF):
                        total = total + scales[n][:, half[h]] * hist[n][at, :]
                    row = t * 8 if t * 8 < LEAD else t * 8 + STAT
                    loc[h, blk, b, row : row + 8, :] = total

    def copy(src, dst, ssem, rsem, to):
        return pltpu.make_async_remote_copy(src_ref=src, dst_ref=dst, send_sem=ssem, recv_sem=rsem, device_id=to, device_id_type=MESH)

    tile = slice(LEAD, LEAD + STAT)
    pieces = (slice(0, LEAD), slice(LEAD + STAT, MSG2))
    turn = (2, 1, 3, 0)
    toward = (1, RING - 1)

    def parcel(k, way):
        half = (way + k) % 2
        if k == 0:
            return slice(0, LEAD + STAT) if half == 0 else slice(LEAD, MSG2)
        return pieces[half]

    partner = {"store": 1 - core}

    def across(axis, delta):
        return {**peer(axis, delta), "store": 1 - core} if delta else partner

    first = [dims[order[p][0]][0] for p in range(PARTS)]
    mid = [dims[order[p][1]][0] for p in range(PARTS)]
    last = [dims[order[p][2]][0] for p in range(PARTS)]

    def place(p, delta):
        return p * RING + (first[p] + delta) % RING

    def near(p, delta):
        blk = place(p, delta)
        return copy(loc.at[1 - core, blk], din.at[blk], s0, v0.at[p if delta == 2 else NEAR[delta]], partner)

    with scope("sum"):

        @pl.loop(0, PARTS)
        def _(p):
            add_up(p)

            @pl.when(jnp.logical_and(core == 1, p == 0))
            def _():
                pl.semaphore_wait(pal, 1)

            blk = p * RING + ((chip >> (2 * p)) + 2) % RING
            copy(loc.at[1 - core, blk], din.at[blk], s0, v0.at[p], partner).start()

    with scope("sum2"):
        pl.loop(PARTS, 3 * PARTS)(add_up)
    for delta in (1, 3):
        for p in range(PARTS):
            near(p, delta).start()

    with scope("barrier"):

        @pl.when(core == 1)
        def _():
            pl.semaphore_wait(barrier, 12)
            pl.semaphore_signal(pal, inc=1, device_id={"store": 0}, device_id_type=MESH)

        @pl.when(core == 0)
        def _():
            pl.semaphore_wait(pal, 1)

    for to in beside:
        pl.semaphore_signal(ready, inc=1, device_id=to, device_id_type=MESH)

    def arrived(ref, sem, ssem=s1):
        copy(ref, ref, ssem, sem, partner).wait_recv()

    def link(axis, tile):
        lt[axis] = tile
        for delta in range(1, RING):
            copy(lt.at[axis], lr.at[axis, delta - 1], sl, vl.at[axis], peer(axis, delta)).start()

    def unlink(axis):
        copy(lr.at[axis], lr.at[axis], sl, vl.at[axis], partner).wait_recv()
        tiles = [lt[axis]] + [lr[axis, i] for i in range(3)]
        top = functools.reduce(jnp.maximum, [t[0:1] for t in tiles])
        total = sum(jnp.exp(t[0:1] - top) * t[1:2] for t in tiles)
        return jnp.concatenate([top, total, jnp.zeros((6, LANES), F32)], axis=0)

    def combine(stats):
        m = functools.reduce(jnp.maximum, [s[0:1] for s in stats])
        scales = [jnp.exp(s[0:1] - m) for s in stats]
        zz = sum(c * s[1:2] for c, s in zip(scales, stats))
        return scales, jnp.concatenate([m, zz, jnp.zeros((STAT - 2, LANES), F32)], axis=0)

    chipwise = []

    def issue(delta):
        for p in range(PARTS):
            blk = place(p, delta)
            with scope("w0"):
                if delta == 2:
                    near(p, delta).wait_recv()
                elif p == 0:
                    arrived(din.at[0:PARTS], v0.at[NEAR[delta]], s0)
            if not chipwise:
                chipwise.append(combine([loc[core, blk, 0, tile, :], din[blk, 0, tile, :]]))
            (c_own, c_par), stats = chipwise[0]
            for k in range(RING):
                b = (mid[p] + turn[k]) % RING
                if k == 0:
                    d[p, delta, k, tile, :] = stats
                for rows in pieces:
                    d[p, delta, k, rows, :] = c_own * loc[core, blk, b, rows, :] + c_par * din[blk, b, rows, :]
                for way in range(2):
                    rows = parcel(k, way)
                    if delta == 2:
                        to = peer(order[p][0], toward[way])
                        copy(d.at[p, delta, k, rows], ra.at[way, p, k, rows], s1, va.at[k], to).start()
                    elif delta == toward[1 - way]:
                        to = peer(order[p][0], delta)
                        copy(d.at[p, delta, k, rows], rb.at[way, p, k, rows], s1, vb.at[k * PARTS + p], to).start()

    joint = {}

    def relay(k):
        with scope("wa"):
            arrived(din.at[0:11, 0, 0:24] if k == 0 else ra.at[0, :, k, 0:BLOCK2], va.at[k])
        for p in range(PARTS):
            for way in range(2):
                if k == 0:
                    joint[p, way] = combine([d[p, toward[way], k, tile, :], ra[way, p, k, tile, :]])
                    rd[way, p, k, tile, :] = joint[p, way][1]
                c_own, c_far = joint[p, way][0]
                rows = pieces[(way + k) % 2]
                rd[way, p, k, rows, :] = c_own * d[p, toward[way], k, rows, :] + c_far * ra[way, p, k, rows, :]
                rows = parcel(k, way)
                to = peer(order[p][0], toward[way])
                copy(rd.at[way, p, k, rows], rc.at[way, p, k, rows], s1, vb.at[k * PARTS + p], to).start()

    factors = {}

    def gather(k):
        for p in range(PARTS):
            with scope("w1"):
                arrived(din.at[0:11, 0, 0:16] if k == 0 else din.at[0:2, 0, 0:BLOCK2], vb.at[k * PARTS + p])
            for way in range(2):
                if k == 0:
                    factors[p, way] = combine([d[p, 0, k, tile, :], rb[way, p, k, tile, :], rc[way, p, k, tile, :]])
                c_own, c_one, c_two = factors[p, way][0]
                rows = pieces[(way + k) % 2]
                at = STAT + (rows.start if rows.start == 0 else LEAD)
                e[p, k, at : at + rows.stop - rows.start, :] = (
                    c_own * d[p, 0, k, rows, :] + c_one * rb[way, p, k, rows, :] + c_two * rc[way, p, k, rows, :]
                )
            e[p, k, 0:STAT, :] = factors[p, 0][1]
            to = across(order[p][1], turn[k])
            copy(e.at[p, k], r2.at[p, turn[k]], s2, v2.at[p], to).start()

    issue(2)
    with scope("sum3"):
        pl.loop(3 * PARTS, 4 * PARTS)(add_up)
    for p in range(PARTS):
        near(p, 0).start()
    issue(1)
    with scope("lm"):
        head.wait()
        both = lax.dot_general(q_ref[...], w_ref[...], (((1,), (1,)), ((), ())), preferred_element_type=F32)
        mine = jnp.where(core == 0, both[:ROWS], both[ROWS:])
        logits[...] = mine
        lm_top = jnp.max(mine, axis=1, keepdims=True)
        lm_sum = jnp.sum(jnp.exp(mine - lm_top), axis=1, keepdims=True)
        lane = lax.broadcasted_iota(jnp.int32, (ROWS, LANES), 1)
        pair = jnp.where(lane == 0, lm_top, lm_sum)
        pair = jnp.concatenate([pair] * GROUPS, axis=0).T
        pl.semaphore_wait(ready, 6)
        link(0, pair[0:8, :])
    issue(3)
    issue(0)
    for b in range(RING):
        relay(b)
    link(1, unlink(0))
    for b in range(RING):
        gather(b)
    link(2, unlink(1))

    for p in range(PARTS):
        with scope("w2"):
            copy(r2.at[p], r2.at[p], s2, v2.at[p], partner).wait_recv()
        scales, stats = combine([r2[p, i, 0:STAT, :] for i in range(RING)])
        for c in range(RING):
            rows = slice(STAT + c * SLOTS, STAT + (c + 1) * SLOTS)
            total = scales[0] * r2[p, 0, rows, :]
            for i in range(1, RING):
                total = total + scales[i] * r2[p, i, rows, :]
            g3[p, c, 0:SLOTS, :] = total
            g3[p, c, SLOTS:MSG3, :] = stats[0 : MSG3 - SLOTS]
        for delta in (2, 1, 3, 0):
            to = (last[p] + delta) % RING
            copy(g3.at[p, to], r3.at[p, delta], s3, v3.at[p], across(order[p][2], delta)).start()

    slots = logits.shape[1] // GROUPS
    mix = mix_ref[0, 0]
    with scope("lm2"):
        tsc[...] = jnp.zeros(tsc.shape, F32)
        tsc[0:STAT, :] = unlink(2)
        turned = tsc[...].T
        lm = jnp.exp(logits[...] - turned[0:ROWS, 0:1]) / turned[0:ROWS, 1:2]
        logits[...] = (1.0 - mix) * lm
        copy(loc.at[1 - core], din, s0, v0.at[0], partner).wait_send()
        for sent in (ra, rb, rc):
            for ref in (din.at[0:11, 0, 0:24], sent.at[0, :, 1:RING, 0:BLOCK2]):
                copy(ref, ref, s1, va.at[0], partner).wait_send()
        copy(r2, r2, s2, v2.at[0], partner).wait_send()
        copy(lr, lr, sl, vl.at[0], partner).wait_send()

    for p in range(PARTS):
        with scope("w3"):
            copy(r3.at[p], r3.at[p], s3, v3.at[p], partner).wait_recv()
        blocks = [r3[p, i] for i in range(RING)]
        scales, stats = combine([v[SLOTS : SLOTS + 2] for v in blocks])
        count = min(SLOTS, slots - p * SLOTS)
        total = sum(c * v[0:count] for c, v in zip(scales, blocks))
        tsc[p * SLOTS : p * SLOTS + count, :] = total / stats[1:2]

    with scope("final"):
        turned = tsc[...].T
        for g in range(GROUPS):
            knn[:, g * slots : (g + 1) * slots] = turned[g * ROWS : (g + 1) * ROWS, 0:slots]
        out_ref[...] = jnp.log(mix * knn[...] + logits[...])

    copy(r3, r3, s3, v3.at[0], partner).wait_send()


def solution(mesh):
    def local_step(queries, w_head, store_keys, store_tok, temperature, mix_weight):
        n_keys, width = store_keys.shape
        vocab_loc = w_head.shape[1]
        vmem, smem, hbm = (pl.BlockSpec(memory_space=s) for s in (pltpu.VMEM, pltpu.SMEM, pltpu.HBM))

        in_hbm = lambda a: pltpu.with_memory_space_constraint(a, pltpu.HBM)
        *hist, stats = pl.pallas_call(
            functools.partial(local_kernel, vocab_loc),
            out_shape=[jax.ShapeDtypeStruct((HROWS, LANES), F32)] * NBUF + [jax.ShapeDtypeStruct((2 * NBUF, 2 * LANES), F32)],
            in_specs=[smem, hbm, hbm, hbm],
            out_specs=[vmem] * (NBUF + 1),
            scratch_shapes=[
                pltpu.VMEM(queries.shape, jnp.bfloat16),
                pltpu.VMEM(store_keys.shape, jnp.bfloat16),
                pltpu.VMEM((2 * LANES, width), jnp.bfloat16),
                pltpu.VMEM((n_keys // NBUF, 2 * LANES), F32),
                pltpu.VMEM((2 * n_keys, LANES), F32),
                pltpu.VMEM((n_keys, LANES), F32),
                pltpu.VMEM((n_keys // LANES, LANES), jnp.int32),
                pltpu.SMEM((n_keys,), jnp.int32),
                pltpu.VMEM((n_keys // LANES, LANES), jnp.int32),
                pltpu.SemaphoreType.DMA,
                pltpu.SemaphoreType.DMA,
                pltpu.SemaphoreType.DMA,
                pltpu.SemaphoreType.DMA((2 * NBUF,)),
            ],
            compiler_params=pltpu.CompilerParams(vmem_limit_bytes=KA_LIMIT * 2**20),
            name="histogram",
        )(temperature.reshape(1, 1), in_hbm(store_tok.reshape(n_keys // LANES, LANES)), in_hbm(queries), in_hbm(store_keys))

        return pl.pallas_call(
            comm_kernel,
            out_shape=jax.ShapeDtypeStruct((ROWS, vocab_loc), F32),
            in_specs=[smem] + [vmem] * (NBUF + 2) + [hbm],
            out_specs=vmem,
            scratch_shapes=[
                pltpu.VMEM(w_head.shape[::-1], jnp.bfloat16),
                pltpu.VMEM((ROWS, vocab_loc), F32),
                pltpu.VMEM((2, PARTS * RING, RING, MSG2, LANES), F32),
                pltpu.VMEM((PARTS * RING, RING, MSG2, LANES), F32),
                pltpu.VMEM((PARTS, RING, RING, MSG2, LANES), F32),
                pltpu.VMEM((2, PARTS, RING, MSG2, LANES), F32),
                pltpu.VMEM((2, PARTS, RING, MSG2, LANES), F32),
                pltpu.VMEM((2, PARTS, RING, MSG2, LANES), F32),
                pltpu.VMEM((2, PARTS, RING, MSG2, LANES), F32),
                pltpu.VMEM((PARTS, RING, MSG2, LANES), F32),
                pltpu.VMEM((PARTS, RING, MSG2, LANES), F32),
                pltpu.VMEM((PARTS, RING, MSG3, LANES), F32),
                pltpu.VMEM((PARTS, RING, MSG3, LANES), F32),
                pltpu.VMEM((3, STAT, LANES), F32),
                pltpu.VMEM((3, RING - 1, STAT, LANES), F32),
                pltpu.VMEM((LANES, LANES), F32),
                pltpu.VMEM((ROWS, vocab_loc), F32),
                pltpu.SemaphoreType.DMA,
                pltpu.SemaphoreType.DMA,
                pltpu.SemaphoreType.DMA((6,)),
                pltpu.SemaphoreType.DMA,
                pltpu.SemaphoreType.DMA((4,)),
                pltpu.SemaphoreType.DMA((12,)),
                pltpu.SemaphoreType.REGULAR,
                pltpu.SemaphoreType.REGULAR,
            ]
            + [pltpu.SemaphoreType.DMA, pltpu.SemaphoreType.DMA((3,))] * 3,
            compiler_params=pltpu.CompilerParams(collective_id=0, has_side_effects=True, vmem_limit_bytes=KB_LIMIT * 2**20),
            name="exchange",
        )(mix_weight.reshape(1, 1), *hist, stats, queries, in_hbm(w_head.T))

    return jax.shard_map(
        local_step,
        mesh=mesh,
        in_specs=(P("data", None), P(None, "model"), P(("store", "model"), None), P(("store", "model")), P(), P()),
        out_specs=P(("data", "store"), "model"),
        check_vma=False,
    )
```

```python
import functools

import jax
import jax.numpy as jnp
from jax import lax
from jax.experimental import pallas as pl
from jax.experimental.pallas import tpu as pltpu
from jax.sharding import PartitionSpec as P

F32 = jnp.float32
LANES = 128
RING = 4
CHIPS = RING**3
ROWS = 8
GROUPS = LANES // ROWS
SLOTS = 18
PARTS = 3
BLOCK = SLOTS * CHIPS // RING
BLOCK2 = BLOCK // RING
STAT = 8
MSG2 = STAT + BLOCK2
MSG3 = 24
NEAR = {1: 3, 3: 4, 0: 5}
LEAD = 40
NBUF = 4
KA_LIMIT = 36
KB_LIMIT = 36
HALF = SLOTS * CHIPS * PARTS + 8
HROWS = 2 * HALF
MESH = pl.DeviceIdType.MESH
scope = jax.named_scope


def below(a, n):
    return ((a.astype(F32) + 0.5) * (1.0 / n)).astype(jnp.int32)


def local_kernel(vocab_loc, tau_ref, tok_hbm, q_hbm, k_hbm, *refs):
    hist, stats_ref = refs[:NBUF], refs[NBUF]
    q_ref, k_ref, qrep, sc, wx, grp, idx, idx_smem, tok_ref, qsem, isem, tsem, ksem = refs[NBUF + 1 :]
    n_keys = k_ref.shape[0]
    quarter = n_keys // NBUF
    chunk = quarter // 2
    part_rows = 256

    def fetch(j):
        rows = pl.ds(pl.multiple_of(j * chunk, chunk), chunk)
        return pltpu.make_async_copy(k_hbm.at[rows], k_ref.at[rows], ksem.at[j])

    get_tok = pltpu.make_async_copy(tok_hbm, tok_ref, tsem)
    get_tok.start()
    get_q = pltpu.make_async_copy(q_hbm, q_ref, qsem)
    get_q.start()
    for j in range(2):
        fetch(j).start()
    span = 288
    pieces = 8

    for third in range(3):

        @pl.loop(third * pieces, (third + 1) * pieces)
        def _(i):
            for buf in hist:
                buf[pl.ds(pl.multiple_of(i * span + (i // 12) * 8, 8), span), :] = jnp.zeros((span, LANES), F32)

        for j in ((), (2, 3), (4, 5, 6, 7))[third]:
            fetch(j).start()

    get_tok.wait()
    with scope("index"):
        tok = tok_ref[...]
        chip = below(tok, vocab_loc)
        within = tok - chip * vocab_loc
        slots = vocab_loc // GROUPS
        group = below(within, slots)
        slot = within - group * slots
        part = (slot >= SLOTS).astype(jnp.int32) + (slot >= 2 * SLOTS).astype(jnp.int32)
        row = slot - part * SLOTS
        x, y, z = chip & 3, (chip >> 2) & 3, chip >> 4
        first = jnp.where(part == 0, x, jnp.where(part == 1, y, z))
        second = jnp.where(part == 0, y, jnp.where(part == 1, z, x))
        third = jnp.where(part == 0, z, jnp.where(part == 1, x, y))
        place = ((part * RING + first) * RING + second) * RING + third
        place = place * SLOTS + row
        idx[...] = place
        for r in range(n_keys // LANES):
            pltpu.make_async_copy(idx.at[r], idx_smem.at[pl.ds(r * LANES, LANES)], isem).start()
        lane = lax.broadcasted_iota(jnp.int32, place.shape, 1)
        again = jnp.logical_and(place == pltpu.roll(place, 1, 1), lane % 2 == 1)
    with scope("mask"):
        group = group.astype(F32) + jnp.where(again, float(GROUPS), 0.0)
        square = (LANES, LANES)
        eye = lax.broadcasted_iota(jnp.int32, square, 0) == lax.broadcasted_iota(jnp.int32, square, 1)
        ones = jnp.ones(square, jnp.bfloat16)
        for c in range(n_keys // LANES):
            spread = jnp.where(eye, jnp.broadcast_to(group[c : c + 1, :], square), 0.0).astype(jnp.bfloat16)
            grp[c * LANES : (c + 1) * LANES, :] = jnp.dot(spread, ones, preferred_element_type=F32)

    with scope("turn"):
        get_q.wait()
        for h in range(2):
            half = q_ref[h * ROWS : (h + 1) * ROWS, :].astype(F32)
            pair = jnp.concatenate([half, half], axis=0).astype(jnp.bfloat16)
            for g in range(GROUPS // 2):
                qrep[pl.ds(h * LANES + g * 2 * ROWS, 2 * ROWS), :] = pair

    tau = tau_ref[0, 0]
    unit = jnp.where(tau > 1.0, 2.0**-64, 1.0)
    inv = 1.0 / (tau * unit)
    lane_group = (lax.broadcasted_iota(jnp.int32, (LANES, LANES), 1) // ROWS).astype(F32)

    @pl.loop(0, NBUF)
    def _(b):
        with scope("kw"):
            for sub in range(2):
                fetch(b * 2 + sub).wait()
        with scope("dots"):
            keys = k_ref[pl.ds(pl.multiple_of(b * quarter, quarter), quarter), :]
            dots = lax.dot_general(keys, qrep[...], (((1,), (1,)), ((), ())), preferred_element_type=F32)
            tops = []
            for r in range(0, quarter, part_rows):
                squares = jnp.zeros((part_rows, LANES), F32)
                for c in range(0, keys.shape[1], LANES):
                    kf = keys[r : r + part_rows, c : c + LANES].astype(F32)
                    squares = squares + kf * kf
                norms = jnp.sum(squares, axis=1, keepdims=True)
                scores = ((2.0 * unit) * dots[r : r + part_rows] - unit * norms) * inv
                sc[r : r + part_rows, :] = scores
                tops.append(jnp.max(scores.reshape(part_rows // 8, 8, 2 * LANES), axis=0))
            m = jnp.max(functools.reduce(jnp.maximum, tops), axis=0, keepdims=True)
        with scope("expand"):
            total = jnp.zeros((8, 2 * LANES), F32)
            for c in range(quarter // LANES):
                w = jnp.exp(sc[c * LANES : (c + 1) * LANES, :] - m)
                total = total + jnp.sum(w.reshape(LANES // 8, 8, 2 * LANES), axis=0)
                at = b * quarter + c * LANES
                tag = grp[pl.ds(pl.multiple_of(at, LANES), LANES), :]
                repeat = tag >= GROUPS
                mine = jnp.where(repeat, tag - GROUPS, tag) == lane_group
                for h in range(2):
                    own = jnp.where(mine, w[:, h * LANES : (h + 1) * LANES], 0.0)
                    before = pltpu.roll(own.reshape(LANES // 8, 8, LANES), 1, 1).reshape(LANES, LANES)
                    wx[pl.ds(at * 2 + h, LANES, stride=2), :] = own + jnp.where(repeat, before, 0.0)
            total = jnp.sum(total, axis=0, keepdims=True)
            stats_ref[pl.ds(b, 1), :] = m
            stats_ref[pl.ds(NBUF + b, 1), :] = total

    pltpu.make_async_copy(idx, tok_ref, isem).wait()
    unroll = 32
    rows = quarter // LANES
    with scope("scatter"):
        for c in range(rows):

            @pl.loop(0, LANES // unroll)
            def _(i):
                views = []
                for b in range(NBUF):
                    start = ((b * rows + c) * LANES + i * unroll) * 2
                    views.append(wx.at[pl.ds(pl.multiple_of(start, 2 * unroll), 2 * unroll), :])
                for u in range(0, unroll, 2):
                    both = [(b, v) for b in range(NBUF) for v in (u, u + 1)]
                    at = [idx_smem[(b * rows + c) * LANES + i * unroll + v] for b, v in both]
                    at = [pl.ds(row, 2, stride=HALF) for row in at]
                    new = [hist[b][at[n], :] + views[b][2 * v : 2 * v + 2, :] for n, (b, v) in enumerate(both)]
                    for n, (b, v) in enumerate(both):
                        hist[b][at[n], :] = new[n]


def comm_kernel(
    mix_ref, h0, h1, h2, h3, kstats, q_ref, w_hbm, out_ref,
    w_ref, logits, loc, din, d, ra, rb, rc, rd, e, r2, g3, r3, lt, lr, tsc, knn,
    wsem, s0, v0, s1, va, vb, ready, pal, s2, v2, s3, v3, sl, vl,
):
    core = lax.axis_index("store")
    chip = lax.axis_index("model")
    x, y, z = chip % RING, (chip // RING) % RING, chip // (RING * RING)
    dims = ((x, 1), (y, RING), (z, RING * RING))
    order = ((0, 1, 2), (1, 2, 0), (2, 0, 1))

    def peer(axis, delta):
        at, stride = dims[axis]
        return {"model": chip + ((at + delta) % RING - at) * stride}

    barrier = pltpu.get_barrier_semaphore()
    beside = [peer(axis, delta) for axis in range(3) for delta in (1, RING - 1)]
    for to in beside:
        pl.semaphore_signal(barrier, inc=1, device_id={**to, "store": 1}, device_id_type=MESH)

    @pl.when(core == 1)
    def _():
        pl.semaphore_signal(barrier, inc=1, device_id={"store": 0}, device_id_type=MESH)

    head = pltpu.make_async_copy(w_hbm, w_ref, wsem)
    head.start()

    @pl.when(core == 0)
    def _():
        pl.semaphore_wait(barrier, 1)
        pl.semaphore_signal(pal, inc=1, device_id={"store": 1}, device_id_type=MESH)

    hist = (h0, h1, h2, h3)
    top = functools.reduce(jnp.maximum, [kstats[b : b + 1, :] for b in range(NBUF)])
    scales = [jnp.exp(kstats[b : b + 1, :] - top) for b in range(NBUF)]
    mass = sum(c * kstats[NBUF + b : NBUF + b + 1, :] for b, c in enumerate(scales))
    half = [slice(h * LANES, (h + 1) * LANES) for h in range(2)]

    def add_up(j):
        turn, p = j // PARTS, j % PARTS
        delta = jnp.where(turn == 0, 2, jnp.where(turn == 1, 1, jnp.where(turn == 2, 3, 0)))
        blk = p * RING + ((chip >> (2 * p)) + delta) % RING
        for h in range(2):
            stats = jnp.concatenate([top[:, half[h]], mass[:, half[h]], jnp.zeros((STAT - 2, LANES), F32)], axis=0)
            for b in range(RING):
                loc[h, blk, b, LEAD : LEAD + STAT, :] = stats
                for t in range(BLOCK2 // 8):
                    at = pl.ds(pl.multiple_of(h * HALF + blk * BLOCK + b * BLOCK2 + t * 8, 8), 8)
                    total = scales[0][:, half[h]] * hist[0][at, :]
                    for n in range(1, NBUF):
                        total = total + scales[n][:, half[h]] * hist[n][at, :]
                    row = t * 8 if t * 8 < LEAD else t * 8 + STAT
                    loc[h, blk, b, row : row + 8, :] = total

    def copy(src, dst, ssem, rsem, to):
        return pltpu.make_async_remote_copy(src_ref=src, dst_ref=dst, send_sem=ssem, recv_sem=rsem, device_id=to, device_id_type=MESH)

    tile = slice(LEAD, LEAD + STAT)
    pieces = (slice(0, LEAD), slice(LEAD + STAT, MSG2))
    turn = (2, 1, 3, 0)
    toward = (1, RING - 1)

    def parcel(k, way):
        half = (way + k) % 2
        if k == 0:
            return slice(0, LEAD + STAT) if half == 0 else slice(LEAD, MSG2)
        return pieces[half]

    partner = {"store": 1 - core}

    def across(axis, delta):
        return {**peer(axis, delta), "store": 1 - core} if delta else partner

    first = [dims[order[p][0]][0] for p in range(PARTS)]
    mid = [dims[order[p][1]][0] for p in range(PARTS)]
    last = [dims[order[p][2]][0] for p in range(PARTS)]

    def place(p, delta):
        return p * RING + (first[p] + delta) % RING

    def near(p, delta):
        blk = place(p, delta)
        return copy(loc.at[1 - core, blk], din.at[blk], s0, v0.at[p if delta == 2 else NEAR[delta]], partner)

    with scope("sum"):

        @pl.loop(0, PARTS)
        def _(p):
            add_up(p)

            @pl.when(jnp.logical_and(core == 1, p == 0))
            def _():
                pl.semaphore_wait(pal, 1)

            blk = p * RING + ((chip >> (2 * p)) + 2) % RING
            copy(loc.at[1 - core, blk], din.at[blk], s0, v0.at[p], partner).start()

    with scope("sum2"):
        pl.loop(PARTS, 3 * PARTS)(add_up)
    for delta in (1, 3):
        for p in range(PARTS):
            near(p, delta).start()

    with scope("barrier"):

        @pl.when(core == 1)
        def _():
            pl.semaphore_wait(barrier, 12)
            pl.semaphore_signal(pal, inc=1, device_id={"store": 0}, device_id_type=MESH)

        @pl.when(core == 0)
        def _():
            pl.semaphore_wait(pal, 1)

    for to in beside:
        pl.semaphore_signal(ready, inc=1, device_id=to, device_id_type=MESH)

    def arrived(ref, sem, ssem=s1):
        copy(ref, ref, ssem, sem, partner).wait_recv()

    def link(axis, tile):
        lt[axis] = tile
        for delta in range(1, RING):
            copy(lt.at[axis], lr.at[axis, delta - 1], sl, vl.at[axis], peer(axis, delta)).start()

    def unlink(axis):
        copy(lr.at[axis], lr.at[axis], sl, vl.at[axis], partner).wait_recv()
        tiles = [lt[axis]] + [lr[axis, i] for i in range(3)]
        top = functools.reduce(jnp.maximum, [t[0:1] for t in tiles])
        total = sum(jnp.exp(t[0:1] - top) * t[1:2] for t in tiles)
        return jnp.concatenate([top, total, jnp.zeros((6, LANES), F32)], axis=0)

    def combine(stats):
        m = functools.reduce(jnp.maximum, [s[0:1] for s in stats])
        scales = [jnp.exp(s[0:1] - m) for s in stats]
        zz = sum(c * s[1:2] for c, s in zip(scales, stats))
        return scales, jnp.concatenate([m, zz, jnp.zeros((STAT - 2, LANES), F32)], axis=0)

    chipwise = []

    def issue(delta):
        for p in range(PARTS):
            blk = place(p, delta)
            with scope("w0"):
                if delta == 2:
                    near(p, delta).wait_recv()
                elif p == 0:
                    arrived(din.at[0:PARTS], v0.at[NEAR[delta]], s0)
            if not chipwise:
                chipwise.append(combine([loc[core, blk, 0, tile, :], din[blk, 0, tile, :]]))
            (c_own, c_par), stats = chipwise[0]
            for k in range(RING):
                b = (mid[p] + turn[k]) % RING
                if k == 0:
                    d[p, delta, k, tile, :] = stats
                for rows in pieces:
                    d[p, delta, k, rows, :] = c_own * loc[core, blk, b, rows, :] + c_par * din[blk, b, rows, :]
                for way in range(2):
                    rows = parcel(k, way)
                    if delta == 2:
                        to = peer(order[p][0], toward[way])
                        copy(d.at[p, delta, k, rows], ra.at[way, p, k, rows], s1, va.at[k], to).start()
                    elif delta == toward[1 - way]:
                        to = peer(order[p][0], delta)
                        copy(d.at[p, delta, k, rows], rb.at[way, p, k, rows], s1, vb.at[k * PARTS + p], to).start()

    joint = {}

    def relay(k):
        with scope("wa"):
            arrived(din.at[0:11, 0, 0:24] if k == 0 else ra.at[0, :, k, 0:BLOCK2], va.at[k])
        for p in range(PARTS):
            for way in range(2):
                if k == 0:
                    joint[p, way] = combine([d[p, toward[way], k, tile, :], ra[way, p, k, tile, :]])
                    rd[way, p, k, tile, :] = joint[p, way][1]
                c_own, c_far = joint[p, way][0]
                rows = pieces[(way + k) % 2]
                rd[way, p, k, rows, :] = c_own * d[p, toward[way], k, rows, :] + c_far * ra[way, p, k, rows, :]
                rows = parcel(k, way)
                to = peer(order[p][0], toward[way])
                copy(rd.at[way, p, k, rows], rc.at[way, p, k, rows], s1, vb.at[k * PARTS + p], to).start()

    factors = {}

    def gather(k):
        for p in range(PARTS):
            with scope("w1"):
                arrived(din.at[0:11, 0, 0:16] if k == 0 else din.at[0:2, 0, 0:BLOCK2], vb.at[k * PARTS + p])
            for way in range(2):
                if k == 0:
                    factors[p, way] = combine([d[p, 0, k, tile, :], rb[way, p, k, tile, :], rc[way, p, k, tile, :]])
                c_own, c_one, c_two = factors[p, way][0]
                rows = pieces[(way + k) % 2]
                at = STAT + (rows.start if rows.start == 0 else LEAD)
                e[p, k, at : at + rows.stop - rows.start, :] = (
                    c_own * d[p, 0, k, rows, :] + c_one * rb[way, p, k, rows, :] + c_two * rc[way, p, k, rows, :]
                )
            e[p, k, 0:STAT, :] = factors[p, 0][1]
            to = across(order[p][1], turn[k])
            copy(e.at[p, k], r2.at[p, turn[k]], s2, v2.at[p], to).start()

    issue(2)
    with scope("sum3"):
        pl.loop(3 * PARTS, 4 * PARTS)(add_up)
    for p in range(PARTS):
        near(p, 0).start()
    issue(1)
    with scope("lm"):
        head.wait()
        both = lax.dot_general(q_ref[...], w_ref[...], (((1,), (1,)), ((), ())), preferred_element_type=F32)
        mine = jnp.where(core == 0, both[:ROWS], both[ROWS:])
        logits[...] = mine
        lm_top = jnp.max(mine, axis=1, keepdims=True)
        lm_sum = jnp.sum(jnp.exp(mine - lm_top), axis=1, keepdims=True)
        lane = lax.broadcasted_iota(jnp.int32, (ROWS, LANES), 1)
        pair = jnp.where(lane == 0, lm_top, lm_sum)
        pair = jnp.concatenate([pair] * GROUPS, axis=0).T
        pl.semaphore_wait(ready, 6)
        link(0, pair[0:8, :])
    issue(3)
    issue(0)
    for b in range(RING):
        relay(b)
    link(1, unlink(0))
    for b in range(RING):
        gather(b)
    link(2, unlink(1))

    for p in range(PARTS):
        with scope("w2"):
            copy(r2.at[p], r2.at[p], s2, v2.at[p], partner).wait_recv()
        scales, stats = combine([r2[p, i, 0:STAT, :] for i in range(RING)])
        for c in range(RING):
            rows = slice(STAT + c * SLOTS, STAT + (c + 1) * SLOTS)
            total = scales[0] * r2[p, 0, rows, :]
            for i in range(1, RING):
                total = total + scales[i] * r2[p, i, rows, :]
            g3[p, c, 0:SLOTS, :] = total
            g3[p, c, SLOTS:MSG3, :] = stats[0 : MSG3 - SLOTS]
        for delta in (2, 1, 3, 0):
            to = (last[p] + delta) % RING
            copy(g3.at[p, to], r3.at[p, delta], s3, v3.at[p], across(order[p][2], delta)).start()

    slots = logits.shape[1] // GROUPS
    mix = mix_ref[0, 0]
    with scope("lm2"):
        tsc[...] = jnp.zeros(tsc.shape, F32)
        tsc[0:STAT, :] = unlink(2)
        turned = tsc[...].T
        lm = jnp.exp(logits[...] - turned[0:ROWS, 0:1]) / turned[0:ROWS, 1:2]
        logits[...] = (1.0 - mix) * lm
        copy(loc.at[1 - core], din, s0, v0.at[0], partner).wait_send()
        for sent in (ra, rb, rc):
            for ref in (din.at[0:11, 0, 0:24], sent.at[0, :, 1:RING, 0:BLOCK2]):
                copy(ref, ref, s1, va.at[0], partner).wait_send()
        copy(r2, r2, s2, v2.at[0], partner).wait_send()
        copy(lr, lr, sl, vl.at[0], partner).wait_send()

    for p in range(PARTS):
        with scope("w3"):
            copy(r3.at[p], r3.at[p], s3, v3.at[p], partner).wait_recv()
        blocks = [r3[p, i] for i in range(RING)]
        scales, stats = combine([v[SLOTS : SLOTS + 2] for v in blocks])
        count = min(SLOTS, slots - p * SLOTS)
        total = sum(c * v[0:count] for c, v in zip(scales, blocks))
        tsc[p * SLOTS : p * SLOTS + count, :] = total / stats[1:2]

    with scope("final"):
        turned = tsc[...].T
        for g in range(GROUPS):
            knn[:, g * slots : (g + 1) * slots] = turned[g * ROWS : (g + 1) * ROWS, 0:slots]
        out_ref[...] = jnp.log(mix * knn[...] + logits[...])

    copy(r3, r3, s3, v3.at[0], partner).wait_send()


def solution(mesh):
    def local_step(queries, w_head, store_keys, store_tok, temperature, mix_weight):
        n_keys, width = store_keys.shape
        vocab_loc = w_head.shape[1]
        vmem, smem, hbm = (pl.BlockSpec(memory_space=s) for s in (pltpu.VMEM, pltpu.SMEM, pltpu.HBM))

        in_hbm = lambda a: pltpu.with_memory_space_constraint(a, pltpu.HBM)
        *hist, stats = pl.pallas_call(
            functools.partial(local_kernel, vocab_loc),
            out_shape=[jax.ShapeDtypeStruct((HROWS, LANES), F32)] * NBUF + [jax.ShapeDtypeStruct((2 * NBUF, 2 * LANES), F32)],
            in_specs=[smem, hbm, hbm, hbm],
            out_specs=[vmem] * (NBUF + 1),
            scratch_shapes=[
                pltpu.VMEM(queries.shape, jnp.bfloat16),
                pltpu.VMEM(store_keys.shape, jnp.bfloat16),
                pltpu.VMEM((2 * LANES, width), jnp.bfloat16),
                pltpu.VMEM((n_keys // NBUF, 2 * LANES), F32),
                pltpu.VMEM((2 * n_keys, LANES), F32),
                pltpu.VMEM((n_keys, LANES), F32),
                pltpu.VMEM((n_keys // LANES, LANES), jnp.int32),
                pltpu.SMEM((n_keys,), jnp.int32),
                pltpu.VMEM((n_keys // LANES, LANES), jnp.int32),
                pltpu.SemaphoreType.DMA,
                pltpu.SemaphoreType.DMA,
                pltpu.SemaphoreType.DMA,
                pltpu.SemaphoreType.DMA((2 * NBUF,)),
            ],
            compiler_params=pltpu.CompilerParams(vmem_limit_bytes=KA_LIMIT * 2**20),
            name="histogram",
        )(temperature.reshape(1, 1), in_hbm(store_tok.reshape(n_keys // LANES, LANES)), in_hbm(queries), in_hbm(store_keys))

        return pl.pallas_call(
            comm_kernel,
            out_shape=jax.ShapeDtypeStruct((ROWS, vocab_loc), F32),
            in_specs=[smem] + [vmem] * (NBUF + 2) + [hbm],
            out_specs=vmem,
            scratch_shapes=[
                pltpu.VMEM(w_head.shape[::-1], jnp.bfloat16),
                pltpu.VMEM((ROWS, vocab_loc), F32),
                pltpu.VMEM((2, PARTS * RING, RING, MSG2, LANES), F32),
                pltpu.VMEM((PARTS * RING, RING, MSG2, LANES), F32),
                pltpu.VMEM((PARTS, RING, RING, MSG2, LANES), F32),
                pltpu.VMEM((2, PARTS, RING, MSG2, LANES), F32),
                pltpu.VMEM((2, PARTS, RING, MSG2, LANES), F32),
                pltpu.VMEM((2, PARTS, RING, MSG2, LANES), F32),
                pltpu.VMEM((2, PARTS, RING, MSG2, LANES), F32),
                pltpu.VMEM((PARTS, RING, MSG2, LANES), F32),
                pltpu.VMEM((PARTS, RING, MSG2, LANES), F32),
                pltpu.VMEM((PARTS, RING, MSG3, LANES), F32),
                pltpu.VMEM((PARTS, RING, MSG3, LANES), F32),
                pltpu.VMEM((3, STAT, LANES), F32),
                pltpu.VMEM((3, RING - 1, STAT, LANES), F32),
                pltpu.VMEM((LANES, LANES), F32),
                pltpu.VMEM((ROWS, vocab_loc), F32),
                pltpu.SemaphoreType.DMA,
                pltpu.SemaphoreType.DMA,
                pltpu.SemaphoreType.DMA((6,)),
                pltpu.SemaphoreType.DMA,
                pltpu.SemaphoreType.DMA((4,)),
                pltpu.SemaphoreType.DMA((12,)),
                pltpu.SemaphoreType.REGULAR,
                pltpu.SemaphoreType.REGULAR,
            ]
            + [pltpu.SemaphoreType.DMA, pltpu.SemaphoreType.DMA((3,))] * 3,
            compiler_params=pltpu.CompilerParams(collective_id=0, has_side_effects=True, vmem_limit_bytes=KB_LIMIT * 2**20),
            name="exchange",
        )(mix_weight.reshape(1, 1), *hist, stats, queries, in_hbm(w_head.T))

    return jax.shard_map(
        local_step,
        mesh=mesh,
        in_specs=(P("data", None), P(None, "model"), P(("store", "model"), None), P(("store", "model")), P(), P()),
        out_specs=P(("data", "store"), "model"),
        check_vma=False,
    )
```
